32 devices in a mesh: rep: 8 (over y, x, core), grp: 4 (over z).
Axes of the slice: x: 2, y: 2, z: 4, core: 2. Of those that a mesh axis runs over, the one named last changes fastest.
Arguments:
- images: bfloat16 [320, 197, 384], P(('rep', 'grp')), may hold values from -6 to 6
- cotangent: bfloat16 [320, 197, 384], P(('rep', 'grp')), may hold values from -6 to 6
- ln1_gain: bfloat16 [2, 384], P(None, 'grp'), may hold values from 0.5 to 1.5
- ln1_bias: bfloat16 [2, 384], P(None, 'grp'), may hold values from -1.5 to 1.5
- w_qkv: bfloat16 [2, 384, 1152], P(None, 'grp'), may hold values from -2 to 2
- q_bias: bfloat16 [2, 384], P(None, 'grp'), may hold values from -1.5 to 1.5
- v_bias: bfloat16 [2, 384], P(None, 'grp'), may hold values from -1.5 to 1.5
- w_proj: bfloat16 [2, 384, 384], P(None, 'grp'), may hold values from -1.25 to 1.25
- proj_bias: bfloat16 [2, 384], P(None, 'grp'), may hold values from -1.5 to 1.5
- ln2_gain: bfloat16 [2, 384], P(None, 'grp'), may hold values from 0.5 to 1.5
- ln2_bias: bfloat16 [2, 384], P(None, 'grp'), may hold values from -1.5 to 1.5
- w_up: bfloat16 [2, 384, 1536], P(None, 'grp'), may hold values from -0.3125 to 0.3125
- up_bias: bfloat16 [2, 1536], P(None, 'grp'), may hold values from -1.5 to 1.5
- w_down: bfloat16 [2, 1536, 384], P(None, 'grp'), may hold values from -0.15625 to 0.15625
- down_bias: bfloat16 [2, 384], P(None, 'grp'), may hold values from -1.5 to 1.5
Outputs:
- encoded: bfloat16 [320, 197, 384], P(('rep', 'grp'))
- images_grad: bfloat16 [320, 197, 384], P(('rep', 'grp'))
- grad_ln1_gain: float32 [2, 384], P(None, 'grp')
- grad_ln1_bias: float32 [2, 384], P(None, 'grp')
- grad_w_qkv: float32 [2, 384, 1152], P(None, 'grp')
- grad_q_bias: float32 [2, 384], P(None, 'grp')
- grad_v_bias: float32 [2, 384], P(None, 'grp')
- grad_w_proj: float32 [2, 384, 384], P(None, 'grp')
- grad_proj_bias: float32 [2, 384], P(None, 'grp')
- grad_ln2_gain: float32 [2, 384], P(None, 'grp')
- grad_ln2_bias: float32 [2, 384], P(None, 'grp')
- grad_w_up: float32 [2, 384, 1536], P(None, 'grp')
- grad_up_bias: float32 [2, 1536], P(None, 'grp')
- grad_w_down: float32 [2, 1536, 384], P(None, 'grp')
- grad_down_bias: float32 [2, 384], P(None, 'grp')
The draws below stay inside these ranges and needn't reach their ends.
All inputs are finite; a program needn't handle non-finite values.
Results may differ from the reference program's by a relative error of at most 0.03.
The reference program's roundings to bfloat16 on the way count: a program that leaves them out, or rounds other values in their place, can miss the bound.
Values may be sent and summed in bfloat16 or wider, within the bound.
A program may use at most 256 MiB of HBM per device.

```python
import math
import jax
import jax.numpy as jnp
from jax import lax

D = 384
HEADS = 6
HEAD_DIM = 64
FF = 1536
SEQ = 197
LAYERS = 2
IMG_DEV = 10
IMAGES = 320
N_REP = 8
N_GRP = 4


def draw_w_qkv(key, part):
    width = math.sqrt(D)
    base = jnp.clip(jax.random.normal(key, (LAYERS, D, 3 * D), jnp.float32), -5.0, 5.0) / width
    result = base
    return result.astype(jnp.bfloat16)


def spiked(drawn, stream_key, source, target, shards_of, factor):
    def block_of(dim):
        return (jnp.arange(drawn.shape[dim]) // (drawn.shape[dim] // shards_of)).reshape((-1,) + (1,) * (drawn.ndim - 1 - dim))

    near = jax.random.permutation(stream_key, shards_of)[block_of(target)]
    far = (block_of(target) + shards_of // 2) % shards_of
    return jnp.where((block_of(source) == near) | (block_of(source) == far), factor * drawn, drawn)


def level_of(key, extent, shards, low, high):
    level = 1.0
    for axis_at, blocks in shards:
        heights = jax.random.uniform(jax.random.fold_in(jax.random.fold_in(key, 6), axis_at), (blocks,), jnp.float32, low / len(shards), high / len(shards))
        level = level * jnp.repeat(jnp.exp(heights), extent[axis_at] // blocks).reshape((-1,) + (1,) * (len(extent) - 1 - axis_at))
    return level


def bell_draw(key, extent, scale, bound, shards=(), held_as=jnp.bfloat16):
    array = jax.random.normal(key, extent, jnp.float32) * scale
    if len(shards) > 0:
        array = level_of(key, extent, shards, -0.22, 0.18) * array
    return jnp.clip(array, min=-bound, max=bound).astype(held_as)


def gaussian_with(own_key, shape, scale, bound, cuts, heavy, dtype=jnp.bfloat16):
    entries = scale * jax.random.normal(own_key, shape, jnp.float32)
    if cuts:
        entries = entries * level_of(own_key, shape, cuts, -0.22, 0.18)
    return jnp.clip(spiked(entries, jax.random.fold_in(own_key, 3), *heavy), -bound, bound).astype(dtype)


def setup_inputs(seed: int = 0) -> dict:
    streams_of = jax.random.split(jax.random.key(seed), 16)
    return {
        "images": bell_draw(streams_of[0], (IMAGES, SEQ, D), 1.0, 6.0, ((0, 32),)),
        "cotangent": gaussian_with(streams_of[1], (IMAGES, SEQ, D), 1.0, 6.0, ((0, 32),), (0, 2, 32, 2.75)),
        "ln1_gain": jnp.clip(1.0 + 0.1 * jax.random.normal(streams_of[2], (LAYERS, D), jnp.float32), 0.5, 1.5).astype(jnp.bfloat16),
        "ln1_bias": bell_draw(streams_of[3], (LAYERS, D), 0.3, 1.5, ((1, 4),)),
        "w_qkv": draw_w_qkv(jax.random.fold_in(streams_of[15], 71), 0),
        "q_bias": bell_draw(streams_of[5], (LAYERS, D), 0.3, 1.5, ((1, 4),)),
        "v_bias": bell_draw(streams_of[6], (LAYERS, D), 0.3, 1.5, ((1, 4),)),
        "w_proj": bell_draw(streams_of[7], (LAYERS, D, D), (D // 14) ** -0.5, 1.25, ((1, 4),)),
        "proj_bias": bell_draw(streams_of[8], (LAYERS, D), 0.3, 1.5, ((1, 4),)),
        "ln2_gain": jnp.clip(1.0 + 0.1 * jax.random.normal(streams_of[9], (LAYERS, D), jnp.float32), 0.5, 1.5).astype(jnp.bfloat16),
        "ln2_bias": bell_draw(streams_of[10], (LAYERS, D), 0.3, 1.5, ((1, 4),)),
        "w_up": bell_draw(streams_of[11], (LAYERS, D, FF), D ** -0.5, 0.3125, ((1, 4),)),
        "up_bias": bell_draw(streams_of[12], (LAYERS, FF), 0.3, 1.5, ((1, 4),)),
        "w_down": bell_draw(streams_of[13], (LAYERS, FF, D), FF ** -0.5, 0.15625, ((1, 4),)),
        "down_bias": bell_draw(streams_of[14], (LAYERS, D), 0.3, 1.5, ((1, 4),)),
    }


EPS = 1e-06
INV_ROOT_TWO = 0.7071067811865476
INV_ROOT_TAU = 0.3989422804014327

def norm_forward(hidden, gain_vec, bias_vec):
    mean_rows = lax.optimization_barrier(jnp.mean(hidden, axis=-1, keepdims=True))
    centered = hidden - mean_rows
    variance = lax.optimization_barrier(jnp.mean(centered * centered, axis=-1, keepdims=True))
    inv_std = lax.rsqrt(variance + EPS)
    normed = centered * inv_std
    return (normed * gain_vec.astype(jnp.float32) + bias_vec.astype(jnp.float32), normed, inv_std)

def norm_backward(out_grad, normed, inv_std, gain_vec):
    scaled = out_grad * gain_vec.astype(jnp.float32)
    in_grad = inv_std * (scaled - lax.optimization_barrier(jnp.mean(scaled, axis=-1, keepdims=True)) - normed * lax.optimization_barrier(jnp.mean(scaled * normed, axis=-1, keepdims=True)))
    return (in_grad, lax.optimization_barrier(jnp.sum(out_grad * normed, axis=0)), lax.optimization_barrier(jnp.sum(out_grad, axis=0)))

def gelu_parts(upward):
    cumul = 0.5 * (1.0 + lax.erf(upward * INV_ROOT_TWO))
    return (upward * cumul, cumul + upward * jnp.exp(-0.5 * upward * upward) * INV_ROOT_TAU)

def weight_grad(left, right):
    return lax.dot_general(left, right, (((0,), (0,)), ((), ())), preferred_element_type=jnp.float32)

def back_dot(grad_rows, weight):
    return lax.dot_general(grad_rows, weight, (((1,), (1,)), ((), ())), preferred_element_type=jnp.float32)

def head_split(rows, num_images):
    return rows.reshape(num_images, SEQ, HEADS, HEAD_DIM).astype(jnp.float32)

def attn_scores(query_rows, key_rows, num_images):
    return jnp.einsum('nqhd,nkhd->nhqk', head_split(query_rows, num_images), head_split(key_rows, num_images)) / math.sqrt(HEAD_DIM)

def layer_forward(hidden, weights, num_images):
    gain_one, bias_one, w_qkv, q_bias, v_bias, w_proj, proj_bias, gain_two, bias_two, w_up, up_bias, w_down, down_bias = weights
    normed_in, normed_one, inv_one = norm_forward(hidden, gain_one, bias_one)
    normed_in = normed_in.astype(jnp.bfloat16)
    projected = jnp.dot(normed_in, w_qkv, preferred_element_type=jnp.float32)
    query_rows = (projected[:, :D] + q_bias.astype(jnp.float32)).astype(jnp.bfloat16)
    key_rows = projected[:, D:2 * D].astype(jnp.bfloat16)
    value_rows = (projected[:, 2 * D:] + v_bias.astype(jnp.float32)).astype(jnp.bfloat16)
    scores = attn_scores(query_rows, key_rows, num_images)
    row_max = lax.optimization_barrier(jnp.max(scores, axis=-1, keepdims=True))
    row_total = lax.optimization_barrier(jnp.sum(jnp.exp(scores - row_max), axis=-1, keepdims=True))
    attn_probs = (jnp.exp(scores - row_max) / row_total).astype(jnp.bfloat16)
    context = jnp.einsum('nhqk,nkhd->nqhd', attn_probs.astype(jnp.float32), head_split(value_rows, num_images))
    context = context.reshape(num_images * SEQ, D).astype(jnp.bfloat16)
    mixed = hidden + jnp.dot(context, w_proj, preferred_element_type=jnp.float32) + proj_bias.astype(jnp.float32)
    normed_mid, normed_two, inv_two = norm_forward(mixed, gain_two, bias_two)
    normed_mid = normed_mid.astype(jnp.bfloat16)
    upward = jnp.dot(normed_mid, w_up, preferred_element_type=jnp.float32) + up_bias.astype(jnp.float32)
    active, slope = gelu_parts(upward)
    active = active.astype(jnp.bfloat16)
    output = mixed + jnp.dot(active, w_down, preferred_element_type=jnp.float32) + down_bias.astype(jnp.float32)
    saved = (normed_in, query_rows, key_rows, value_rows, row_max, row_total, context, normed_one, inv_one, normed_mid, slope, active, normed_two, inv_two)
    return (output, saved)

def layer_backward(saved, weights, out_grad, num_images):
    gain_one, bias_one, w_qkv, q_bias, v_bias, w_proj, proj_bias, gain_two, bias_two, w_up, up_bias, w_down, down_bias = weights
    normed_in, query_rows, key_rows, value_rows, row_max, row_total, context, normed_one, inv_one, normed_mid, slope, active, normed_two, inv_two = saved
    out_rounded = out_grad.astype(jnp.bfloat16)
    grad_w_down = weight_grad(active, out_rounded)
    grad_down_bias = lax.optimization_barrier(jnp.sum(out_grad, axis=0))
    up_grad = back_dot(out_rounded, w_down) * slope
    up_rounded = up_grad.astype(jnp.bfloat16)
    grad_up_bias = lax.optimization_barrier(jnp.sum(up_grad, axis=0))
    grad_w_up = weight_grad(normed_mid, up_rounded)
    mid_grad = back_dot(up_rounded, w_up)
    mixed_part, grad_gain_two, grad_bias_two = norm_backward(mid_grad, normed_two, inv_two, gain_two)
    mixed_grad = out_grad + mixed_part
    mixed_rounded = mixed_grad.astype(jnp.bfloat16)
    grad_proj_bias = lax.optimization_barrier(jnp.sum(mixed_grad, axis=0))
    grad_w_proj = weight_grad(context, mixed_rounded)
    context_grad = back_dot(mixed_rounded, w_proj).astype(jnp.bfloat16)
    scores = attn_scores(query_rows, key_rows, num_images)
    attn_full = jnp.exp(scores - row_max) / row_total
    attn_probs = attn_full.astype(jnp.bfloat16)
    ctx_heads = head_split(context_grad, num_images)
    prob_grad = jnp.einsum('nqhd,nkhd->nhqk', ctx_heads, head_split(value_rows, num_images))
    value_grad = jnp.einsum('nhqk,nqhd->nkhd', attn_probs.astype(jnp.float32), ctx_heads)
    row_dot = lax.optimization_barrier(jnp.sum(attn_full * prob_grad, axis=-1, keepdims=True))
    score_grad = (attn_full * (prob_grad - row_dot) / math.sqrt(HEAD_DIM)).astype(jnp.bfloat16)
    query_grad = jnp.einsum('nhqk,nkhd->nqhd', score_grad.astype(jnp.float32), head_split(key_rows, num_images))
    key_grad = jnp.einsum('nhqk,nqhd->nkhd', score_grad.astype(jnp.float32), head_split(query_rows, num_images))
    total_rows = num_images * SEQ
    query_grad = query_grad.reshape(total_rows, D)
    key_grad = key_grad.reshape(total_rows, D)
    value_grad = value_grad.reshape(total_rows, D)
    grad_q_bias = lax.optimization_barrier(jnp.sum(query_grad, axis=0))
    grad_v_bias = lax.optimization_barrier(jnp.sum(value_grad, axis=0))
    joint = jnp.concatenate([query_grad, key_grad, value_grad], axis=1).astype(jnp.bfloat16)
    grad_w_qkv = weight_grad(normed_in, joint)
    in_part, grad_gain_one, grad_bias_one = norm_backward(back_dot(joint, w_qkv), normed_one, inv_one, gain_one)
    grads = (grad_gain_one, grad_bias_one, grad_w_qkv, grad_q_bias, grad_v_bias, grad_w_proj, grad_proj_bias, grad_gain_two, grad_bias_two, grad_w_up, grad_up_bias, grad_w_down, grad_down_bias)
    return (grads, mixed_grad + in_part)

def reference(images, cotangent, ln1_gain, ln1_bias, w_qkv, q_bias, v_bias, w_proj, proj_bias, ln2_gain, ln2_bias, w_up, up_bias, w_down, down_bias):
    params = (ln1_gain, ln1_bias, w_qkv, q_bias, v_bias, w_proj, proj_bias, ln2_gain, ln2_bias, w_up, up_bias, w_down, down_bias)
    blocks = N_REP * N_GRP
    block_rows = IMG_DEV * SEQ
    image_blocks = images.reshape(blocks, block_rows, D)
    grad_blocks = cotangent.reshape(blocks, block_rows, D)

    def scan_step(totals, block_pair):
        block_images, block_grad = block_pair
        hidden = block_images.astype(jnp.float32)
        saved_list = []
        for layer_index in range(LAYERS):
            weights = tuple((member[layer_index] for member in params))
            hidden, saved = layer_forward(hidden, weights, IMG_DEV)
            saved_list.append(saved)
        flowing = block_grad.astype(jnp.float32)
        per_layer = [None] * LAYERS
        for layer_index in reversed(range(LAYERS)):
            weights = tuple((member[layer_index] for member in params))
            grads, flowing = layer_backward(saved_list[layer_index], weights, flowing, IMG_DEV)
            per_layer[layer_index] = grads
        updated = tuple((totals[position] + jnp.stack([per_layer[idx][position] for idx in range(LAYERS)]) for position in range(len(params))))
        return (updated, (hidden.astype(jnp.bfloat16), flowing.astype(jnp.bfloat16)))
    initial = tuple((jnp.zeros(member.shape, jnp.float32) for member in params))
    totals, (outputs, in_grads) = lax.scan(scan_step, initial, (image_blocks, grad_blocks))
    encoded = outputs.reshape(images.shape)
    images_grad = in_grads.reshape(images.shape)
    return (encoded, images_grad, totals[0], totals[1], totals[2], totals[3], totals[4], totals[5], totals[6], totals[7], totals[8], totals[9], totals[10], totals[11], totals[12])
```

```python
import functools

import jax
import jax.numpy as jnp
from jax import lax
from jax.experimental import pallas as pl
from jax.experimental.pallas import tpu as pltpu
from jax.sharding import PartitionSpec as P

HEAD_DIM = 64
PAIR = 2 * HEAD_DIM
EPS = 1e-06
INV_ROOT_TWO = 0.7071067811865476
INV_ROOT_TAU = 0.3989422804014327
MASKED = -1e30
F32 = jnp.float32
BF16 = jnp.bfloat16

G1, B1, QB, VB, PB, G2, B2, DB = range(8)


def dot(left, right):
    return jnp.dot(left, right, preferred_element_type=F32)


def dot_nt(left, right):
    return lax.dot_general(
        left, right, (((1,), (1,)), ((), ())), preferred_element_type=F32
    )


def col_sum(rows):
    return jnp.sum(rows, axis=0, keepdims=True)


def norm(rows):
    mean = jnp.mean(rows, axis=-1, keepdims=True)
    centered = rows - mean
    inv = lax.rsqrt(jnp.mean(centered * centered, axis=-1, keepdims=True) + EPS)
    return centered * inv, inv


def norm_backward(grad, normed, inv, gain):
    scaled = grad * gain
    return inv * (
        scaled
        - jnp.mean(scaled, axis=-1, keepdims=True)
        - normed * jnp.mean(scaled * normed, axis=-1, keepdims=True)
    )


def attn_forward(qkv, keep, image, seq, pad):
    width = qkv.shape[1] // 3
    base = image * pad
    rows = pl.ds(base, pad)
    value_t = qkv[rows, pl.ds(2 * width, width)].T
    lane = lax.broadcasted_iota(jnp.int32, (1, PAIR), 1)
    halves = [(lane < HEAD_DIM).astype(F32).astype(BF16), (lane >= HEAD_DIM).astype(F32).astype(BF16)]
    full = seq // 8 * 8
    for pair in range(width // PAIR):
        queries = qkv[rows, pl.ds(pair * PAIR, PAIR)]
        keys = qkv[rows, pl.ds(width + pair * PAIR, PAIR)]
        for half in range(2):
            head = 2 * pair + half
            scores = dot_nt(keys * halves[half], queries)
            parts = [scores[:full]]
            if full < seq:
                tail = scores[full : full + 8]
                row = lax.broadcasted_iota(jnp.int32, tail.shape, 0)
                parts.append(jnp.where(row < seq - full, tail, MASKED))
            scores = jnp.concatenate(parts, axis=0)
            top = jnp.max(scores, axis=0, keepdims=True)
            raised = jnp.exp(scores - top)
            probs = raised * (1.0 / col_sum(raised))
            rest = pad - probs.shape[0]
            if rest:
                probs = jnp.concatenate([probs, jnp.zeros((rest, pad), F32)], axis=0)
            keep["probs"][image, head] = probs
            context = dot(value_t[head * HEAD_DIM : (head + 1) * HEAD_DIM], probs.astype(BF16))
            keep["context"][image, pl.ds(head * HEAD_DIM, HEAD_DIM), :] = context.astype(BF16)


def layer_forward(hidden, weights, vecs, up_bias, keep, images, seq, pad):
    w_qkv, w_proj, w_up, w_down = weights
    width = hidden.shape[1]
    normed, _ = norm(hidden)
    rows_in = (normed * vecs[G1 : G1 + 1] + vecs[B1 : B1 + 1]).astype(BF16)
    qkv = keep["qkv"]
    projected = dot(rows_in, w_qkv[...])
    qkv[:, :width] = (projected[:, :width] + vecs[QB : QB + 1]).astype(BF16) * jnp.asarray(
        HEAD_DIM**-0.5, BF16
    )
    qkv[:, width : 2 * width] = projected[:, width : 2 * width].astype(BF16)
    qkv[:, 2 * width :] = (projected[:, 2 * width :] + vecs[VB : VB + 1]).astype(BF16)
    for image in range(images):
        attn_forward(qkv, keep, image, seq, pad)
    context = jnp.concatenate([keep["context"][image].T for image in range(images)], axis=0)
    mixed = hidden + dot(context, w_proj[...]) + vecs[PB : PB + 1]
    keep["mixed"][...] = mixed
    normed, _ = norm(mixed)
    rows_mid = (normed * vecs[G2 : G2 + 1] + vecs[B2 : B2 + 1]).astype(BF16)
    upward = dot(rows_mid, w_up[...]) + up_bias[...]
    cumul = 0.5 * (1.0 + lax.erf(upward * INV_ROOT_TWO))
    keep["active"][...] = (upward * cumul).astype(BF16)
    slope = cumul + upward * jnp.exp(-0.5 * upward * upward) * INV_ROOT_TAU
    keep["slope"][...] = slope.astype(keep["slope"].dtype)
    return mixed + dot(keep["active"][...], w_down[...]) + vecs[DB : DB + 1]


def attn_backward(qkv, keep, context_grad, joint, vec_grads, image, pad):
    width = qkv.shape[1] // 3
    rows = pl.ds(image * pad, pad)
    keys_t = qkv[rows, pl.ds(width, width)].T
    lane = lax.broadcasted_iota(jnp.int32, (1, PAIR), 1)
    low = lax.broadcasted_iota(jnp.int32, (pad, PAIR), 1) < HEAD_DIM
    halves = [(lane < HEAD_DIM).astype(F32).astype(BF16), (lane >= HEAD_DIM).astype(F32).astype(BF16)]
    query_parts = []
    for pair in range(width // PAIR):
        queries = qkv[rows, pl.ds(pair * PAIR, PAIR)]
        values = qkv[rows, pl.ds(2 * width + pair * PAIR, PAIR)]
        ctx = context_grad[rows, pl.ds(pair * PAIR, PAIR)]
        key_parts, value_parts = [], []
        for half in range(2):
            head = 2 * pair + half
            probs = keep["probs"][image, head]
            prob_grad = dot_nt(values * halves[half], ctx)
            value_parts.append(dot(probs.astype(BF16), ctx))
            row_dot = col_sum(probs * prob_grad)
            score_grad = (probs * (prob_grad - row_dot)).astype(BF16)
            key_parts.append(dot(score_grad, queries))
            query_parts.append(dot(keys_t[head * HEAD_DIM : (head + 1) * HEAD_DIM], score_grad))
        key_grad = jnp.where(low, key_parts[0], key_parts[1])
        value_grad = jnp.where(low, value_parts[0], value_parts[1])
        joint[rows, pl.ds(width + pair * PAIR, PAIR)] = key_grad.astype(BF16)
        joint[rows, pl.ds(2 * width + pair * PAIR, PAIR)] = value_grad.astype(BF16)
        vec_grads[VB : VB + 1, pl.ds(pair * PAIR, PAIR)] += col_sum(value_grad)
    query_grad = jnp.concatenate(query_parts, axis=0).T * HEAD_DIM**-0.5
    joint[rows, pl.ds(0, width)] = query_grad.astype(BF16)
    vec_grads[QB : QB + 1, :] += col_sum(query_grad)


def layer_backward(out_grad, hidden, weights, vecs, keep, acc, images, pad):
    w_qkv, w_proj, w_up, w_down = weights
    g_qkv, g_proj, g_up, g_down, vec_grads, up_bias_grad, joint, context_grad = acc
    rounded = out_grad.astype(BF16)
    vec_grads[DB : DB + 1, :] += col_sum(out_grad)
    g_down[...] += dot(rounded.T, keep["active"][...])
    up_grad = dot_nt(rounded, w_down[...]) * keep["slope"][...].astype(F32)
    up_bias_grad[...] += col_sum(up_grad)
    up_rounded = up_grad.astype(BF16)
    mixed = keep["mixed"][...]
    normed, inv = norm(mixed)
    gain = vecs[G2 : G2 + 1]
    rows_mid = (normed * gain + vecs[B2 : B2 + 1]).astype(BF16)
    g_up[...] += dot(rows_mid.T, up_rounded)
    mid_grad = dot_nt(up_rounded, w_up[...])
    vec_grads[G2 : G2 + 1, :] += col_sum(mid_grad * normed)
    vec_grads[B2 : B2 + 1, :] += col_sum(mid_grad)
    mixed_grad = out_grad + norm_backward(mid_grad, normed, inv, gain)
    vec_grads[PB : PB + 1, :] += col_sum(mixed_grad)
    mixed_rounded = mixed_grad.astype(BF16)
    part = g_proj[...]
    for image in range(images):
        part += dot(keep["context"][image], mixed_rounded[image * pad : (image + 1) * pad])
    g_proj[...] = part
    context_grad[...] = dot_nt(mixed_rounded, w_proj[...]).astype(BF16)
    for image in range(images):
        attn_backward(keep["qkv"], keep, context_grad, joint, vec_grads, image, pad)
    normed, inv = norm(hidden)
    gain = vecs[G1 : G1 + 1]
    rows_in = (normed * gain + vecs[B1 : B1 + 1]).astype(BF16)
    g_qkv[...] += dot(rows_in.T, joint[...])
    in_grad = dot_nt(joint[...], w_qkv[...])
    vec_grads[G1 : G1 + 1, :] += col_sum(in_grad * normed)
    vec_grads[B1 : B1 + 1, :] += col_sum(in_grad)
    return mixed_grad + norm_backward(in_grad, normed, inv, gain)


def load_padded(ref, buf, pad):
    images, seq, width = ref.shape
    for image in range(images):
        buf[pl.ds(image * pad, seq), :] = ref[image].astype(F32)
        if pad > seq:
            buf[pl.ds(image * pad + seq, pad - seq), :] = jnp.zeros((pad - seq, width), F32)


def store_images(ref, rows, pad):
    images, seq, _ = ref.shape
    for image in range(images):
        ref[image] = rows[image * pad : image * pad + seq].astype(ref.dtype)


KEEP = ("qkv", "probs", "context", "mixed", "active", "slope")


def keep_shapes(images, pad, width, hidden_width):
    heads = width // HEAD_DIM
    return {
        "qkv": ((images * pad, 3 * width), BF16),
        "probs": ((images, heads, pad, pad), F32),
        "context": ((images, width, pad), BF16),
        "mixed": ((images * pad, width), F32),
        "active": ((images * pad, hidden_width), BF16),
        "slope": ((images * pad, hidden_width), F32),
    }


def init_grads(acc):
    @pl.when(pl.program_id(0) == 0)
    def _():
        for ref in acc[:6]:
            ref[...] = jnp.zeros_like(ref)


def flush_grads(acc, outs):
    @pl.when(pl.program_id(0) == pl.num_programs(0) - 1)
    def _():
        g_qkv, g_proj, g_up, g_down, vec_grads, up_bias_grad = acc[:6]
        outs[0][...] = g_qkv[...].astype(BF16)
        outs[1][...] = g_proj[...].astype(BF16)
        outs[2][...] = g_up[...].astype(BF16)
        outs[3][...] = g_down[...].astype(BF16).T
        outs[4][...] = vec_grads[...]
        outs[5][...] = up_bias_grad[...]


def first_kernel(sizes, *refs):
    group, seq, pad = sizes
    images, w0, w1, w2, w3, vecs, up_bias, out = refs[:8]
    keep = dict(zip(KEEP, refs[8:14]))
    (buf,) = refs[14:]
    load_padded(images, buf, pad)
    out[...] = layer_forward(
        buf[...], (w0, w1, w2, w3), vecs, up_bias, keep, group, seq, pad
    )


def middle_kernel(sizes, *refs):
    group, seq, pad = sizes
    hidden, cotangent, w0, w1, w2, w3, vecs, up_bias, encoded, flowing = refs[:10]
    outs = refs[10:16]
    keep = dict(zip(KEEP, refs[16:22]))
    acc = refs[22:30]
    (buf,) = refs[30:]
    weights = (w0, w1, w2, w3)
    init_grads(acc)
    result = layer_forward(hidden[...], weights, vecs, up_bias, keep, group, seq, pad)
    store_images(encoded, result, pad)
    load_padded(cotangent, buf, pad)
    flowing[...] = layer_backward(buf[...], hidden[...], weights, vecs, keep, acc, group, pad)
    flush_grads(acc, outs)


def last_kernel(sizes, *refs):
    group, seq, pad = sizes
    flowing, images, w0, w1, w2, w3, vecs = refs[:7]
    keep = dict(zip(KEEP, refs[7:13]))
    images_grad = refs[13]
    outs = refs[14:20]
    acc = refs[20:28]
    (buf,) = refs[28:]
    init_grads(acc)
    load_padded(images, buf, pad)
    result = layer_backward(
        flowing[...], buf[...], (w0, w1, w2, w3), vecs, keep, acc, group, pad
    )
    store_images(images_grad, result, pad)
    flush_grads(acc, outs)


def whole(shape):
    return pl.BlockSpec(shape, lambda i: (0,) * len(shape), pipeline_mode=pl.Buffered(1))


def rows_spec(shape, steps):
    return pl.BlockSpec(
        (shape[0] // steps,) + tuple(shape[1:]), lambda i: (i,) + (0,) * (len(shape) - 1)
    )


class Plan:
    def __init__(self, images_shape, hidden_width):
        self.count, self.seq, self.width = images_shape
        self.hidden_width = hidden_width
        self.pad = -(-self.seq // 16) * 16
        self.group = 2 if self.count % 2 == 0 else 1
        self.steps = self.count // self.group
        self.rows = self.count * self.pad
        self.keep = keep_shapes(self.count, self.pad, self.width, hidden_width)
        self.keep_block = keep_shapes(self.group, self.pad, self.width, hidden_width)
        self.weight_shapes = [
            (self.width, 3 * self.width),
            (self.width, self.width),
            (self.width, hidden_width),
            (hidden_width, self.width),
        ]
        self.sizes = (self.group, self.seq, self.pad)
        block_rows = self.group * self.pad
        self.buffer = pltpu.VMEM((block_rows, self.width), F32)
        self.acc = [
            pltpu.VMEM(self.weight_shapes[0], F32),
            pltpu.VMEM(self.weight_shapes[1], F32),
            pltpu.VMEM(self.weight_shapes[2], F32),
            pltpu.VMEM((self.width, hidden_width), F32),
            pltpu.VMEM((8, self.width), F32),
            pltpu.VMEM((1, hidden_width), F32),
            pltpu.VMEM((block_rows, 3 * self.width), BF16),
            pltpu.VMEM((block_rows, self.width), BF16),
        ]
        self.grad_shapes = [jax.ShapeDtypeStruct(s, BF16) for s in self.weight_shapes] + [
            jax.ShapeDtypeStruct((8, self.width), F32),
            jax.ShapeDtypeStruct((1, hidden_width), F32),
        ]
        self.params = pltpu.CompilerParams(
            dimension_semantics=("arbitrary",), vmem_limit_bytes=60 * 2**20
        )

    def image_spec(self):
        return rows_spec((self.count, self.seq, self.width), self.steps)

    def state_spec(self):
        return rows_spec((self.rows, self.width), self.steps)

    def param_specs(self):
        return [whole(s) for s in self.weight_shapes] + [
            whole((8, self.width)),
            whole((1, self.hidden_width)),
        ]

    def keep_specs(self):
        return [rows_spec(self.keep[k][0], self.steps) for k in KEEP]

    def grad_specs(self):
        return [whole(s.shape) for s in self.grad_shapes]

    def cost(self, layers):
        rows, width, hidden = self.count * self.seq, self.width, self.hidden_width
        flops = 2 * rows * width * (4 * width + 2 * hidden) * layers
        return pl.CostEstimate(
            flops=int(flops), bytes_accessed=int(40 * 2**20), transcendentals=0
        )

    def first(self, images, weights, vecs, up_bias):
        state = jax.ShapeDtypeStruct((self.rows, self.width), F32)
        keeps = [jax.ShapeDtypeStruct(*self.keep[k]) for k in KEEP]
        out = pl.pallas_call(
            functools.partial(first_kernel, self.sizes),
            name="layer_first",
            out_shape=[state] + keeps,
            grid=(self.steps,),
            in_specs=[self.image_spec()] + self.param_specs(),
            out_specs=[self.state_spec()] + self.keep_specs(),
            scratch_shapes=[self.buffer],
            compiler_params=self.params,
            cost_estimate=self.cost(1),
        )(images, *weights, vecs, up_bias)
        return out[0], out[1:]

    def middle(self, hidden, cotangent, weights, vecs, up_bias):
        state = jax.ShapeDtypeStruct((self.rows, self.width), F32)
        out = pl.pallas_call(
            functools.partial(middle_kernel, self.sizes),
            name="layer_middle",
            out_shape=[jax.ShapeDtypeStruct(cotangent.shape, BF16), state] + self.grad_shapes,
            grid=(self.steps,),
            in_specs=[self.state_spec(), self.image_spec()] + self.param_specs(),
            out_specs=[self.image_spec(), self.state_spec()] + self.grad_specs(),
            scratch_shapes=[pltpu.VMEM(*self.keep_block[k]) for k in KEEP]
            + self.acc
            + [self.buffer],
            compiler_params=self.params,
            cost_estimate=self.cost(3),
        )(hidden, cotangent, *weights, vecs, up_bias)
        return out[0], out[1], out[2:]

    def last(self, flowing, images, weights, vecs, keeps):
        out = pl.pallas_call(
            functools.partial(last_kernel, self.sizes),
            name="layer_last",
            out_shape=[jax.ShapeDtypeStruct(images.shape, BF16)] + self.grad_shapes,
            grid=(self.steps,),
            in_specs=[self.state_spec(), self.image_spec()]
            + self.param_specs()[:5]
            + self.keep_specs(),
            out_specs=[self.image_spec()] + self.grad_specs(),
            scratch_shapes=self.acc + [self.buffer],
            compiler_params=self.params,
            cost_estimate=self.cost(2),
        )(flowing, images, *weights, vecs, *keeps)
        return out[0], out[1:]


def reduce_weights(grads):
    shares = [
        lax.psum_scatter(g, "grp", scatter_dimension=0, tiled=True) for g in grads
    ]
    return [lax.psum(s, "rep").astype(F32) for s in shares]


def on_device(
    images,
    cotangent,
    ln1_gain,
    ln1_bias,
    w_qkv,
    q_bias,
    v_bias,
    w_proj,
    proj_bias,
    ln2_gain,
    ln2_bias,
    w_up,
    up_bias,
    w_down,
    down_bias,
):
    groups = lax.axis_size("grp")
    layers, part = ln1_gain.shape
    width = part * groups
    hidden_part = up_bias.shape[1]
    plan = Plan(images.shape, hidden_part * groups)
    vectors = [ln1_gain, ln1_bias, q_bias, v_bias, proj_bias, ln2_gain, ln2_bias, down_bias]
    packed = jnp.concatenate(vectors + [up_bias], axis=1)
    packed = lax.all_gather(packed, "grp", axis=0, tiled=False)
    vecs = packed[:, :, : 8 * part].reshape(groups, layers, 8, part)
    vecs = vecs.transpose(1, 2, 0, 3).reshape(layers, 8, width).astype(F32)
    up_vecs = packed[:, :, 8 * part :].transpose(1, 0, 2).reshape(layers, 1, -1).astype(F32)
    weights = [
        [
            lax.all_gather(w[layer], "grp", axis=0, tiled=True)
            for w in (w_qkv, w_proj, w_up, w_down)
        ]
        for layer in range(layers)
    ]
    hidden, keeps = plan.first(images, weights[0], vecs[0], up_vecs[0])
    encoded, flowing, grads1 = plan.middle(hidden, cotangent, weights[1], vecs[1], up_vecs[1])
    shares1 = reduce_weights(grads1[:4])
    images_grad, grads0 = plan.last(flowing, images, weights[0], vecs[0], keeps)
    shares0 = reduce_weights(grads0[:4])
    small = jnp.stack([jnp.concatenate([g[4].reshape(-1), g[5].reshape(-1)]) for g in (grads0, grads1)])
    small = lax.psum(small, ("rep", "grp"))
    me = lax.axis_index("grp")
    vec_out = lax.dynamic_slice_in_dim(
        small[:, : 8 * width].reshape(layers, 8, width), me * part, part, axis=2
    )
    up_out = lax.dynamic_slice_in_dim(small[:, 8 * width :], me * hidden_part, hidden_part, axis=1)
    full = [jnp.stack([a, b]) for a, b in zip(shares0, shares1)]
    return (
        encoded,
        images_grad,
        vec_out[:, G1],
        vec_out[:, B1],
        full[0],
        vec_out[:, QB],
        vec_out[:, VB],
        full[1],
        vec_out[:, PB],
        vec_out[:, G2],
        vec_out[:, B2],
        full[2],
        up_out,
        full[3],
        vec_out[:, DB],
    )


def solution(mesh):
    batch = P(("rep", "grp"), None, None)
    vector = P(None, "grp")
    matrix = P(None, "grp", None)
    params = (
        vector,
        vector,
        matrix,
        vector,
        vector,
        matrix,
        vector,
        vector,
        vector,
        matrix,
        vector,
        matrix,
        vector,
    )
    specs = (batch, batch) + params
    return jax.shard_map(
        on_device, mesh=mesh, in_specs=specs, out_specs=specs, check_vma=False
    )
```

```python
import functools
import math

import jax
import jax.numpy as jnp
from jax import lax
from jax.experimental import pallas as pl
from jax.experimental.pallas import tpu as pltpu
from jax.sharding import PartitionSpec as P

HEAD_DIM = 64
PAIR = 2 * HEAD_DIM
EPS = 1e-06
INV_ROOT_TWO = 0.7071067811865476
INV_ROOT_TAU = 0.3989422804014327
MASKED = -1e30
F32 = jnp.float32
BF16 = jnp.bfloat16

VECTORS = 8
G1, B1, QB, VB, PB, G2, B2, DB = range(VECTORS)


def dot(left, right):
    return jnp.dot(left, right, preferred_element_type=F32)


def dot_nt(left, right):
    return lax.dot_general(
        left, right, (((1,), (1,)), ((), ())), preferred_element_type=F32
    )


def col_sum(rows):
    return jnp.sum(rows, axis=0, keepdims=True)


def norm(rows):
    mean = jnp.mean(rows, axis=-1, keepdims=True)
    centered = rows - mean
    inv = lax.rsqrt(jnp.mean(centered * centered, axis=-1, keepdims=True) + EPS)
    return centered * inv, inv


def norm_backward(grad, normed, inv, gain):
    scaled = grad * gain
    return inv * (
        scaled
        - jnp.mean(scaled, axis=-1, keepdims=True)
        - normed * jnp.mean(scaled * normed, axis=-1, keepdims=True)
    )


def attn_forward(qkv, keep, image, seq, pad):
    width = qkv.shape[1] // 3
    base = image * pad
    rows = pl.ds(base, pad)
    value_t = qkv[rows, pl.ds(2 * width, width)].T
    lane = lax.broadcasted_iota(jnp.int32, (1, PAIR), 1)
    halves = [(lane < HEAD_DIM).astype(F32).astype(BF16), (lane >= HEAD_DIM).astype(F32).astype(BF16)]
    full = seq // 8 * 8
    for pair in range(width // PAIR):
        queries = qkv[rows, pl.ds(pair * PAIR, PAIR)]
        keys = qkv[rows, pl.ds(width + pair * PAIR, PAIR)]
        for half in range(2):
            head = 2 * pair + half
            scores = dot_nt(keys * halves[half], queries)
            parts = [scores[:full]]
            if full < seq:
                tail = scores[full : full + 8]
                row = lax.broadcasted_iota(jnp.int32, tail.shape, 0)
                parts.append(jnp.where(row < seq - full, tail, MASKED))
            scores = jnp.concatenate(parts, axis=0)
            top = jnp.max(scores, axis=0, keepdims=True)
            raised = jnp.exp(scores - top)
            probs = raised * (1.0 / col_sum(raised))
            rest = pad - probs.shape[0]
            if rest:
                probs = jnp.concatenate([probs, jnp.zeros((rest, pad), F32)], axis=0)
            keep["probs"][image, head] = probs
            context = dot(value_t[head * HEAD_DIM : (head + 1) * HEAD_DIM], probs.astype(BF16))
            keep["context"][image, pl.ds(head * HEAD_DIM, HEAD_DIM), :] = context.astype(BF16)


def split_weights(wide, w_down):
    width = w_down.shape[1]
    return (
        wide.at[:, pl.ds(0, 3 * width)],
        wide.at[:, pl.ds(3 * width, width)],
        wide.at[:, pl.ds(4 * width, w_down.shape[0])],
        w_down,
    )


def up_bias_of(vecs, hidden_width):
    rows = hidden_width // vecs.shape[1]
    return jnp.concatenate([vecs[VECTORS + i : VECTORS + i + 1] for i in range(rows)], axis=1)


def layer_forward(hidden, weights, vecs, keep, images, seq, pad):
    w_qkv, w_proj, w_up, w_down = weights
    width = hidden.shape[1]
    up_bias = up_bias_of(vecs, w_down.shape[0])
    normed, _ = norm(hidden)
    rows_in = (normed * vecs[G1 : G1 + 1] + vecs[B1 : B1 + 1]).astype(BF16)
    qkv = keep["qkv"]
    projected = dot(rows_in, w_qkv[...])
    qkv[:, :width] = (projected[:, :width] + vecs[QB : QB + 1]).astype(BF16) * jnp.asarray(
        HEAD_DIM**-0.5, BF16
    )
    qkv[:, width : 2 * width] = projected[:, width : 2 * width].astype(BF16)
    qkv[:, 2 * width :] = (projected[:, 2 * width :] + vecs[VB : VB + 1]).astype(BF16)
    for image in range(images):
        attn_forward(qkv, keep, image, seq, pad)
    context = jnp.concatenate([keep["context"][image].T for image in range(images)], axis=0)
    mixed = hidden + dot(context, w_proj[...]) + vecs[PB : PB + 1]
    keep["mixed"][...] = mixed
    normed, _ = norm(mixed)
    rows_mid = (normed * vecs[G2 : G2 + 1] + vecs[B2 : B2 + 1]).astype(BF16)
    upward = dot(rows_mid, w_up[...]) + up_bias
    cumul = 0.5 * (1.0 + lax.erf(upward * INV_ROOT_TWO))
    keep["active"][...] = (upward * cumul).astype(BF16)
    slope = cumul + upward * jnp.exp(-0.5 * upward * upward) * INV_ROOT_TAU
    keep["slope"][...] = slope.astype(keep["slope"].dtype)
    return mixed + dot(keep["active"][...], w_down[...]) + vecs[DB : DB + 1]


def attn_backward(qkv, keep, context_grad, joint, vec_grads, image, pad):
    width = qkv.shape[1] // 3
    rows = pl.ds(image * pad, pad)
    keys_t = qkv[rows, pl.ds(width, width)].T
    lane = lax.broadcasted_iota(jnp.int32, (1, PAIR), 1)
    low = lax.broadcasted_iota(jnp.int32, (pad, PAIR), 1) < HEAD_DIM
    halves = [(lane < HEAD_DIM).astype(F32).astype(BF16), (lane >= HEAD_DIM).astype(F32).astype(BF16)]
    query_parts = []
    for pair in range(width // PAIR):
        queries = qkv[rows, pl.ds(pair * PAIR, PAIR)]
        values = qkv[rows, pl.ds(2 * width + pair * PAIR, PAIR)]
        ctx = context_grad[rows, pl.ds(pair * PAIR, PAIR)]
        key_parts, value_parts = [], []
        for half in range(2):
            head = 2 * pair + half
            probs = keep["probs"][image, head]
            prob_grad = dot_nt(values * halves[half], ctx)
            value_parts.append(dot(probs.astype(BF16), ctx))
            row_dot = col_sum(probs * prob_grad)
            score_grad = (probs * (prob_grad - row_dot)).astype(BF16)
            key_parts.append(dot(score_grad, queries))
            query_parts.append(dot(keys_t[head * HEAD_DIM : (head + 1) * HEAD_DIM], score_grad))
        key_grad = jnp.where(low, key_parts[0], key_parts[1])
        value_grad = jnp.where(low, value_parts[0], value_parts[1])
        joint[rows, pl.ds(width + pair * PAIR, PAIR)] = key_grad.astype(BF16)
        joint[rows, pl.ds(2 * width + pair * PAIR, PAIR)] = value_grad.astype(BF16)
        vec_grads[VB : VB + 1, pl.ds(pair * PAIR, PAIR)] += col_sum(value_grad)
    query_grad = jnp.concatenate(query_parts, axis=0).T * HEAD_DIM**-0.5
    joint[rows, pl.ds(0, width)] = query_grad.astype(BF16)
    vec_grads[QB : QB + 1, :] += col_sum(query_grad)


def layer_backward(out_grad, hidden, weights, vecs, keep, acc, images, pad):
    w_qkv, w_proj, w_up, w_down = weights
    g_qkv, g_proj, g_up, g_down, vec_grads, up_bias_grad, joint, context_grad = acc
    rounded = out_grad.astype(BF16)
    vec_grads[DB : DB + 1, :] += col_sum(out_grad)
    g_down[...] += dot(rounded.T, keep["active"][...])
    up_grad = dot_nt(rounded, w_down[...]) * keep["slope"][...].astype(F32)
    up_bias_grad[...] += col_sum(up_grad)
    up_rounded = up_grad.astype(BF16)
    mixed = keep["mixed"][...]
    normed, inv = norm(mixed)
    gain = vecs[G2 : G2 + 1]
    rows_mid = (normed * gain + vecs[B2 : B2 + 1]).astype(BF16)
    g_up[...] += dot(rows_mid.T, up_rounded)
    mid_grad = dot_nt(up_rounded, w_up[...])
    vec_grads[G2 : G2 + 1, :] += col_sum(mid_grad * normed)
    vec_grads[B2 : B2 + 1, :] += col_sum(mid_grad)
    mixed_grad = out_grad + norm_backward(mid_grad, normed, inv, gain)
    vec_grads[PB : PB + 1, :] += col_sum(mixed_grad)
    mixed_rounded = mixed_grad.astype(BF16)
    part = g_proj[...]
    for image in range(images):
        part += dot(keep["context"][image], mixed_rounded[image * pad : (image + 1) * pad])
    g_proj[...] = part
    context_grad[...] = dot_nt(mixed_rounded, w_proj[...]).astype(BF16)
    for image in range(images):
        attn_backward(keep["qkv"], keep, context_grad, joint, vec_grads, image, pad)
    normed, inv = norm(hidden)
    gain = vecs[G1 : G1 + 1]
    rows_in = (normed * gain + vecs[B1 : B1 + 1]).astype(BF16)
    g_qkv[...] += dot(rows_in.T, joint[...])
    in_grad = dot_nt(joint[...], w_qkv[...])
    vec_grads[G1 : G1 + 1, :] += col_sum(in_grad * normed)
    vec_grads[B1 : B1 + 1, :] += col_sum(in_grad)
    return mixed_grad + norm_backward(in_grad, normed, inv, gain)


def load_padded(ref, buf, pad):
    images, seq, width = ref.shape
    for image in range(images):
        buf[pl.ds(image * pad, seq), :] = ref[image].astype(F32)
        if pad > seq:
            buf[pl.ds(image * pad + seq, pad - seq), :] = jnp.zeros((pad - seq, width), F32)


def store_images(ref, rows, pad):
    images, seq, _ = ref.shape
    for image in range(images):
        ref[image] = rows[image * pad : image * pad + seq].astype(ref.dtype)


KEEP = ("qkv", "probs", "context", "mixed", "active", "slope")


def keep_shapes(images, pad, width, hidden_width):
    heads = width // HEAD_DIM
    return {
        "qkv": ((images * pad, 3 * width), BF16),
        "probs": ((images, heads, pad, pad), F32),
        "context": ((images, width, pad), BF16),
        "mixed": ((images * pad, width), F32),
        "active": ((images * pad, hidden_width), BF16),
        "slope": ((images * pad, hidden_width), F32),
    }


def init_grads(acc):
    @pl.when(pl.program_id(0) == 0)
    def _():
        for ref in acc[:6]:
            ref[...] = jnp.zeros_like(ref)


def flush_grads(acc, outs):
    @pl.when(pl.program_id(0) == pl.num_programs(0) - 1)
    def _():
        g_qkv, g_proj, g_up, g_down, vec_grads, up_bias_grad = acc[:6]
        wide, down, vecs = outs
        g_qkv_out, g_proj_out, g_up_out, g_down_out = split_weights(wide, down)
        g_qkv_out[...] = g_qkv[...].astype(BF16)
        g_proj_out[...] = g_proj[...].astype(BF16)
        g_up_out[...] = g_up[...].astype(BF16)
        g_down_out[...] = g_down[...].astype(BF16).T
        width = vecs.shape[1]
        extra = up_bias_grad.shape[1] // width
        vecs[:VECTORS, :] = vec_grads[...]
        for i in range(extra):
            vecs[VECTORS + i : VECTORS + i + 1, :] = up_bias_grad[:, i * width : (i + 1) * width]
        rest = vecs.shape[0] - VECTORS - extra
        if rest:
            vecs[VECTORS + extra :, :] = jnp.zeros((rest, width), F32)


def first_kernel(sizes, *refs):
    group, seq, pad = sizes
    images, wide, down, vecs, out = refs[:5]
    keep = dict(zip(KEEP, refs[5:11]))
    (buf,) = refs[11:]
    load_padded(images, buf, pad)
    out[...] = layer_forward(
        buf[...], split_weights(wide, down), vecs, keep, group, seq, pad
    )


def middle_kernel(sizes, *refs):
    group, seq, pad = sizes
    hidden, cotangent, wide, down, vecs, encoded, flowing = refs[:7]
    outs = refs[7:10]
    keep = dict(zip(KEEP, refs[10:16]))
    acc = refs[16:24]
    (buf,) = refs[24:]
    weights = split_weights(wide, down)
    init_grads(acc)
    result = layer_forward(hidden[...], weights, vecs, keep, group, seq, pad)
    store_images(encoded, result, pad)
    load_padded(cotangent, buf, pad)
    flowing[...] = layer_backward(buf[...], hidden[...], weights, vecs, keep, acc, group, pad)
    flush_grads(acc, outs)


def last_kernel(sizes, *refs):
    group, seq, pad = sizes
    flowing, images, wide, down, vecs = refs[:5]
    keep = dict(zip(KEEP, refs[5:11]))
    images_grad = refs[11]
    outs = refs[12:15]
    acc = refs[15:23]
    (buf,) = refs[23:]
    init_grads(acc)
    load_padded(images, buf, pad)
    result = layer_backward(
        flowing[...], buf[...], split_weights(wide, down), vecs, keep, acc, group, pad
    )
    store_images(images_grad, result, pad)
    flush_grads(acc, outs)


def whole(shape):
    return pl.BlockSpec(shape, lambda i: (0,) * len(shape), pipeline_mode=pl.Buffered(1))


def rows_spec(shape, steps):
    return pl.BlockSpec(
        (shape[0] // steps,) + tuple(shape[1:]), lambda i: (i,) + (0,) * (len(shape) - 1)
    )


class Plan:
    def __init__(self, images_shape, hidden_width):
        self.count, self.seq, self.width = images_shape
        self.hidden_width = hidden_width
        self.pad = -(-self.seq // 16) * 16
        self.group = 2 if self.count % 2 == 0 else 1
        self.steps = self.count // self.group
        self.rows = self.count * self.pad
        self.keep = keep_shapes(self.count, self.pad, self.width, hidden_width)
        self.keep_block = keep_shapes(self.group, self.pad, self.width, hidden_width)
        self.weight_shapes = [
            (self.width, 3 * self.width),
            (self.width, self.width),
            (self.width, hidden_width),
            (hidden_width, self.width),
        ]
        self.sizes = (self.group, self.seq, self.pad)
        block_rows = self.group * self.pad
        self.buffer = pltpu.VMEM((block_rows, self.width), F32)
        self.acc = [
            pltpu.VMEM(self.weight_shapes[0], F32),
            pltpu.VMEM(self.weight_shapes[1], F32),
            pltpu.VMEM(self.weight_shapes[2], F32),
            pltpu.VMEM((self.width, hidden_width), F32),
            pltpu.VMEM((8, self.width), F32),
            pltpu.VMEM((1, hidden_width), F32),
            pltpu.VMEM((block_rows, 3 * self.width), BF16),
            pltpu.VMEM((block_rows, self.width), BF16),
        ]
        self.vec_rows = -(-(VECTORS + hidden_width // self.width) // 8) * 8
        self.packed_shapes = [
            (self.width, 4 * self.width + hidden_width),
            (hidden_width, self.width),
        ]
        self.vec_shape = (self.vec_rows, self.width)
        self.grad_shapes = [jax.ShapeDtypeStruct(s, BF16) for s in self.packed_shapes] + [
            jax.ShapeDtypeStruct(self.vec_shape, F32)
        ]
        self.params = pltpu.CompilerParams(
            dimension_semantics=("arbitrary",), vmem_limit_bytes=60 * 2**20
        )

    def image_spec(self):
        return rows_spec((self.count, self.seq, self.width), self.steps)

    def state_spec(self):
        return rows_spec((self.rows, self.width), self.steps)

    def param_specs(self):
        return [whole(s) for s in self.packed_shapes + [self.vec_shape]]

    def keep_specs(self):
        return [rows_spec(self.keep[k][0], self.steps) for k in KEEP]

    def grad_specs(self):
        return [whole(s.shape) for s in self.grad_shapes]

    def cost(self, layers):
        rows, width, hidden = self.count * self.seq, self.width, self.hidden_width
        flops = 2 * rows * width * (4 * width + 2 * hidden) * layers
        return pl.CostEstimate(
            flops=int(flops), bytes_accessed=int(40 * 2**20), transcendentals=0
        )

    def first(self, images, weights, vecs):
        state = jax.ShapeDtypeStruct((self.rows, self.width), F32)
        keeps = [jax.ShapeDtypeStruct(*self.keep[k]) for k in KEEP]
        out = pl.pallas_call(
            functools.partial(first_kernel, self.sizes),
            name="layer_first",
            out_shape=[state] + keeps,
            grid=(self.steps,),
            in_specs=[self.image_spec()] + self.param_specs(),
            out_specs=[self.state_spec()] + self.keep_specs(),
            scratch_shapes=[self.buffer],
            compiler_params=self.params,
            cost_estimate=self.cost(1),
        )(images, *weights, vecs)
        return out[0], out[1:]

    def middle(self, hidden, cotangent, weights, vecs):
        state = jax.ShapeDtypeStruct((self.rows, self.width), F32)
        out = pl.pallas_call(
            functools.partial(middle_kernel, self.sizes),
            name="layer_middle",
            out_shape=[jax.ShapeDtypeStruct(cotangent.shape, BF16), state] + self.grad_shapes,
            grid=(self.steps,),
            in_specs=[self.state_spec(), self.image_spec()] + self.param_specs(),
            out_specs=[self.image_spec(), self.state_spec()] + self.grad_specs(),
            scratch_shapes=[pltpu.VMEM(*self.keep_block[k]) for k in KEEP]
            + self.acc
            + [self.buffer],
            compiler_params=self.params,
            cost_estimate=self.cost(3),
        )(hidden, cotangent, *weights, vecs)
        return out[0], out[1], out[2:]

    def last(self, flowing, images, weights, vecs, keeps):
        out = pl.pallas_call(
            functools.partial(last_kernel, self.sizes),
            name="layer_last",
            out_shape=[jax.ShapeDtypeStruct(images.shape, BF16)] + self.grad_shapes,
            grid=(self.steps,),
            in_specs=[self.state_spec(), self.image_spec()]
            + self.param_specs()
            + self.keep_specs(),
            out_specs=[self.image_spec()] + self.grad_specs(),
            scratch_shapes=self.acc + [self.buffer],
            compiler_params=self.params,
            cost_estimate=self.cost(2),
        )(flowing, images, *weights, vecs, *keeps)
        return out[0], out[1:]


def peers_of(reps):
    rep = lax.axis_index("rep")
    cores = 2 if reps % 2 == 0 else 1
    return rep // cores, lax.rem(rep, cores), cores, reps // cores


def greet(targets):
    barrier = pltpu.get_barrier_semaphore()
    for target in targets:
        pl.semaphore_signal(
            barrier, inc=1, device_id=target, device_id_type=pl.DeviceIdType.MESH
        )
    pl.semaphore_wait(barrier, len(targets))


def send(src, dst, sems, at, target):
    copy = pltpu.make_async_remote_copy(
        src_ref=src,
        dst_ref=dst,
        send_sem=sems[0].at[at],
        recv_sem=sems[1].at[at],
        device_id=target,
        device_id_type=pl.DeviceIdType.MESH,
    )
    copy.start()
    return copy


class Split:
    def __init__(self, blocks, columns, cores, chips):
        self.by_columns = columns % (128 * cores) == 0
        self.columns = columns // cores if self.by_columns else columns
        self.blocks = blocks if self.by_columns else blocks // cores
        self.pieces = math.gcd(self.blocks, chips)
        self.run = self.blocks // self.pieces

    def half(self, ref, core, shard=slice(None)):
        if self.by_columns:
            start = pl.multiple_of(core * self.columns, 128)
            return ref.at[shard, :, :, pl.ds(start, self.columns)]
        return ref.at[shard, pl.ds(core * self.blocks, self.blocks)]

    def part(self, ref, core, piece, shard=slice(None)):
        if self.by_columns:
            start = pl.multiple_of(core * self.columns, 128)
            return ref.at[shard, pl.ds(piece * self.run, self.run), :, pl.ds(start, self.columns)]
        return ref.at[shard, pl.ds(core * self.blocks + piece * self.run, self.run)]


def gather_kernel(splits, sizes, *refs):
    groups, reps = sizes
    count = len(splits)
    vec_in, vec_out = refs[count], refs[2 * count + 1]
    ins, outs = refs[:count], refs[count + 1 : 2 * count + 1]
    own_sem, vec_sem = refs[2 * count + 2], refs[2 * count + 3]
    vec_sems, shard_sems, chip_sems, core_sems = (
        refs[2 * count + 4 + 2 * i : 2 * count + 6 + 2 * i] for i in range(4)
    )
    chip, core, cores, chips = peers_of(reps)
    mine = lax.axis_index("grp")
    rep = lax.axis_index("rep")
    shard_peers = [(rep, lax.rem(mine + d, groups)) for d in range(1, groups)]
    chip_steps = sorted({e for s in splits for e in range(1, s.pieces)})

    def chip_at(split, step):
        base = chip // split.pieces * split.pieces
        return base + lax.rem(lax.rem(chip, split.pieces) + step, split.pieces)

    most = max(splits, key=lambda s: s.pieces)
    chip_peers = [(chip_at(most, e) * cores + core, mine) for e in chip_steps]
    core_peers = [(chip * cores + 1 - core, mine)] if cores > 1 else []
    greet(shard_peers + chip_peers + core_peers)

    started = []
    own, over_shards = [], []
    for i, split in enumerate(splits):
        piece = lax.rem(chip, split.pieces)
        src = split.part(ins[i], core, piece, 0)
        dst = split.part(outs[i], core, piece, mine)
        over_shards.append(
            [send(src, dst, shard_sems, (i, d), t) for d, t in enumerate(shard_peers)]
        )
        copy = pltpu.make_async_copy(src, dst, own_sem.at[i])
        copy.start()
        own.append(copy)
        if i == 0:
            vec_copies = [
                send(vec_in.at[0], vec_out.at[mine], vec_sems, d, t)
                for d, t in enumerate(shard_peers)
            ]
            vec_own = pltpu.make_async_copy(vec_in.at[0], vec_out.at[mine], vec_sem)
            vec_own.start()
    over_chips = []
    for i, split in enumerate(splits):
        own[i].wait()
        for copy in over_shards[i]:
            copy.wait_recv()
        piece = lax.rem(chip, split.pieces)
        block = split.part(outs[i], core, piece)
        over_chips.append(
            [
                send(block, block, chip_sems, (i, e - 1), (chip_at(split, e) * cores + core, mine))
                for e in range(1, split.pieces)
            ]
        )
    over_cores = []
    for i, split in enumerate(splits):
        for copy in over_chips[i]:
            copy.wait_recv()
        if cores > 1:
            block = split.half(outs[i], core)
            over_cores.append(send(block, block, core_sems, i, core_peers[0]))
    for copy in over_cores:
        copy.wait_recv()
    for copy in vec_copies:
        copy.wait()
    vec_own.wait()
    for copy in sum(over_shards, []) + sum(over_chips, []) + over_cores:
        copy.wait_send()


def dma_pair(*shape):
    return [pltpu.SemaphoreType.DMA(shape), pltpu.SemaphoreType.DMA(shape)]


VMEM_SPEC = pl.BlockSpec(memory_space=pltpu.VMEM)


def gather(shards, vec, sizes, collective_id):
    groups, reps = sizes
    cores = 2 if reps % 2 == 0 else 1
    splits = [Split(s.shape[0], s.shape[2], cores, reps // cores) for s in shards]
    count = len(shards)
    most = max(s.pieces for s in splits)
    return pl.pallas_call(
        functools.partial(gather_kernel, splits, sizes),
        name="gather_params",
        out_shape=[jax.ShapeDtypeStruct((groups,) + s.shape, s.dtype) for s in shards]
        + [jax.ShapeDtypeStruct((groups,) + vec.shape, vec.dtype)],
        in_specs=[VMEM_SPEC] * (count + 1),
        out_specs=[VMEM_SPEC] * (count + 1),
        scratch_shapes=[pltpu.SemaphoreType.DMA((count,)), pltpu.SemaphoreType.DMA]
        + dma_pair(groups - 1)
        + dma_pair(count, groups - 1)
        + dma_pair(count, max(most - 1, 1))
        + dma_pair(count),
        compiler_params=pltpu.CompilerParams(
            collective_id=collective_id, has_side_effects=True, vmem_limit_bytes=40 * 2**20
        ),
    )(*[s[None] for s in shards], vec[None])


def add_up(first, rest):
    total = first.astype(F32)
    for term in rest:
        total = total + term.astype(F32)
    return total


def reduce_kernel(splits, sizes, *refs):
    groups, reps = sizes
    count = len(splits)
    ins, vec_in = refs[:count], refs[count]
    outs, vec_out = refs[count + 1 : 2 * count + 1], refs[2 * count + 1]
    at = 2 * count + 2
    from_core, core_sum, from_chips, chip_sum, from_shards = (
        refs[at + i * count : at + (i + 1) * count] for i in range(5)
    )
    at += 5 * count
    vec_parts, vec_held = refs[at], refs[at + 1]
    at += 2
    core_sems, chip_sems, shard_sems, spread_sems, join_sems, vec_sems = (
        refs[at + 2 * i : at + 2 * i + 2] for i in range(6)
    )
    chip, core, cores, chips = peers_of(reps)
    mine = lax.axis_index("grp")
    rep = lax.axis_index("rep")
    shard_peers = [(rep, lax.rem(mine + d, groups)) for d in range(1, groups)]
    chip_ids = [lax.rem(chip + e, chips) for e in range(1, chips)]
    chip_peers = [(c * cores + core, mine) for c in chip_ids]
    core_peers = [(chip * cores + 1 - core, mine)] if cores > 1 else []
    greet(shard_peers + chip_peers + core_peers)
    sent = []
    arrivals = []
    if cores > 1:
        for i, split in enumerate(splits):
            arrivals.append(
                send(split.half(ins[i], 1 - core), from_core[i], core_sems, i, core_peers[0])
            )
        vec_core = send(vec_in, vec_parts.at[0], vec_sems, 0, core_peers[0])
        sent += arrivals + [vec_core]
    chip_arrivals = []
    for i, split in enumerate(splits):
        own = split.half(ins[i], core)[...]
        if cores > 1:
            arrivals[i].wait_recv()
            own = add_up(own, [from_core[i][...]]).astype(BF16)
        core_sum[i][...] = own
        copies = []
        for e, target in enumerate(chip_peers):
            piece = lax.rem(chip_ids[e], split.pieces)
            src = core_sum[i].at[:, pl.ds(piece * split.run, split.run)]
            copies.append(send(src, from_chips[i].at[e], chip_sems, (i, e), target))
        chip_arrivals.append(copies)
        sent += copies
    own = vec_in[...]
    if cores > 1:
        vec_core.wait_recv()
        own = own + vec_parts[0]
    vec_held[0] = own
    vec_chip = [
        send(vec_held.at[0], vec_parts.at[1 + e], vec_sems, 1 + e, t)
        for e, t in enumerate(chip_peers)
    ]
    sent += vec_chip
    shard_arrivals = []
    for i, split in enumerate(splits):
        piece = lax.rem(chip, split.pieces)
        own = core_sum[i][:, pl.ds(piece * split.run, split.run)]
        for copy in chip_arrivals[i]:
            copy.wait_recv()
        total = add_up(own, [from_chips[i][e] for e in range(len(chip_peers))])
        chip_sum[i][...] = total.astype(BF16)
        copies = [
            send(
                chip_sum[i].at[lax.rem(mine + d + 1, groups)],
                from_shards[i].at[d],
                shard_sems,
                (i, d),
                target,
            )
            for d, target in enumerate(shard_peers)
        ]
        shard_arrivals.append(copies)
        sent += copies
    own = vec_held[0]
    for e, copy in enumerate(vec_chip):
        copy.wait_recv()
        own = own + vec_parts[1 + e]
    vec_held[1] = own
    vec_shard = [
        send(vec_held.at[1], vec_parts.at[chips + d], vec_sems, chips + d, t)
        for d, t in enumerate(shard_peers)
    ]
    sent += vec_shard
    spreads = []
    for i, split in enumerate(splits):
        piece = lax.rem(chip, split.pieces)
        own = chip_sum[i][mine]
        for copy in shard_arrivals[i]:
            copy.wait_recv()
        total = add_up(own, [from_shards[i][d] for d in range(len(shard_peers))])
        block = split.part(outs[i], core, piece, 0)
        block[...] = total.astype(BF16)
        base = chip // split.pieces * split.pieces
        copies = []
        for e in range(1, split.pieces):
            other = base + lax.rem(piece + e, split.pieces)
            copies.append(
                send(block, block, spread_sems, (i, e - 1), (other * cores + core, mine))
            )
        spreads.append(copies)
        sent += copies
    own = vec_held[1]
    for d, copy in enumerate(vec_shard):
        copy.wait_recv()
        own = own + vec_parts[chips + d]
    vec_out[...] = own
    joins = []
    for i, split in enumerate(splits):
        for copy in spreads[i]:
            copy.wait_recv()
        if cores > 1:
            block = split.half(outs[i], core, 0)
            joins.append(send(block, block, join_sems, i, core_peers[0]))
    for copy in joins:
        copy.wait_recv()
    for copy in sent + joins:
        copy.wait_send()


def reduce_grads(grads, vec, sizes, collective_id):
    groups, reps = sizes
    cores = 2 if reps % 2 == 0 else 1
    chips = reps // cores
    splits = [Split(g.shape[1], g.shape[3], cores, chips) for g in grads]
    count = len(grads)
    most = max(s.pieces for s in splits)
    half = [(groups, s.blocks, 8, s.columns) for s in splits]
    piece = [(groups, s.run, 8, s.columns) for s in splits]
    shapes = (
        half
        + half
        + [(chips - 1,) + p for p in piece]
        + piece
        + [(groups - 1,) + p[1:] for p in piece]
    )
    vec_terms = chips + groups - 1
    out = pl.pallas_call(
        functools.partial(reduce_kernel, splits, sizes),
        name="reduce_grads",
        out_shape=[jax.ShapeDtypeStruct((1,) + g.shape[1:], BF16) for g in grads]
        + [jax.ShapeDtypeStruct(vec.shape, F32)],
        in_specs=[VMEM_SPEC] * (count + 1),
        out_specs=[VMEM_SPEC] * (count + 1),
        scratch_shapes=[pltpu.VMEM(s, BF16) for s in shapes]
        + [pltpu.VMEM((vec_terms,) + vec.shape, F32), pltpu.VMEM((2,) + vec.shape, F32)]
        + dma_pair(count)
        + dma_pair(count, chips - 1)
        + dma_pair(count, groups - 1)
        + dma_pair(count, max(most - 1, 1))
        + dma_pair(count)
        + dma_pair(vec_terms),
        compiler_params=pltpu.CompilerParams(
            collective_id=collective_id, has_side_effects=True, vmem_limit_bytes=40 * 2**20
        ),
    )(*grads, vec)
    return [o[0] for o in out[:count]], out[count]


def on_device(
    reps,
    images,
    cotangent,
    ln1_gain,
    ln1_bias,
    w_qkv,
    q_bias,
    v_bias,
    w_proj,
    proj_bias,
    ln2_gain,
    ln2_bias,
    w_up,
    up_bias,
    w_down,
    down_bias,
):
    groups = lax.axis_size("grp")
    sizes = (groups, reps)
    layers, part = ln1_gain.shape
    width = part * groups
    hidden_part = up_bias.shape[1]
    plan = Plan(images.shape, hidden_part * groups)
    vectors = [ln1_gain, ln1_bias, q_bias, v_bias, proj_bias, ln2_gain, ln2_bias, down_bias]
    extra = hidden_part // part
    packed = jnp.stack(vectors, axis=1)
    packed = jnp.concatenate([packed, up_bias.reshape(layers, extra, part)], axis=1)
    packed = packed.astype(F32)
    wide = jnp.concatenate([w_qkv, w_proj, w_up], axis=2)

    def layer_params(layer):
        shards = [wide[layer].reshape(-1, 8, wide.shape[2]), w_down[layer].reshape(-1, 8, width)]
        big, down, vecs = gather(shards, packed[layer], sizes, layer)
        vectors = vecs[:, :VECTORS].transpose(1, 0, 2).reshape(VECTORS, width)
        up = vecs[:, VECTORS:].reshape(extra, width)
        rest = plan.vec_rows - VECTORS - extra
        vecs = jnp.concatenate([vectors, up, jnp.zeros((rest, width), F32)], axis=0)
        return [big.reshape(width, -1), down.reshape(-1, width)], vecs

    def reduced(grads, layer):
        blocks = [
            grads[0].reshape(groups, -1, 8, grads[0].shape[1]),
            grads[1].reshape(groups, -1, 8, width),
        ]
        shares, vec = reduce_grads(blocks, grads[2], sizes, layers + layer)
        return [s.reshape(-1, s.shape[2]) for s in shares], vec

    weights0, vecs0 = layer_params(0)
    weights1, vecs1 = layer_params(1)
    hidden, keeps = plan.first(images, weights0, vecs0)
    encoded, flowing, grads1 = plan.middle(hidden, cotangent, weights1, vecs1)
    shares1, small1 = reduced(grads1, 1)
    images_grad, grads0 = plan.last(flowing, images, weights0, vecs0, keeps)
    shares0, small0 = reduced(grads0, 0)
    small = jnp.stack([small0, small1])
    me = lax.axis_index("grp")
    vec_out = lax.dynamic_slice_in_dim(small[:, :VECTORS], me * part, part, axis=2)
    up_out = small[:, VECTORS : VECTORS + extra].reshape(layers, -1)
    up_out = lax.dynamic_slice_in_dim(up_out, me * hidden_part, hidden_part, axis=1)
    full = [jnp.stack([a, b]).astype(F32) for a, b in zip(shares0, shares1)]
    columns = w_qkv.shape[2], w_qkv.shape[2] + width
    return (
        encoded,
        images_grad,
        vec_out[:, G1],
        vec_out[:, B1],
        full[0][:, :, : columns[0]],
        vec_out[:, QB],
        vec_out[:, VB],
        full[0][:, :, columns[0] : columns[1]],
        vec_out[:, PB],
        vec_out[:, G2],
        vec_out[:, B2],
        full[0][:, :, columns[1] :],
        up_out,
        full[1],
        vec_out[:, DB],
    )


def solution(mesh):
    batch = P(("rep", "grp"), None, None)
    vector = P(None, "grp")
    matrix = P(None, "grp", None)
    params = (
        vector,
        vector,
        matrix,
        vector,
        vector,
        matrix,
        vector,
        vector,
        vector,
        matrix,
        vector,
        matrix,
        vector,
    )
    specs = (batch, batch) + params
    return jax.shard_map(
        functools.partial(on_device, mesh.shape["rep"]), mesh=mesh, in_specs=specs, out_specs=specs, check_vma=False
    )
```

```python
import functools
import math

import jax
import jax.numpy as jnp
from jax import lax
from jax.experimental import pallas as pl
from jax.experimental.pallas import tpu as pltpu
from jax.sharding import PartitionSpec as P

HEAD_DIM = 64
PAIR = 2 * HEAD_DIM
EPS = 1e-06
INV_ROOT_TWO = 0.7071067811865476
INV_ROOT_TAU = 0.3989422804014327
MASKED = -1e30
F32 = jnp.float32
BF16 = jnp.bfloat16

VECTORS = 8
G1, B1, QB, VB, PB, G2, B2, DB = range(VECTORS)


def dot(left, right):
    return jnp.dot(left, right, preferred_element_type=F32)


def dot_nt(left, right):
    return lax.dot_general(
        left, right, (((1,), (1,)), ((), ())), preferred_element_type=F32
    )


def col_sum(rows):
    return jnp.sum(rows, axis=0, keepdims=True)


def norm(rows):
    mean = jnp.mean(rows, axis=-1, keepdims=True)
    centered = rows - mean
    inv = lax.rsqrt(jnp.mean(centered * centered, axis=-1, keepdims=True) + EPS)
    return centered * inv, inv


def norm_backward(grad, normed, inv, gain):
    scaled = grad * gain
    return inv * (
        scaled
        - jnp.mean(scaled, axis=-1, keepdims=True)
        - normed * jnp.mean(scaled * normed, axis=-1, keepdims=True)
    )


def attn_forward(qkv, keep, image, seq, pad):
    width = qkv.shape[1] // 3
    base = image * pad
    rows = pl.ds(base, pad)
    value_t = qkv[rows, pl.ds(2 * width, width)].T
    lane = lax.broadcasted_iota(jnp.int32, (1, PAIR), 1)
    halves = [(lane < HEAD_DIM).astype(F32).astype(BF16), (lane >= HEAD_DIM).astype(F32).astype(BF16)]
    full = seq // 8 * 8
    for pair in range(width // PAIR):
        queries = qkv[rows, pl.ds(pair * PAIR, PAIR)]
        keys = qkv[rows, pl.ds(width + pair * PAIR, PAIR)]
        for half in range(2):
            head = 2 * pair + half
            scores = dot_nt(keys * halves[half], queries)
            parts = [scores[:full]]
            if full < seq:
                tail = scores[full : full + 8]
                row = lax.broadcasted_iota(jnp.int32, tail.shape, 0)
                parts.append(jnp.where(row < seq - full, tail, MASKED))
            scores = jnp.concatenate(parts, axis=0)
            top = jnp.max(scores, axis=0, keepdims=True)
            raised = jnp.exp(scores - top)
            probs = raised * (1.0 / col_sum(raised))
            rest = pad - probs.shape[0]
            if rest:
                probs = jnp.concatenate([probs, jnp.zeros((rest, pad), F32)], axis=0)
            keep["probs"][image, head] = probs
            context = dot(value_t[head * HEAD_DIM : (head + 1) * HEAD_DIM], probs.astype(BF16))
            keep["context"][image, pl.ds(head * HEAD_DIM, HEAD_DIM), :] = context.astype(BF16)


def split_weights(wide, w_down):
    width = w_down.shape[1]
    return (
        wide.at[:, pl.ds(0, 3 * width)],
        wide.at[:, pl.ds(3 * width, width)],
        wide.at[:, pl.ds(4 * width, w_down.shape[0])],
        w_down,
    )


def up_bias_of(vecs, hidden_width):
    rows = hidden_width // vecs.shape[1]
    return jnp.concatenate([vecs[VECTORS + i : VECTORS + i + 1] for i in range(rows)], axis=1)


def layer_forward(hidden, weights, vecs, keep, images, seq, pad):
    w_qkv, w_proj, w_up, w_down = weights
    width = hidden.shape[1]
    up_bias = up_bias_of(vecs, w_down.shape[0])
    normed, _ = norm(hidden)
    rows_in = (normed * vecs[G1 : G1 + 1] + vecs[B1 : B1 + 1]).astype(BF16)
    qkv = keep["qkv"]
    projected = dot(rows_in, w_qkv[...])
    qkv[:, :width] = (projected[:, :width] + vecs[QB : QB + 1]).astype(BF16) * jnp.asarray(
        HEAD_DIM**-0.5, BF16
    )
    qkv[:, width : 2 * width] = projected[:, width : 2 * width].astype(BF16)
    qkv[:, 2 * width :] = (projected[:, 2 * width :] + vecs[VB : VB + 1]).astype(BF16)
    for image in range(images):
        attn_forward(qkv, keep, image, seq, pad)
    context = jnp.concatenate([keep["context"][image].T for image in range(images)], axis=0)
    mixed = hidden + dot(context, w_proj[...]) + vecs[PB : PB + 1]
    keep["mixed"][...] = mixed
    normed, _ = norm(mixed)
    rows_mid = (normed * vecs[G2 : G2 + 1] + vecs[B2 : B2 + 1]).astype(BF16)
    upward = dot(rows_mid, w_up[...]) + up_bias
    cumul = 0.5 * (1.0 + lax.erf(upward * INV_ROOT_TWO))
    keep["active"][...] = (upward * cumul).astype(BF16)
    slope = cumul + upward * jnp.exp(-0.5 * upward * upward) * INV_ROOT_TAU
    keep["slope"][...] = slope.astype(keep["slope"].dtype)
    return mixed + dot(keep["active"][...], w_down[...]) + vecs[DB : DB + 1]


def attn_backward(qkv, keep, context_grad, joint, vec_grads, image, pad):
    width = qkv.shape[1] // 3
    rows = pl.ds(image * pad, pad)
    keys_t = qkv[rows, pl.ds(width, width)].T
    lane = lax.broadcasted_iota(jnp.int32, (1, PAIR), 1)
    low = lax.broadcasted_iota(jnp.int32, (pad, PAIR), 1) < HEAD_DIM
    halves = [(lane < HEAD_DIM).astype(F32).astype(BF16), (lane >= HEAD_DIM).astype(F32).astype(BF16)]
    query_parts = []
    for pair in range(width // PAIR):
        queries = qkv[rows, pl.ds(pair * PAIR, PAIR)]
        values = qkv[rows, pl.ds(2 * width + pair * PAIR, PAIR)]
        ctx = context_grad[rows, pl.ds(pair * PAIR, PAIR)]
        key_parts, value_parts = [], []
        for half in range(2):
            head = 2 * pair + half
            probs = keep["probs"][image, head]
            prob_grad = dot_nt(values * halves[half], ctx)
            value_parts.append(dot(probs.astype(BF16), ctx))
            row_dot = col_sum(probs * prob_grad)
            score_grad = (probs * (prob_grad - row_dot)).astype(BF16)
            key_parts.append(dot(score_grad, queries))
            query_parts.append(dot(keys_t[head * HEAD_DIM : (head + 1) * HEAD_DIM], score_grad))
        key_grad = jnp.where(low, key_parts[0], key_parts[1])
        value_grad = jnp.where(low, value_parts[0], value_parts[1])
        joint[rows, pl.ds(width + pair * PAIR, PAIR)] = key_grad.astype(BF16)
        joint[rows, pl.ds(2 * width + pair * PAIR, PAIR)] = value_grad.astype(BF16)
        vec_grads[VB : VB + 1, pl.ds(pair * PAIR, PAIR)] += col_sum(value_grad)
    query_grad = jnp.concatenate(query_parts, axis=0).T * HEAD_DIM**-0.5
    joint[rows, pl.ds(0, width)] = query_grad.astype(BF16)
    vec_grads[QB : QB + 1, :] += col_sum(query_grad)


def layer_backward(out_grad, hidden, weights, vecs, keep, acc, images, pad):
    w_qkv, w_proj, w_up, w_down = weights
    g_qkv, g_proj, g_up, g_down, vec_grads, up_bias_grad, joint, context_grad = acc
    rounded = out_grad.astype(BF16)
    vec_grads[DB : DB + 1, :] += col_sum(out_grad)
    g_down[...] += dot(rounded.T, keep["active"][...])
    up_grad = dot_nt(rounded, w_down[...]) * keep["slope"][...].astype(F32)
    up_bias_grad[...] += col_sum(up_grad)
    up_rounded = up_grad.astype(BF16)
    mixed = keep["mixed"][...]
    normed, inv = norm(mixed)
    gain = vecs[G2 : G2 + 1]
    rows_mid = (normed * gain + vecs[B2 : B2 + 1]).astype(BF16)
    g_up[...] += dot(rows_mid.T, up_rounded)
    mid_grad = dot_nt(up_rounded, w_up[...])
    vec_grads[G2 : G2 + 1, :] += col_sum(mid_grad * normed)
    vec_grads[B2 : B2 + 1, :] += col_sum(mid_grad)
    mixed_grad = out_grad + norm_backward(mid_grad, normed, inv, gain)
    vec_grads[PB : PB + 1, :] += col_sum(mixed_grad)
    mixed_rounded = mixed_grad.astype(BF16)
    part = g_proj[...]
    for image in range(images):
        part += dot(keep["context"][image], mixed_rounded[image * pad : (image + 1) * pad])
    g_proj[...] = part
    context_grad[...] = dot_nt(mixed_rounded, w_proj[...]).astype(BF16)
    for image in range(images):
        attn_backward(keep["qkv"], keep, context_grad, joint, vec_grads, image, pad)
    normed, inv = norm(hidden)
    gain = vecs[G1 : G1 + 1]
    rows_in = (normed * gain + vecs[B1 : B1 + 1]).astype(BF16)
    g_qkv[...] += dot(rows_in.T, joint[...])
    in_grad = dot_nt(joint[...], w_qkv[...])
    vec_grads[G1 : G1 + 1, :] += col_sum(in_grad * normed)
    vec_grads[B1 : B1 + 1, :] += col_sum(in_grad)
    return mixed_grad + norm_backward(in_grad, normed, inv, gain)


def load_padded(ref, buf, pad):
    images, seq, width = ref.shape
    for image in range(images):
        buf[pl.ds(image * pad, seq), :] = ref[image].astype(F32)
        if pad > seq:
            buf[pl.ds(image * pad + seq, pad - seq), :] = jnp.zeros((pad - seq, width), F32)


def store_images(ref, rows, pad):
    images, seq, _ = ref.shape
    for image in range(images):
        ref[image] = rows[image * pad : image * pad + seq].astype(ref.dtype)


KEEP = ("qkv", "probs", "context", "mixed", "active", "slope")


def keep_shapes(images, pad, width, hidden_width):
    heads = width // HEAD_DIM
    return {
        "qkv": ((images * pad, 3 * width), BF16),
        "probs": ((images, heads, pad, pad), F32),
        "context": ((images, width, pad), BF16),
        "mixed": ((images * pad, width), F32),
        "active": ((images * pad, hidden_width), BF16),
        "slope": ((images * pad, hidden_width), F32),
    }


def init_grads(acc):
    @pl.when(pl.program_id(0) == 0)
    def _():
        for ref in acc[:6]:
            ref[...] = jnp.zeros_like(ref)


def flush_grads(acc, outs):
    @pl.when(pl.program_id(0) == pl.num_programs(0) - 1)
    def _():
        g_qkv, g_proj, g_up, g_down, vec_grads, up_bias_grad = acc[:6]
        wide, down, vecs = outs
        g_qkv_out, g_proj_out, g_up_out, g_down_out = split_weights(wide, down)
        g_qkv_out[...] = g_qkv[...].astype(BF16)
        g_proj_out[...] = g_proj[...].astype(BF16)
        g_up_out[...] = g_up[...].astype(BF16)
        g_down_out[...] = g_down[...].astype(BF16).T
        width = vecs.shape[1]
        extra = up_bias_grad.shape[1] // width
        vecs[:VECTORS, :] = vec_grads[...]
        for i in range(extra):
            vecs[VECTORS + i : VECTORS + i + 1, :] = up_bias_grad[:, i * width : (i + 1) * width]
        rest = vecs.shape[0] - VECTORS - extra
        if rest:
            vecs[VECTORS + extra :, :] = jnp.zeros((rest, width), F32)


def step_at(step, body):
    pl.when(pl.program_id(0) == step)(body)


def first_kernel(sizes, steps, chunks, mesh_sizes, *refs):
    group, seq, pad = sizes
    images, wide, down, vecs = refs[:4]
    out = refs[7]
    keep = dict(zip(KEEP, refs[8:14]))
    buf = refs[17]
    work = Gather(chunks, mesh_sizes, refs[4:6], refs[6], refs[14:16], refs[16], refs[18:])
    every = list(range(len(chunks)))
    early = every[: len(every) // 2]
    late = every[len(every) // 2 :]
    plans = [
        (0, lambda: work.begin()),
        (steps // 5, lambda: [work.to_chips(i) for i in early]),
        (2 * steps // 5, lambda: [work.to_chips(i) for i in late]),
        (3 * steps // 5, lambda: [work.to_cores(i) for i in early]),
    ]
    for step, body in plans:
        step_at(step, lambda body=body: (body(), None)[1])
    load_padded(images, buf, pad)
    out[...] = layer_forward(
        buf[...], split_weights(wide, down), vecs, keep, group, seq, pad
    )

    @pl.when(pl.program_id(0) == steps - 1)
    def _():
        for i in late:
            work.to_cores(i)
        work.finish()


def middle_kernel(sizes, *refs):
    group, seq, pad = sizes
    hidden, cotangent, wide, down, vecs, encoded, flowing = refs[:7]
    outs = refs[7:10]
    keep = dict(zip(KEEP, refs[10:16]))
    acc = refs[16:24]
    (buf,) = refs[24:]
    weights = split_weights(wide, down)
    init_grads(acc)
    result = layer_forward(hidden[...], weights, vecs, keep, group, seq, pad)
    store_images(encoded, result, pad)
    load_padded(cotangent, buf, pad)
    flowing[...] = layer_backward(buf[...], hidden[...], weights, vecs, keep, acc, group, pad)
    flush_grads(acc, outs)


def last_kernel(sizes, steps, chunks, mesh_sizes, *refs):
    group, seq, pad = sizes
    flowing, images, wide, down, vecs = refs[:5]
    keep = dict(zip(KEEP, refs[5:11]))
    images_grad = refs[14]
    outs = refs[15:18]
    acc = refs[21:29]
    buf = refs[29]
    shares = refs[30:32]
    work = Reduce(chunks, mesh_sizes, refs[11:13], refs[13], shares, refs[20], refs[32:])
    every = range(len(chunks))

    @pl.when(pl.program_id(0) == 0)
    def _():
        work.begin()

    @pl.when(pl.program_id(0) == steps // 5)
    def _():
        for i in every:
            work.to_chips(i)
        work.vec_to_chips()

    @pl.when(pl.program_id(0) == 3 * steps // 5)
    def _():
        for i in every:
            work.to_shards(i)
        work.vec_to_shards()

    @pl.when(pl.program_id(0) == 4 * steps // 5)
    def _():
        for i in every:
            work.to_spread(i)
        work.vec_end()

    init_grads(acc)
    load_padded(images, buf, pad)
    result = layer_backward(
        flowing[...], buf[...], split_weights(wide, down), vecs, keep, acc, group, pad
    )
    store_images(images_grad, result, pad)

    @pl.when(pl.program_id(0) == steps - 1)
    def _():
        for i in every:
            work.to_join(i)

    flush_grads(acc, outs)

    @pl.when(pl.program_id(0) == steps - 1)
    def _():
        work.finish()
        for share, ref in zip(shares, refs[18:20]):
            ref[...] = share[...]


def whole(shape):
    return pl.BlockSpec(shape, lambda i: (0,) * len(shape), pipeline_mode=pl.Buffered(1))


def rows_spec(shape, steps):
    return pl.BlockSpec(
        (shape[0] // steps,) + tuple(shape[1:]), lambda i: (i,) + (0,) * (len(shape) - 1)
    )


class Plan:
    def __init__(self, images_shape, hidden_width):
        self.count, self.seq, self.width = images_shape
        self.hidden_width = hidden_width
        self.pad = -(-self.seq // 16) * 16
        self.group = 2 if self.count % 2 == 0 else 1
        self.steps = self.count // self.group
        self.rows = self.count * self.pad
        self.keep = keep_shapes(self.count, self.pad, self.width, hidden_width)
        self.keep_block = keep_shapes(self.group, self.pad, self.width, hidden_width)
        self.weight_shapes = [
            (self.width, 3 * self.width),
            (self.width, self.width),
            (self.width, hidden_width),
            (hidden_width, self.width),
        ]
        self.sizes = (self.group, self.seq, self.pad)
        block_rows = self.group * self.pad
        self.buffer = pltpu.VMEM((block_rows, self.width), F32)
        self.acc = [
            pltpu.VMEM(self.weight_shapes[0], F32),
            pltpu.VMEM(self.weight_shapes[1], F32),
            pltpu.VMEM(self.weight_shapes[2], F32),
            pltpu.VMEM((self.width, hidden_width), F32),
            pltpu.VMEM((8, self.width), F32),
            pltpu.VMEM((1, hidden_width), F32),
            pltpu.VMEM((block_rows, 3 * self.width), BF16),
            pltpu.VMEM((block_rows, self.width), BF16),
        ]
        self.vec_rows = -(-(VECTORS + hidden_width // self.width) // 8) * 8
        self.packed_shapes = [
            (self.width, 4 * self.width + hidden_width),
            (hidden_width, self.width),
        ]
        self.vec_shape = (self.vec_rows, self.width)
        self.grad_shapes = [jax.ShapeDtypeStruct(s, BF16) for s in self.packed_shapes] + [
            jax.ShapeDtypeStruct(self.vec_shape, F32)
        ]
        self.params = pltpu.CompilerParams(
            dimension_semantics=("arbitrary",), vmem_limit_bytes=60 * 2**20
        )

    def image_spec(self):
        return rows_spec((self.count, self.seq, self.width), self.steps)

    def state_spec(self):
        return rows_spec((self.rows, self.width), self.steps)

    def param_specs(self):
        return [whole(s) for s in self.packed_shapes + [self.vec_shape]]

    def keep_specs(self):
        return [rows_spec(self.keep[k][0], self.steps) for k in KEEP]

    def grad_specs(self):
        return [whole(s.shape) for s in self.grad_shapes]

    def cost(self, layers):
        rows, width, hidden = self.count * self.seq, self.width, self.hidden_width
        flops = 2 * rows * width * (4 * width + 2 * hidden) * layers
        return pl.CostEstimate(
            flops=int(flops), bytes_accessed=int(40 * 2**20), transcendentals=0
        )

    def comm_params(self, collective_id):
        return pltpu.CompilerParams(
            dimension_semantics=("arbitrary",),
            vmem_limit_bytes=62 * 2**20,
            collective_id=collective_id,
            has_side_effects=True,
        )

    def first(self, images, weights, vecs, shards, mesh_sizes, collective_id):
        state = jax.ShapeDtypeStruct((self.rows, self.width), F32)
        keeps = [jax.ShapeDtypeStruct(*self.keep[k]) for k in KEEP]
        chunks = chunks_of([(s.shape[1], s.shape[3]) for s in shards[:2]], mesh_sizes[1])
        out = pl.pallas_call(
            functools.partial(first_kernel, self.sizes, self.steps, chunks, mesh_sizes),
            name="layer_first",
            out_shape=[state] + keeps + gathered_shapes(shards, mesh_sizes[0]),
            grid=(self.steps,),
            in_specs=[self.image_spec()] + self.param_specs() + [ANY_SPEC] * 3,
            out_specs=[self.state_spec()] + self.keep_specs() + [ANY_SPEC] * 3,
            scratch_shapes=[self.buffer] + Gather.semaphores(chunks, mesh_sizes),
            compiler_params=self.comm_params(collective_id),
            cost_estimate=self.cost(1),
        )(images, *weights, vecs, *shards)
        return out[0], out[1:7], out[7:]

    def middle(self, hidden, cotangent, weights, vecs):
        state = jax.ShapeDtypeStruct((self.rows, self.width), F32)
        out = pl.pallas_call(
            functools.partial(middle_kernel, self.sizes),
            name="layer_middle",
            out_shape=[jax.ShapeDtypeStruct(cotangent.shape, BF16), state] + self.grad_shapes,
            grid=(self.steps,),
            in_specs=[self.state_spec(), self.image_spec()] + self.param_specs(),
            out_specs=[self.image_spec(), self.state_spec()] + self.grad_specs(),
            scratch_shapes=[pltpu.VMEM(*self.keep_block[k]) for k in KEEP]
            + self.acc
            + [self.buffer],
            compiler_params=self.params,
            cost_estimate=self.cost(3),
        )(hidden, cotangent, *weights, vecs)
        return out[0], out[1], out[2:]

    def last(self, flowing, images, weights, vecs, keeps, grads, mesh_sizes, collective_id):
        chunks = chunks_of([(g.shape[1], g.shape[3]) for g in grads[:2]], mesh_sizes[1])
        shares = reduced_shapes(grads)
        out = pl.pallas_call(
            functools.partial(last_kernel, self.sizes, self.steps, chunks, mesh_sizes),
            name="layer_last",
            out_shape=[jax.ShapeDtypeStruct(images.shape, BF16)] + self.grad_shapes + shares,
            grid=(self.steps,),
            in_specs=[self.state_spec(), self.image_spec()]
            + self.param_specs()
            + self.keep_specs()
            + [whole(g.shape) for g in grads],
            out_specs=[self.image_spec()] + self.grad_specs() + [whole(s.shape) for s in shares],
            scratch_shapes=self.acc
            + [self.buffer]
            + [pltpu.VMEM(s.shape, s.dtype) for s in shares[:2]]
            + Reduce.scratch(chunks, mesh_sizes, grads[2].shape),
            compiler_params=self.comm_params(collective_id),
            cost_estimate=self.cost(2),
        )(flowing, images, *weights, vecs, *keeps, *grads)
        return out[0], out[1:4], out[4:]


def greet(targets):
    barrier = pltpu.get_barrier_semaphore()
    for target in targets:
        pl.semaphore_signal(
            barrier, inc=1, device_id=target, device_id_type=pl.DeviceIdType.MESH
        )
    pl.semaphore_wait(barrier, len(targets))


def transfer(src, dst, sems, at, target):
    return pltpu.make_async_remote_copy(
        src_ref=src,
        dst_ref=dst,
        send_sem=sems[0].at[at],
        recv_sem=sems[1].at[at],
        device_id=target,
        device_id_type=pl.DeviceIdType.MESH,
    )


class Chunk:
    def __init__(self, array, blocks, columns, by_columns, extent, start, chips):
        self.array, self.by_columns, self.start, self.extent = array, by_columns, start, extent
        self.blocks = blocks if by_columns else extent
        self.columns = extent if by_columns else columns
        self.stride = (columns if by_columns else blocks) // 2
        self.pieces = math.gcd(self.blocks, chips)
        self.run = self.blocks // self.pieces

    def part(self, ref, core, piece=None, shard=slice(None)):
        at = core * self.stride + self.start
        first, size = (0, self.blocks) if piece is None else (piece * self.run, self.run)
        if self.by_columns:
            columns = pl.ds(pl.multiple_of(at, 128), self.columns)
            return ref.at[shard, pl.ds(first, size), :, columns]
        return ref.at[shard, pl.ds(at + first, size)]


def chunks_of(shapes, reps):
    chips = reps // 2
    lists = []
    for array, (blocks, columns) in enumerate(shapes):
        by_columns = columns % 256 == 0
        half = columns // 2 if by_columns else blocks // 2
        unit = 128 if by_columns else 1
        want = 3 if by_columns else 2
        parts = want if half % (want * unit) == 0 else 1
        extent = half // parts
        lists.append(
            [
                Chunk(array, blocks, columns, by_columns, extent, j * extent, chips)
                for j in range(parts)
            ]
        )
    merged = []
    for j in range(max(len(part) for part in lists)):
        merged += [part[j] for part in lists if j < len(part)]
    return merged


class Place:
    def __init__(self, sizes):
        self.groups, self.reps = sizes
        self.rep, self.mine = lax.axis_index("rep"), lax.axis_index("grp")
        self.chip, self.core = self.rep // 2, lax.rem(self.rep, 2)
        self.chips = self.reps // 2
        self.shard_peers = [
            (self.rep, lax.rem(self.mine + d, self.groups)) for d in range(1, self.groups)
        ]
        self.core_peer = (self.chip * 2 + 1 - self.core, self.mine)

    def piece(self, chunk):
        return lax.rem(self.chip, chunk.pieces)

    def mate(self, chunk, step):
        piece = self.piece(chunk)
        return self.chip - piece + lax.rem(piece + step, chunk.pieces)

    def at(self, chip):
        return (chip * 2 + self.core, self.mine)


class Gather:
    def __init__(self, chunks, sizes, ins, vec_in, outs, vec_out, sems):
        self.chunks, self.place = chunks, Place(sizes)
        self.ins, self.outs, self.vec_in, self.vec_out = ins, outs, vec_in, vec_out
        self.own_sem, self.vec_own_sem = sems[:2]
        self.vec_sems, self.shard_sems, self.chip_sems, self.core_sems = (
            sems[2 + 2 * i : 4 + 2 * i] for i in range(4)
        )

    @staticmethod
    def semaphores(chunks, sizes):
        groups = sizes[0]
        most = max(c.pieces for c in chunks)
        count = len(chunks)
        return (
            [pltpu.SemaphoreType.DMA((count,)), pltpu.SemaphoreType.DMA]
            + dma_pair(groups - 1)
            + dma_pair(count, groups - 1)
            + dma_pair(count, max(most - 1, 1))
            + dma_pair(count)
        )

    def shards(self, i):
        chunk, place = self.chunks[i], self.place
        piece = place.piece(chunk)
        src = chunk.part(self.ins[chunk.array], place.core, piece, 0)
        dst = chunk.part(self.outs[chunk.array], place.core, piece, place.mine)
        return [
            transfer(src, dst, self.shard_sems, (i, d), t)
            for d, t in enumerate(place.shard_peers)
        ]

    def own(self, i):
        chunk, place = self.chunks[i], self.place
        piece = place.piece(chunk)
        src = chunk.part(self.ins[chunk.array], place.core, piece, 0)
        dst = chunk.part(self.outs[chunk.array], place.core, piece, place.mine)
        return pltpu.make_async_copy(src, dst, self.own_sem.at[i])

    def vectors(self):
        return [
            transfer(self.vec_in.at[0], self.vec_out.at[self.place.mine], self.vec_sems, d, t)
            for d, t in enumerate(self.place.shard_peers)
        ]

    def vector_own(self):
        return pltpu.make_async_copy(
            self.vec_in.at[0], self.vec_out.at[self.place.mine], self.vec_own_sem
        )

    def chips(self, i):
        chunk, place = self.chunks[i], self.place
        block = chunk.part(self.outs[chunk.array], place.core, place.piece(chunk))
        return [
            transfer(block, block, self.chip_sems, (i, e - 1), place.at(place.mate(chunk, e)))
            for e in range(1, chunk.pieces)
        ]

    def cores(self, i):
        chunk, place = self.chunks[i], self.place
        block = chunk.part(self.outs[chunk.array], place.core)
        return [transfer(block, block, self.core_sems, i, place.core_peer)]

    def begin(self):
        place = self.place
        most = max(self.chunks, key=lambda c: c.pieces)
        greet(
            place.shard_peers
            + [place.at(place.mate(most, e)) for e in range(1, most.pieces)]
            + [place.core_peer]
        )
        for i in range(len(self.chunks)):
            start(self.shards(i))
            self.own(i).start()
            if i == 0:
                start(self.vectors())
                self.vector_own().start()

    def to_chips(self, i):
        self.own(i).wait()
        arrive(self.shards(i))
        start(self.chips(i))

    def to_cores(self, i):
        arrive(self.chips(i))
        start(self.cores(i))

    def finish(self):
        every = range(len(self.chunks))
        for i in every:
            arrive(self.cores(i))
        arrive(self.vectors())
        self.vector_own().wait()
        for copy in self.vectors():
            copy.wait_send()
        for i in every:
            for copy in self.shards(i) + self.chips(i) + self.cores(i):
                copy.wait_send()


def start(copies):
    for copy in copies:
        copy.start()


def arrive(copies):
    for copy in copies:
        copy.wait_recv()


def gather_kernel(chunks, sizes, *refs):
    work = Gather(chunks, sizes, refs[:2], refs[2], refs[3:5], refs[5], refs[6:])
    work.begin()
    for i in range(len(chunks)):
        work.to_chips(i)
    for i in range(len(chunks)):
        work.to_cores(i)
    work.finish()


def dma_pair(*shape):
    return [pltpu.SemaphoreType.DMA(shape), pltpu.SemaphoreType.DMA(shape)]


VMEM_SPEC = pl.BlockSpec(memory_space=pltpu.VMEM)
ANY_SPEC = pl.BlockSpec(memory_space=pl.ANY)


def gathered_shapes(shards, groups):
    return [jax.ShapeDtypeStruct((groups,) + s.shape[1:], s.dtype) for s in shards]


def gather(shards, sizes, collective_id):
    chunks = chunks_of([(s.shape[1], s.shape[3]) for s in shards[:2]], sizes[1])
    return pl.pallas_call(
        functools.partial(gather_kernel, chunks, sizes),
        name="gather_params",
        out_shape=gathered_shapes(shards, sizes[0]),
        in_specs=[VMEM_SPEC] * 3,
        out_specs=[VMEM_SPEC] * 3,
        scratch_shapes=Gather.semaphores(chunks, sizes),
        compiler_params=pltpu.CompilerParams(
            collective_id=collective_id, has_side_effects=True, vmem_limit_bytes=40 * 2**20
        ),
    )(*shards)


def add_up(first, rest):
    total = first.astype(F32)
    for term in rest:
        total = total + term.astype(F32)
    return total


class Reduce:
    def __init__(self, chunks, sizes, ins, vec_in, outs, vec_out, scratch):
        count = len(chunks)
        self.chunks, self.place = chunks, Place(sizes)
        self.ins, self.vec_in, self.outs, self.vec_out = ins, vec_in, outs, vec_out
        self.from_core, self.core_sum, self.from_chips, self.chip_sum, self.from_shards = (
            scratch[i * count : (i + 1) * count] for i in range(5)
        )
        self.vec_parts, self.vec_held = scratch[5 * count : 5 * count + 2]
        sems = scratch[5 * count + 2 :]
        (
            self.core_sems,
            self.chip_sems,
            self.shard_sems,
            self.spread_sems,
            self.join_sems,
            self.vec_sems,
        ) = (sems[2 * i : 2 * i + 2] for i in range(6))

    @staticmethod
    def scratch(chunks, sizes, vec_shape):
        groups, reps = sizes
        chips, count = reps // 2, len(chunks)
        most = max(c.pieces for c in chunks)
        half = [(groups, c.blocks, 8, c.columns) for c in chunks]
        piece = [(groups, c.run, 8, c.columns) for c in chunks]
        shapes = (
            half
            + half
            + [(chips - 1,) + p for p in piece]
            + piece
            + [(groups - 1,) + p[1:] for p in piece]
        )
        terms = chips + groups - 1
        return (
            [pltpu.VMEM(s, BF16) for s in shapes]
            + [pltpu.VMEM((terms,) + vec_shape, F32), pltpu.VMEM((2,) + vec_shape, F32)]
            + dma_pair(count)
            + dma_pair(count, chips - 1)
            + dma_pair(count, groups - 1)
            + dma_pair(count, max(most - 1, 1))
            + dma_pair(count)
            + dma_pair(terms)
        )

    def chip_ids(self):
        place = self.place
        return [lax.rem(place.chip + e, place.chips) for e in range(1, place.chips)]

    def cores(self, i):
        chunk, place = self.chunks[i], self.place
        src = chunk.part(self.ins[chunk.array], 1 - place.core)
        return [transfer(src, self.from_core[i], self.core_sems, i, place.core_peer)]

    def chips(self, i):
        chunk, copies = self.chunks[i], []
        for e, chip in enumerate(self.chip_ids()):
            piece = lax.rem(chip, chunk.pieces)
            src = self.core_sum[i].at[:, pl.ds(piece * chunk.run, chunk.run)]
            dst = self.from_chips[i].at[e]
            copies.append(transfer(src, dst, self.chip_sems, (i, e), self.place.at(chip)))
        return copies

    def shards(self, i):
        place = self.place
        return [
            transfer(
                self.chip_sum[i].at[lax.rem(place.mine + d + 1, place.groups)],
                self.from_shards[i].at[d],
                self.shard_sems,
                (i, d),
                target,
            )
            for d, target in enumerate(place.shard_peers)
        ]

    def spread(self, i):
        chunk, place = self.chunks[i], self.place
        block = chunk.part(self.outs[chunk.array], place.core, place.piece(chunk), 0)
        return [
            transfer(block, block, self.spread_sems, (i, e - 1), place.at(place.mate(chunk, e)))
            for e in range(1, chunk.pieces)
        ]

    def join(self, i):
        chunk, place = self.chunks[i], self.place
        block = chunk.part(self.outs[chunk.array], place.core, None, 0)
        return [transfer(block, block, self.join_sems, i, place.core_peer)]

    def vec_cores(self):
        return [transfer(self.vec_in, self.vec_parts.at[0], self.vec_sems, 0, self.place.core_peer)]

    def vec_chips(self):
        return [
            transfer(
                self.vec_held.at[0],
                self.vec_parts.at[1 + e],
                self.vec_sems,
                1 + e,
                self.place.at(chip),
            )
            for e, chip in enumerate(self.chip_ids())
        ]

    def vec_shards(self):
        chips = self.place.chips
        return [
            transfer(
                self.vec_held.at[1],
                self.vec_parts.at[chips + d],
                self.vec_sems,
                chips + d,
                target,
            )
            for d, target in enumerate(self.place.shard_peers)
        ]

    def begin(self):
        place = self.place
        greet(
            place.shard_peers + [place.at(c) for c in self.chip_ids()] + [place.core_peer]
        )
        for i in range(len(self.chunks)):
            start(self.cores(i))
        start(self.vec_cores())

    def to_chips(self, i):
        chunk = self.chunks[i]
        own = chunk.part(self.ins[chunk.array], self.place.core)[...]
        arrive(self.cores(i))
        self.core_sum[i][...] = add_up(own, [self.from_core[i][...]]).astype(BF16)
        start(self.chips(i))

    def vec_to_chips(self):
        arrive(self.vec_cores())
        self.vec_held[0] = self.vec_in[...] + self.vec_parts[0]
        start(self.vec_chips())

    def to_shards(self, i):
        chunk = self.chunks[i]
        piece = self.place.piece(chunk)
        own = self.core_sum[i][:, pl.ds(piece * chunk.run, chunk.run)]
        copies = self.chips(i)
        arrive(copies)
        total = add_up(own, [self.from_chips[i][e] for e in range(len(copies))])
        self.chip_sum[i][...] = total.astype(BF16)
        start(self.shards(i))

    def vec_to_shards(self):
        copies = self.vec_chips()
        arrive(copies)
        self.vec_held[1] = add_up(
            self.vec_held[0], [self.vec_parts[1 + e] for e in range(len(copies))]
        )
        start(self.vec_shards())

    def to_spread(self, i):
        chunk, place = self.chunks[i], self.place
        copies = self.shards(i)
        arrive(copies)
        total = add_up(
            self.chip_sum[i][place.mine], [self.from_shards[i][d] for d in range(len(copies))]
        )
        block = chunk.part(self.outs[chunk.array], place.core, place.piece(chunk), 0)
        block[...] = total.astype(BF16)
        start(self.spread(i))

    def vec_end(self):
        copies = self.vec_shards()
        arrive(copies)
        self.vec_out[...] = add_up(
            self.vec_held[1], [self.vec_parts[self.place.chips + d] for d in range(len(copies))]
        )

    def to_join(self, i):
        arrive(self.spread(i))
        start(self.join(i))

    def finish(self):
        every = range(len(self.chunks))
        for i in every:
            arrive(self.join(i))
        copies = self.vec_cores() + self.vec_chips() + self.vec_shards()
        for i in every:
            copies += self.cores(i) + self.chips(i) + self.shards(i)
            copies += self.spread(i) + self.join(i)
        for copy in copies:
            copy.wait_send()


def reduce_kernel(chunks, sizes, *refs):
    work = Reduce(chunks, sizes, refs[:2], refs[2], refs[3:5], refs[5], refs[6:])
    count = len(chunks)
    work.begin()
    for i in range(count):
        work.to_chips(i)
    work.vec_to_chips()
    for i in range(count):
        work.to_shards(i)
        if i == 0:
            work.vec_to_shards()
        if i > 0:
            work.to_spread(i - 1)
        if i > 1:
            work.to_join(i - 2)
    work.to_spread(count - 1)
    work.vec_end()
    for i in range(max(count - 2, 0), count):
        work.to_join(i)
    work.finish()


def reduced_shapes(grads):
    return [jax.ShapeDtypeStruct((1,) + g.shape[1:], BF16) for g in grads[:2]] + [
        jax.ShapeDtypeStruct(grads[2].shape, F32)
    ]


def reduce_grads(grads, sizes, collective_id):
    chunks = chunks_of([(g.shape[1], g.shape[3]) for g in grads[:2]], sizes[1])
    return pl.pallas_call(
        functools.partial(reduce_kernel, chunks, sizes),
        name="reduce_grads",
        out_shape=reduced_shapes(grads),
        in_specs=[VMEM_SPEC] * 3,
        out_specs=[VMEM_SPEC] * 3,
        scratch_shapes=Reduce.scratch(chunks, sizes, grads[2].shape),
        compiler_params=pltpu.CompilerParams(
            collective_id=collective_id, has_side_effects=True, vmem_limit_bytes=40 * 2**20
        ),
    )(*grads)


def on_device(
    reps,
    images,
    cotangent,
    ln1_gain,
    ln1_bias,
    w_qkv,
    q_bias,
    v_bias,
    w_proj,
    proj_bias,
    ln2_gain,
    ln2_bias,
    w_up,
    up_bias,
    w_down,
    down_bias,
):
    groups = lax.axis_size("grp")
    sizes = (groups, reps)
    layers, part = ln1_gain.shape
    width = part * groups
    hidden_part = up_bias.shape[1]
    plan = Plan(images.shape, hidden_part * groups)
    vectors = [ln1_gain, ln1_bias, q_bias, v_bias, proj_bias, ln2_gain, ln2_bias, down_bias]
    extra = hidden_part // part
    packed = jnp.stack(vectors, axis=1)
    packed = jnp.concatenate([packed, up_bias.reshape(layers, extra, part)], axis=1)
    packed = packed.astype(F32)
    wide = jnp.concatenate([w_qkv, w_proj, w_up], axis=2)

    def shards_of(layer):
        return [
            wide[layer].reshape(1, -1, 8, wide.shape[2]),
            w_down[layer].reshape(1, -1, 8, width),
            packed[layer][None],
        ]

    def unpack(gathered):
        big, down, vecs = gathered
        vectors = vecs[:, :VECTORS].transpose(1, 0, 2).reshape(VECTORS, width)
        up = vecs[:, VECTORS:].reshape(extra, width)
        rest = plan.vec_rows - VECTORS - extra
        vecs = jnp.concatenate([vectors, up, jnp.zeros((rest, width), F32)], axis=0)
        return [big.reshape(width, -1), down.reshape(-1, width)], vecs

    def blocks_of(grads):
        return [
            grads[0].reshape(groups, -1, 8, grads[0].shape[1]),
            grads[1].reshape(groups, -1, 8, width),
            grads[2],
        ]

    weights0, vecs0 = unpack(gather(shards_of(0), sizes, 0))
    hidden, keeps, gathered = plan.first(images, weights0, vecs0, shards_of(1), sizes, 1)
    weights1, vecs1 = unpack(gathered)
    encoded, flowing, grads1 = plan.middle(hidden, cotangent, weights1, vecs1)
    images_grad, grads0, reduced1 = plan.last(
        flowing, images, weights0, vecs0, keeps, blocks_of(grads1), sizes, 2
    )
    reduced0 = reduce_grads(blocks_of(grads0), sizes, 3)
    small0, small1 = reduced0[2], reduced1[2]
    shares0, shares1 = (
        [s.reshape(-1, s.shape[3]) for s in reduced[:2]] for reduced in (reduced0, reduced1)
    )
    small = jnp.stack([small0, small1])
    me = lax.axis_index("grp")
    vec_out = lax.dynamic_slice_in_dim(small[:, :VECTORS], me * part, part, axis=2)
    up_out = small[:, VECTORS : VECTORS + extra].reshape(layers, -1)
    up_out = lax.dynamic_slice_in_dim(up_out, me * hidden_part, hidden_part, axis=1)
    full = [jnp.stack([a, b]).astype(F32) for a, b in zip(shares0, shares1)]
    columns = w_qkv.shape[2], w_qkv.shape[2] + width
    return (
        encoded,
        images_grad,
        vec_out[:, G1],
        vec_out[:, B1],
        full[0][:, :, : columns[0]],
        vec_out[:, QB],
        vec_out[:, VB],
        full[0][:, :, columns[0] : columns[1]],
        vec_out[:, PB],
        vec_out[:, G2],
        vec_out[:, B2],
        full[0][:, :, columns[1] :],
        up_out,
        full[1],
        vec_out[:, DB],
    )


def solution(mesh):
    batch = P(("rep", "grp"), None, None)
    vector = P(None, "grp")
    matrix = P(None, "grp", None)
    params = (
        vector,
        vector,
        matrix,
        vector,
        vector,
        matrix,
        vector,
        vector,
        vector,
        matrix,
        vector,
        matrix,
        vector,
    )
    specs = (batch, batch) + params
    return jax.shard_map(
        functools.partial(on_device, mesh.shape["rep"]), mesh=mesh, in_specs=specs, out_specs=specs, check_vma=False
    )
```

```python
import functools
import math

import jax
import jax.numpy as jnp
from jax import lax
from jax.experimental import pallas as pl
from jax.experimental.pallas import tpu as pltpu
from jax.sharding import PartitionSpec as P

HEAD_DIM = 64
PAIR = 2 * HEAD_DIM
EPS = 1e-06
INV_ROOT_TWO = 0.7071067811865476
INV_ROOT_TAU = 0.3989422804014327
MASKED = -1e30
F32 = jnp.float32
BF16 = jnp.bfloat16

VECTORS = 8
G1, B1, QB, VB, PB, G2, B2, DB = range(VECTORS)


def dot(left, right):
    return jnp.dot(left, right, preferred_element_type=F32)


def dot_nt(left, right):
    return lax.dot_general(
        left, right, (((1,), (1,)), ((), ())), preferred_element_type=F32
    )


def col_sum(rows):
    return jnp.sum(rows, axis=0, keepdims=True)


def norm(rows):
    mean = jnp.mean(rows, axis=-1, keepdims=True)
    centered = rows - mean
    inv = lax.rsqrt(jnp.mean(centered * centered, axis=-1, keepdims=True) + EPS)
    return centered * inv, inv


def norm_backward(grad, normed, inv, gain):
    scaled = grad * gain
    return inv * (
        scaled
        - jnp.mean(scaled, axis=-1, keepdims=True)
        - normed * jnp.mean(scaled * normed, axis=-1, keepdims=True)
    )


def attn_forward(qkv, keep, image, seq, pad):
    width = qkv.shape[1] // 3
    base = image * pad
    rows = pl.ds(base, pad)
    value_t = qkv[rows, pl.ds(2 * width, width)].T
    lane = lax.broadcasted_iota(jnp.int32, (1, PAIR), 1)
    halves = [(lane < HEAD_DIM).astype(F32).astype(BF16), (lane >= HEAD_DIM).astype(F32).astype(BF16)]
    full = seq // 8 * 8
    for pair in range(width // PAIR):
        queries = qkv[rows, pl.ds(pair * PAIR, PAIR)]
        keys = qkv[rows, pl.ds(width + pair * PAIR, PAIR)]
        for half in range(2):
            head = 2 * pair + half
            scores = dot_nt(keys * halves[half], queries)
            parts = [scores[:full]]
            if full < seq:
                tail = scores[full : full + 8]
                row = lax.broadcasted_iota(jnp.int32, tail.shape, 0)
                parts.append(jnp.where(row < seq - full, tail, MASKED))
            scores = jnp.concatenate(parts, axis=0)
            top = jnp.max(scores, axis=0, keepdims=True)
            raised = jnp.exp(scores - top)
            probs = raised * (1.0 / col_sum(raised))
            rest = pad - probs.shape[0]
            if rest:
                probs = jnp.concatenate([probs, jnp.zeros((rest, pad), F32)], axis=0)
            keep["probs"][image, head] = probs
            context = dot(value_t[head * HEAD_DIM : (head + 1) * HEAD_DIM], probs.astype(BF16))
            keep["context"][image, pl.ds(head * HEAD_DIM, HEAD_DIM), :] = context.astype(BF16)


def split_attention(packed):
    width = packed.shape[0]
    return packed.at[:, pl.ds(0, 3 * width)], packed.at[:, pl.ds(3 * width, width)]


def up_bias_of(vecs, hidden_width):
    rows = hidden_width // vecs.shape[1]
    return jnp.concatenate([vecs[VECTORS + i : VECTORS + i + 1] for i in range(rows)], axis=1)


def attention_part(hidden, packed, vecs, keep, images, seq, pad):
    w_qkv, w_proj = split_attention(packed)
    width = hidden.shape[1]
    normed, _ = norm(hidden)
    rows_in = (normed * vecs[G1 : G1 + 1] + vecs[B1 : B1 + 1]).astype(BF16)
    qkv = keep["qkv"]
    projected = dot(rows_in, w_qkv[...])
    qkv[:, :width] = (projected[:, :width] + vecs[QB : QB + 1]).astype(BF16) * jnp.asarray(
        HEAD_DIM**-0.5, BF16
    )
    qkv[:, width : 2 * width] = projected[:, width : 2 * width].astype(BF16)
    qkv[:, 2 * width :] = (projected[:, 2 * width :] + vecs[VB : VB + 1]).astype(BF16)
    for image in range(images):
        attn_forward(qkv, keep, image, seq, pad)
    context = jnp.concatenate([keep["context"][image].T for image in range(images)], axis=0)
    mixed = hidden + dot(context, w_proj[...]) + vecs[PB : PB + 1]
    keep["mixed"][...] = mixed
    return mixed


def mlp_part(mixed, w_up, w_down, vecs, keep):
    up_bias = up_bias_of(vecs, w_down.shape[0])
    normed, _ = norm(mixed)
    rows_mid = (normed * vecs[G2 : G2 + 1] + vecs[B2 : B2 + 1]).astype(BF16)
    upward = dot(rows_mid, w_up[...]) + up_bias
    cumul = 0.5 * (1.0 + lax.erf(upward * INV_ROOT_TWO))
    keep["active"][...] = (upward * cumul).astype(BF16)
    slope = cumul + upward * jnp.exp(-0.5 * upward * upward) * INV_ROOT_TAU
    keep["slope"][...] = slope.astype(keep["slope"].dtype)
    return mixed + dot(keep["active"][...], w_down[...]) + vecs[DB : DB + 1]


def attn_backward(qkv, keep, context_grad, joint, vec_grads, image, pad):
    width = qkv.shape[1] // 3
    rows = pl.ds(image * pad, pad)
    keys_t = qkv[rows, pl.ds(width, width)].T
    lane = lax.broadcasted_iota(jnp.int32, (1, PAIR), 1)
    low = lax.broadcasted_iota(jnp.int32, (pad, PAIR), 1) < HEAD_DIM
    halves = [(lane < HEAD_DIM).astype(F32).astype(BF16), (lane >= HEAD_DIM).astype(F32).astype(BF16)]
    query_parts = []
    for pair in range(width // PAIR):
        queries = qkv[rows, pl.ds(pair * PAIR, PAIR)]
        values = qkv[rows, pl.ds(2 * width + pair * PAIR, PAIR)]
        ctx = context_grad[rows, pl.ds(pair * PAIR, PAIR)]
        key_parts, value_parts = [], []
        for half in range(2):
            head = 2 * pair + half
            probs = keep["probs"][image, head]
            prob_grad = dot_nt(values * halves[half], ctx)
            value_parts.append(dot(probs.astype(BF16), ctx))
            row_dot = col_sum(probs * prob_grad)
            score_grad = (probs * (prob_grad - row_dot)).astype(BF16)
            key_parts.append(dot(score_grad, queries))
            query_parts.append(dot(keys_t[head * HEAD_DIM : (head + 1) * HEAD_DIM], score_grad))
        key_grad = jnp.where(low, key_parts[0], key_parts[1])
        value_grad = jnp.where(low, value_parts[0], value_parts[1])
        joint[rows, pl.ds(width + pair * PAIR, PAIR)] = key_grad.astype(BF16)
        joint[rows, pl.ds(2 * width + pair * PAIR, PAIR)] = value_grad.astype(BF16)
        vec_grads[VB : VB + 1, pl.ds(pair * PAIR, PAIR)] += col_sum(value_grad)
    query_grad = jnp.concatenate(query_parts, axis=0).T * HEAD_DIM**-0.5
    joint[rows, pl.ds(0, width)] = query_grad.astype(BF16)
    vec_grads[QB : QB + 1, :] += col_sum(query_grad)


def mlp_backward(out_grad, w_up, w_down, vecs, keep, acc):
    _, _, g_up, g_down, vec_grads, up_bias_grad = acc[:6]
    rounded = out_grad.astype(BF16)
    vec_grads[DB : DB + 1, :] += col_sum(out_grad)
    g_down[...] += dot(rounded.T, keep["active"][...])
    up_grad = dot_nt(rounded, w_down[...]) * keep["slope"][...].astype(F32)
    up_bias_grad[...] += col_sum(up_grad)
    up_rounded = up_grad.astype(BF16)
    normed, inv = norm(keep["mixed"][...])
    gain = vecs[G2 : G2 + 1]
    rows_mid = (normed * gain + vecs[B2 : B2 + 1]).astype(BF16)
    g_up[...] += dot(rows_mid.T, up_rounded)
    mid_grad = dot_nt(up_rounded, w_up[...])
    vec_grads[G2 : G2 + 1, :] += col_sum(mid_grad * normed)
    vec_grads[B2 : B2 + 1, :] += col_sum(mid_grad)
    return out_grad + norm_backward(mid_grad, normed, inv, gain)


def attention_backward(mixed_grad, hidden, packed, vecs, keep, acc, images, pad):
    w_qkv, w_proj = split_attention(packed)
    g_qkv, g_proj, _, _, vec_grads, _, joint, context_grad = acc
    vec_grads[PB : PB + 1, :] += col_sum(mixed_grad)
    mixed_rounded = mixed_grad.astype(BF16)
    part = g_proj[...]
    for image in range(images):
        part += dot(keep["context"][image], mixed_rounded[image * pad : (image + 1) * pad])
    g_proj[...] = part
    context_grad[...] = dot_nt(mixed_rounded, w_proj[...]).astype(BF16)
    for image in range(images):
        attn_backward(keep["qkv"], keep, context_grad, joint, vec_grads, image, pad)
    normed, inv = norm(hidden)
    gain = vecs[G1 : G1 + 1]
    rows_in = (normed * gain + vecs[B1 : B1 + 1]).astype(BF16)
    g_qkv[...] += dot(rows_in.T, joint[...])
    in_grad = dot_nt(joint[...], w_qkv[...])
    vec_grads[G1 : G1 + 1, :] += col_sum(in_grad * normed)
    vec_grads[B1 : B1 + 1, :] += col_sum(in_grad)
    return mixed_grad + norm_backward(in_grad, normed, inv, gain)


def load_padded(ref, buf, pad):
    images, seq, width = ref.shape
    for image in range(images):
        buf[pl.ds(image * pad, seq), :] = ref[image].astype(F32)
        if pad > seq:
            buf[pl.ds(image * pad + seq, pad - seq), :] = jnp.zeros((pad - seq, width), F32)


def store_images(ref, rows, pad):
    images, seq, _ = ref.shape
    for image in range(images):
        ref[image] = rows[image * pad : image * pad + seq].astype(ref.dtype)


KEEP = ("qkv", "probs", "context", "mixed", "active", "slope")


def keep_shapes(images, pad, width, hidden_width):
    heads = width // HEAD_DIM
    return {
        "qkv": ((images * pad, 3 * width), BF16),
        "probs": ((images, heads, pad, pad), F32),
        "context": ((images, width, pad), BF16),
        "mixed": ((images * pad, width), F32),
        "active": ((images * pad, hidden_width), BF16),
        "slope": ((images * pad, hidden_width), F32),
    }


def init_grads(acc):
    @pl.when(pl.program_id(0) == 0)
    def _():
        for ref in acc[:6]:
            ref[...] = jnp.zeros_like(ref)


def flush_vectors(acc, vecs):
    vec_grads, up_bias_grad = acc[4:6]
    width = vecs.shape[1]
    extra = up_bias_grad.shape[1] // width
    vecs[:VECTORS, :] = vec_grads[...]
    for i in range(extra):
        vecs[VECTORS + i : VECTORS + i + 1, :] = up_bias_grad[:, i * width : (i + 1) * width]
    rest = vecs.shape[0] - VECTORS - extra
    if rest:
        vecs[VECTORS + extra :, :] = jnp.zeros((rest, width), F32)


def step_at(step):
    return pl.when(pl.program_id(0) == step)


def first_kernel(sizes, steps, mesh_sizes, chunks, *refs):
    group, seq, pad = sizes
    images, packed, vecs = refs[:3]
    shards0, shards1 = refs[3:5], refs[5:9]
    out = refs[9]
    keep = dict(zip(KEEP, refs[10:16]))
    mlp_out = refs[16:18]
    full1 = refs[18:22]
    buf, mixed_rows = refs[22:24]
    landed = refs[24:26]
    rest = refs[26:]
    half = len(rest) // 2
    now = Gather(chunks[0], mesh_sizes, shards0, None, landed, None, rest[:half])
    later = Gather(
        chunks[1], mesh_sizes, shards1[:3], shards1[3], full1[:3], full1[3], rest[half:]
    )
    step = pl.program_id(0)
    rows = group * pad

    @step_at(0)
    def _():
        now.greet()
        now.begin()
        later.begin()

    @step_at(2 * steps // 5)
    def _():
        now.all_to_chips()

    @step_at(4 * steps // 5)
    def _():
        later.all_to_chips()

    @pl.when(step < steps)
    def _():
        load_padded(images, buf, pad)
        mixed = attention_part(buf[...], packed, vecs, keep, group, seq, pad)
        mixed_rows[pl.ds(pl.multiple_of(step * rows, rows), rows), :] = mixed

    @step_at(steps)
    def _():
        now.all_to_cores()
        now.finish()
        for matrix, source in zip(mlp_out, landed):
            flat = source[...].astype(F32).reshape(matrix.shape)
            matrix[...] = flat.astype(BF16)

    @step_at(2 * steps - 1)
    def _():
        later.all_to_cores()

    @pl.when(step >= steps)
    def _():
        at = pl.multiple_of((step - steps) * rows, rows)
        mixed = mixed_rows[pl.ds(at, rows), :]
        out[...] = mlp_part(mixed, mlp_out[0], mlp_out[1], vecs, keep)

    @step_at(2 * steps - 1)
    def _():
        later.finish()


def middle_kernel(sizes, *refs):
    group, seq, pad = sizes
    hidden, cotangent, packed, w_up, w_down, vecs, encoded, flowing = refs[:8]
    outs, vec_out = refs[8:11], refs[11]
    keep = dict(zip(KEEP, refs[12:18]))
    acc = refs[18:26]
    (buf,) = refs[26:]
    init_grads(acc)
    mixed = attention_part(hidden[...], packed, vecs, keep, group, seq, pad)
    result = mlp_part(mixed, w_up, w_down, vecs, keep)
    store_images(encoded, result, pad)
    load_padded(cotangent, buf, pad)
    mixed_grad = mlp_backward(buf[...], w_up, w_down, vecs, keep, acc)
    flowing[...] = attention_backward(
        mixed_grad, hidden[...], packed, vecs, keep, acc, group, pad
    )

    @step_at(pl.num_programs(0) - 1)
    def _():
        g_qkv_out, g_proj_out = split_attention(outs[0])
        g_qkv_out[...] = acc[0][...].astype(BF16)
        g_proj_out[...] = acc[1][...].astype(BF16)
        outs[1][...] = acc[2][...].astype(BF16)
        outs[2][...] = acc[3][...].astype(BF16).T
        flush_vectors(acc, vec_out)


def last_kernel(sizes, steps, mesh_sizes, chunks, counts, *refs):
    group, seq, pad = sizes
    flowing, images, packed, w_up, w_down, vecs = refs[:6]
    keep = dict(zip(KEEP, refs[6:12]))
    grads1, vec1 = refs[12:15], refs[15]
    images_grad, sums, vec_out0, vec_out1 = refs[16], refs[17:20], refs[20], refs[21]
    acc = refs[22:30]
    buf, grad_rows, vec0 = refs[30:33]
    grads0, shares0, shares1 = refs[33:36], refs[36:39], refs[39:42]
    scratch = refs[42:]
    ends = [sum(counts[: i + 1]) for i in range(3)]
    later = Reduce(chunks[0], mesh_sizes, grads1, vec1, shares1, vec_out1, scratch[: ends[0]])
    mlp = Reduce(
        chunks[1], mesh_sizes, grads0[1:], None, shares0[1:], None, scratch[ends[0] : ends[1]]
    )
    tail = Reduce(
        chunks[2], mesh_sizes, grads0[:1], vec0, shares0[:1], vec_out0, scratch[ends[1] :]
    )
    step = pl.program_id(0)
    rows = group * pad
    last = 2 * steps - 1

    @step_at(0)
    def _():
        later.greet()
        later.begin()

    @step_at(1 * steps // 5)
    def _():
        later.all_to_chips()

    init_grads(acc)

    @pl.when(step < steps)
    def _():
        mixed_grad = mlp_backward(flowing[...], w_up, w_down, vecs, keep, acc)
        grad_rows[pl.ds(pl.multiple_of(step * rows, rows), rows), :] = mixed_grad

    @step_at(steps)
    def _():
        grads0[1][...] = acc[2][...].reshape(grads0[1].shape).astype(BF16)
        grads0[2][...] = acc[3][...].T.reshape(grads0[2].shape).astype(BF16)
        mlp.begin()

    @step_at(steps + 1 * steps // 5)
    def _():
        later.all_to_shards()
        mlp.all_to_chips()

    @step_at(steps + 3 * steps // 5)
    def _():
        later.all_to_spread()
        mlp.all_to_shards()

    @step_at(last)
    def _():
        later.all_to_join()

    @pl.when(step >= steps)
    def _():
        load_padded(images, buf, pad)
        at = pl.multiple_of((step - steps) * rows, rows)
        result = attention_backward(
            grad_rows[pl.ds(at, rows), :], buf[...], packed, vecs, keep, acc, group, pad
        )
        store_images(images_grad, result, pad)

    @step_at(last)
    def _():
        shape = grads0[0].shape
        three = acc[0].shape[1]
        grads0[0][:, :, :, :three] = acc[0][...].reshape(shape[:3] + (three,)).astype(BF16)
        grads0[0][:, :, :, three:] = (
            acc[1][...].reshape(shape[:3] + (shape[3] - three,)).astype(BF16)
        )
        flush_vectors(acc, vec0)
        tail.begin()
        mlp.all_to_spread()
        tail.all_to_chips()
        later.finish()
        for total, share in zip(sums, shares1):
            total[1] = share[0].astype(F32)
        tail.all_to_shards()
        mlp.all_to_join()
        tail.all_to_spread()
        mlp.finish()
        for total, share in zip(sums[1:], shares0[1:]):
            total[0] = share[0].astype(F32)
        tail.all_to_join()
        tail.finish()
        sums[0][0] = shares0[0][0].astype(F32)


def whole(shape):
    return pl.BlockSpec(shape, lambda i: (0,) * len(shape), pipeline_mode=pl.Buffered(1))


def rows_spec(shape, steps, start=0):
    return pl.BlockSpec(
        (shape[0] // steps,) + tuple(shape[1:]),
        lambda i: (jnp.clip(i - start, 0, steps - 1),) + (0,) * (len(shape) - 1),
    )


class Plan:
    def __init__(self, images_shape, hidden_width):
        self.count, self.seq, self.width = images_shape
        self.hidden_width = hidden_width
        self.pad = -(-self.seq // 16) * 16
        self.group = 2 if self.count % 2 == 0 else 1
        self.steps = self.count // self.group
        self.rows = self.count * self.pad
        self.keep = keep_shapes(self.count, self.pad, self.width, hidden_width)
        self.keep_block = keep_shapes(self.group, self.pad, self.width, hidden_width)
        self.weight_shapes = [
            (self.width, 3 * self.width),
            (self.width, self.width),
            (self.width, hidden_width),
            (hidden_width, self.width),
        ]
        self.sizes = (self.group, self.seq, self.pad)
        block_rows = self.group * self.pad
        self.buffer = pltpu.VMEM((block_rows, self.width), F32)
        self.acc = [
            pltpu.VMEM(self.weight_shapes[0], F32),
            pltpu.VMEM(self.weight_shapes[1], F32),
            pltpu.VMEM(self.weight_shapes[2], F32),
            pltpu.VMEM((self.width, hidden_width), F32),
            pltpu.VMEM((8, self.width), F32),
            pltpu.VMEM((1, hidden_width), F32),
            pltpu.VMEM((block_rows, 3 * self.width), BF16),
            pltpu.VMEM((block_rows, self.width), BF16),
        ]
        self.vec_rows = -(-(VECTORS + hidden_width // self.width) // 8) * 8
        self.packed_shapes = [
            (self.width, 4 * self.width),
            (self.width, hidden_width),
            (hidden_width, self.width),
        ]
        self.vec_shape = (self.vec_rows, self.width)
        self.grad_shapes = [jax.ShapeDtypeStruct(s, BF16) for s in self.packed_shapes] + [
            jax.ShapeDtypeStruct(self.vec_shape, F32)
        ]
        self.params = pltpu.CompilerParams(
            dimension_semantics=("arbitrary",), vmem_limit_bytes=60 * 2**20
        )

    def image_spec(self, start=0):
        return rows_spec((self.count, self.seq, self.width), self.steps, start)

    def state_spec(self, start=0):
        return rows_spec((self.rows, self.width), self.steps, start)

    def param_specs(self):
        return [whole(s) for s in self.packed_shapes + [self.vec_shape]]

    def keep_specs(self, starts):
        return [rows_spec(self.keep[k][0], self.steps, at) for k, at in zip(KEEP, starts)]

    def grad_specs(self):
        return [whole(s.shape) for s in self.grad_shapes]

    def cost(self, layers):
        rows, width, hidden = self.count * self.seq, self.width, self.hidden_width
        flops = 2 * rows * width * (4 * width + 2 * hidden) * layers
        return pl.CostEstimate(
            flops=int(flops), bytes_accessed=int(40 * 2**20), transcendentals=0
        )

    def comm_params(self, collective_id):
        return pltpu.CompilerParams(
            dimension_semantics=("arbitrary",),
            vmem_limit_bytes=62 * 2**20,
            collective_id=collective_id,
            has_side_effects=True,
        )

    def first(self, images, packed, vecs, shards0, shards1, mesh_sizes, collective_id):
        state = jax.ShapeDtypeStruct((self.rows, self.width), F32)
        keeps = [jax.ShapeDtypeStruct(*self.keep[k]) for k in KEEP]
        mlp = [jax.ShapeDtypeStruct(s, BF16) for s in self.packed_shapes[1:]]
        chunks = [chunks_of(shards0, mesh_sizes), chunks_of(shards1[:3], mesh_sizes)]
        n = self.steps
        out = pl.pallas_call(
            functools.partial(first_kernel, self.sizes, n, mesh_sizes, chunks),
            name="layer_first",
            out_shape=[state] + keeps + mlp + gathered_shapes(shards1, mesh_sizes[0]),
            grid=(2 * n,),
            in_specs=[self.image_spec(), whole(packed.shape), whole(self.vec_shape)]
            + [ANY_SPEC] * 6,
            out_specs=[self.state_spec(n)]
            + self.keep_specs((0, 0, 0, 0, n, n))
            + [whole(m.shape) for m in mlp]
            + [ANY_SPEC] * 4,
            scratch_shapes=[self.buffer, pltpu.VMEM((self.rows, self.width), F32)]
            + [pltpu.VMEM(s.shape, BF16) for s in gathered_shapes(shards0, mesh_sizes[0])]
            + Gather.semaphores(chunks[0], mesh_sizes)
            + Gather.semaphores(chunks[1], mesh_sizes),
            compiler_params=self.comm_params(collective_id),
            cost_estimate=self.cost(1),
        )(images, packed, vecs, *shards0, *shards1)
        return out[0], out[1:7], out[7:9], out[9:]

    def middle(self, hidden, cotangent, weights, vecs):
        state = jax.ShapeDtypeStruct((self.rows, self.width), F32)
        out = pl.pallas_call(
            functools.partial(middle_kernel, self.sizes),
            name="layer_middle",
            out_shape=[jax.ShapeDtypeStruct(cotangent.shape, BF16), state] + self.grad_shapes,
            grid=(self.steps,),
            in_specs=[self.state_spec(), self.image_spec()] + self.param_specs(),
            out_specs=[self.image_spec(), self.state_spec()] + self.grad_specs(),
            scratch_shapes=[pltpu.VMEM(*self.keep_block[k]) for k in KEEP]
            + self.acc
            + [self.buffer],
            compiler_params=self.params,
            cost_estimate=self.cost(3),
        )(hidden, cotangent, *weights, vecs)
        return out[0], out[1], out[2:]

    def last(self, flowing, images, weights, vecs, keeps, grads, mesh_sizes, collective_id):
        groups = mesh_sizes[0]
        whole_grads = [
            jax.ShapeDtypeStruct(g.shape, BF16) for g in grads[:3]
        ]
        chunks = [
            chunks_of(whole_grads, mesh_sizes),
            chunks_of(whole_grads[1:], mesh_sizes),
            chunks_of(whole_grads[:1], mesh_sizes, 2),
        ]
        shares = [(1,) + g.shape[1:] for g in whole_grads]
        sums = [jax.ShapeDtypeStruct((2,) + g.shape[1:], F32) for g in whole_grads]
        vec = jax.ShapeDtypeStruct(self.vec_shape, F32)
        scratch = [
            Reduce.scratch(chunks[0], mesh_sizes, self.vec_shape),
            Reduce.scratch(chunks[1], mesh_sizes, None),
            Reduce.scratch(chunks[2], mesh_sizes, self.vec_shape),
        ]
        n = self.steps
        outs = [jax.ShapeDtypeStruct(images.shape, BF16)] + sums + [vec, vec]
        out = pl.pallas_call(
            functools.partial(
                last_kernel, self.sizes, n, mesh_sizes, chunks, [len(x) for x in scratch]
            ),
            name="layer_last",
            out_shape=outs,
            grid=(2 * n,),
            in_specs=[self.state_spec(), self.image_spec(n)]
            + self.param_specs()
            + self.keep_specs((n, n, n, 0, 0, 0))
            + [whole(g.shape) for g in grads],
            out_specs=[self.image_spec(n)] + [whole(o.shape) for o in outs[1:]],
            scratch_shapes=self.acc
            + [
                self.buffer,
                pltpu.VMEM((self.rows, self.width), F32),
                pltpu.VMEM(self.vec_shape, F32),
            ]
            + [pltpu.VMEM(g.shape, BF16) for g in whole_grads]
            + [pltpu.VMEM(s, BF16) for s in shares]
            + [pltpu.VMEM(s, BF16) for s in shares]
            + sum(scratch, []),
            compiler_params=self.comm_params(collective_id),
            cost_estimate=self.cost(2),
        )(flowing, images, *weights, vecs, *keeps, *grads)
        return out[0], out[1:4], out[4], out[5]


def greet(targets):
    barrier = pltpu.get_barrier_semaphore()
    for target in targets:
        pl.semaphore_signal(
            barrier, inc=1, device_id=target, device_id_type=pl.DeviceIdType.MESH
        )
    pl.semaphore_wait(barrier, len(targets))


def transfer(src, dst, sems, at, target):
    return pltpu.make_async_remote_copy(
        src_ref=src,
        dst_ref=dst,
        send_sem=sems[0].at[at],
        recv_sem=sems[1].at[at],
        device_id=target,
        device_id_type=pl.DeviceIdType.MESH,
    )


class Chunk:
    def __init__(self, array, blocks, columns, by_columns, extent, start, chips):
        self.array, self.by_columns, self.start, self.extent = array, by_columns, start, extent
        self.blocks = blocks if by_columns else extent
        self.columns = extent if by_columns else columns
        self.stride = (columns if by_columns else blocks) // 2
        self.pieces = math.gcd(self.blocks, chips)
        self.run = self.blocks // self.pieces

    def part(self, ref, core, piece=None, shard=slice(None)):
        at = core * self.stride + self.start
        first, size = (0, self.blocks) if piece is None else (piece * self.run, self.run)
        if self.by_columns:
            columns = pl.ds(pl.multiple_of(at, 128), self.columns)
            return ref.at[shard, pl.ds(first, size), :, columns]
        return ref.at[shard, pl.ds(at + first, size)]


def chunks_of(arrays, mesh_sizes, want=1):
    chips = mesh_sizes[1] // 2
    lists = []
    for array, (_, blocks, _, columns) in enumerate(a.shape for a in arrays):
        by_columns = columns % 256 == 0 and columns > blocks * 8
        half = columns // 2 if by_columns else blocks // 2
        unit = 128 if by_columns else 1
        parts = want if half % (want * unit) == 0 else 1
        extent = half // parts
        lists.append(
            [
                Chunk(array, blocks, columns, by_columns, extent, j * extent, chips)
                for j in range(parts)
            ]
        )
    return sum(lists, [])


class Place:
    def __init__(self, sizes):
        self.groups, self.reps = sizes
        self.rep, self.mine = lax.axis_index("rep"), lax.axis_index("grp")
        self.chip, self.core = self.rep // 2, lax.rem(self.rep, 2)
        self.chips = self.reps // 2
        self.shard_peers = [
            (self.rep, lax.rem(self.mine + d, self.groups)) for d in range(1, self.groups)
        ]
        self.core_peer = (self.chip * 2 + 1 - self.core, self.mine)

    def piece(self, chunk):
        return lax.rem(self.chip, chunk.pieces)

    def mate(self, chunk, step):
        piece = self.piece(chunk)
        return self.chip - piece + lax.rem(piece + step, chunk.pieces)

    def at(self, chip):
        return (chip * 2 + self.core, self.mine)


class Gather:
    def __init__(self, chunks, sizes, ins, vec_in, outs, vec_out, sems):
        self.chunks, self.place = chunks, Place(sizes)
        self.ins, self.outs, self.vec_in, self.vec_out = ins, outs, vec_in, vec_out
        self.own_sem, self.vec_own_sem = sems[:2]
        self.vec_sems, self.shard_sems, self.chip_sems, self.core_sems = (
            sems[2 + 2 * i : 4 + 2 * i] for i in range(4)
        )

    @staticmethod
    def semaphores(chunks, sizes):
        groups = sizes[0]
        most = max(c.pieces for c in chunks)
        count = len(chunks)
        return (
            [pltpu.SemaphoreType.DMA((count,)), pltpu.SemaphoreType.DMA]
            + dma_pair(groups - 1)
            + dma_pair(count, groups - 1)
            + dma_pair(count, max(most - 1, 1))
            + dma_pair(count)
        )

    def shards(self, i):
        chunk, place = self.chunks[i], self.place
        piece = place.piece(chunk)
        src = chunk.part(self.ins[chunk.array], place.core, piece, 0)
        dst = chunk.part(self.outs[chunk.array], place.core, piece, place.mine)
        return [
            transfer(src, dst, self.shard_sems, (i, d), t)
            for d, t in enumerate(place.shard_peers)
        ]

    def own(self, i):
        chunk, place = self.chunks[i], self.place
        piece = place.piece(chunk)
        src = chunk.part(self.ins[chunk.array], place.core, piece, 0)
        dst = chunk.part(self.outs[chunk.array], place.core, piece, place.mine)
        return pltpu.make_async_copy(src, dst, self.own_sem.at[i])

    def vectors(self):
        return [
            transfer(self.vec_in.at[0], self.vec_out.at[self.place.mine], self.vec_sems, d, t)
            for d, t in enumerate(self.place.shard_peers)
        ]

    def vector_own(self):
        return pltpu.make_async_copy(
            self.vec_in.at[0], self.vec_out.at[self.place.mine], self.vec_own_sem
        )

    def chips(self, i):
        chunk, place = self.chunks[i], self.place
        block = chunk.part(self.outs[chunk.array], place.core, place.piece(chunk))
        return [
            transfer(block, block, self.chip_sems, (i, e - 1), place.at(place.mate(chunk, e)))
            for e in range(1, chunk.pieces)
        ]

    def cores(self, i):
        chunk, place = self.chunks[i], self.place
        block = chunk.part(self.outs[chunk.array], place.core)
        return [transfer(block, block, self.core_sems, i, place.core_peer)]

    def greet(self):
        place = self.place
        most = max(self.chunks, key=lambda c: c.pieces)
        greet(
            place.shard_peers
            + [place.at(place.mate(most, e)) for e in range(1, most.pieces)]
            + [place.core_peer]
        )

    def begin(self):
        for i in range(len(self.chunks)):
            start(self.shards(i))
            self.own(i).start()
        if self.vec_in is not None:
            start(self.vectors())
            self.vector_own().start()

    def all_to_chips(self):
        for i in range(len(self.chunks)):
            self.to_chips(i)

    def all_to_cores(self):
        for i in range(len(self.chunks)):
            self.to_cores(i)

    def to_chips(self, i):
        self.own(i).wait()
        arrive(self.shards(i))
        start(self.chips(i))

    def to_cores(self, i):
        arrive(self.chips(i))
        start(self.cores(i))

    def finish(self):
        every = range(len(self.chunks))
        for i in every:
            arrive(self.cores(i))
        if self.vec_in is not None:
            arrive(self.vectors())
            self.vector_own().wait()
            for copy in self.vectors():
                copy.wait_send()
        for i in every:
            for copy in self.shards(i) + self.chips(i) + self.cores(i):
                copy.wait_send()


def start(copies):
    for copy in copies:
        copy.start()


def arrive(copies):
    for copy in copies:
        copy.wait_recv()


def gather_kernel(chunks, sizes, *refs):
    work = Gather(chunks, sizes, refs[:1], refs[1], refs[2:3], refs[3], refs[4:])
    work.greet()
    work.begin()
    work.all_to_chips()
    work.all_to_cores()
    work.finish()


def dma_pair(*shape):
    return [pltpu.SemaphoreType.DMA(shape), pltpu.SemaphoreType.DMA(shape)]


VMEM_SPEC = pl.BlockSpec(memory_space=pltpu.VMEM)
ANY_SPEC = pl.BlockSpec(memory_space=pl.ANY)


def gathered_shapes(shards, groups):
    return [jax.ShapeDtypeStruct((groups,) + s.shape[1:], s.dtype) for s in shards]


def gather(shard, vec, sizes, collective_id):
    chunks = chunks_of([shard], sizes, 2)
    return pl.pallas_call(
        functools.partial(gather_kernel, chunks, sizes),
        name="gather_params",
        out_shape=gathered_shapes([shard, vec], sizes[0]),
        in_specs=[VMEM_SPEC] * 2,
        out_specs=[VMEM_SPEC] * 2,
        scratch_shapes=Gather.semaphores(chunks, sizes),
        compiler_params=pltpu.CompilerParams(
            collective_id=collective_id, has_side_effects=True, vmem_limit_bytes=40 * 2**20
        ),
    )(shard, vec)


def add_up(first, rest):
    total = first.astype(F32)
    for term in rest:
        total = total + term.astype(F32)
    return total


class Reduce:
    def __init__(self, chunks, sizes, ins, vec_in, outs, vec_out, scratch):
        count = len(chunks)
        self.chunks, self.place = chunks, Place(sizes)
        self.ins, self.vec_in, self.outs, self.vec_out = ins, vec_in, outs, vec_out
        self.core_sum, self.from_chips, self.chip_sum, self.from_shards = (
            scratch[i * count : (i + 1) * count] for i in range(4)
        )
        sems = scratch[4 * count :]
        names = ("core_sems", "chip_sems", "shard_sems", "spread_sems", "join_sems")
        for i, name in enumerate(names):
            setattr(self, name, sems[2 * i : 2 * i + 2])
        if vec_in is not None:
            self.vec_sems = sems[10:12]
            self.vec_parts, self.vec_held = sems[12:]

    @staticmethod
    def scratch(chunks, sizes, vec_shape):
        groups, reps = sizes
        chips, count = reps // 2, len(chunks)
        most = max(c.pieces for c in chunks)
        half = [(groups, c.blocks, 8, c.columns) for c in chunks]
        piece = [(groups, c.run, 8, c.columns) for c in chunks]
        shapes = (
            half
            + [(chips - 1,) + p for p in piece]
            + piece
            + [(groups - 1,) + p[1:] for p in piece]
        )
        made = (
            [pltpu.VMEM(s, BF16) for s in shapes]
            + dma_pair(count)
            + dma_pair(count, chips - 1)
            + dma_pair(count, groups - 1)
            + dma_pair(count, max(most - 1, 1))
            + dma_pair(count)
        )
        if vec_shape is not None:
            terms = chips + groups - 1
            made += dma_pair(terms)
            made += [pltpu.VMEM((terms,) + vec_shape, F32), pltpu.VMEM((2,) + vec_shape, F32)]
        return made

    def chip_ids(self):
        place = self.place
        return [lax.rem(place.chip + e, place.chips) for e in range(1, place.chips)]

    def cores(self, i):
        chunk, place = self.chunks[i], self.place
        src = chunk.part(self.ins[chunk.array], 1 - place.core)
        return [transfer(src, self.core_sum[i], self.core_sems, i, place.core_peer)]

    def chips(self, i):
        chunk, copies = self.chunks[i], []
        for e, chip in enumerate(self.chip_ids()):
            piece = lax.rem(chip, chunk.pieces)
            src = self.core_sum[i].at[:, pl.ds(piece * chunk.run, chunk.run)]
            dst = self.from_chips[i].at[e]
            copies.append(transfer(src, dst, self.chip_sems, (i, e), self.place.at(chip)))
        return copies

    def shards(self, i):
        place = self.place
        return [
            transfer(
                self.chip_sum[i].at[lax.rem(place.mine + d + 1, place.groups)],
                self.from_shards[i].at[d],
                self.shard_sems,
                (i, d),
                target,
            )
            for d, target in enumerate(place.shard_peers)
        ]

    def spread(self, i):
        chunk, place = self.chunks[i], self.place
        block = chunk.part(self.outs[chunk.array], place.core, place.piece(chunk), 0)
        return [
            transfer(block, block, self.spread_sems, (i, e - 1), place.at(place.mate(chunk, e)))
            for e in range(1, chunk.pieces)
        ]

    def join(self, i):
        chunk, place = self.chunks[i], self.place
        block = chunk.part(self.outs[chunk.array], place.core, None, 0)
        return [transfer(block, block, self.join_sems, i, place.core_peer)]

    def vec_cores(self):
        return [transfer(self.vec_in, self.vec_parts.at[0], self.vec_sems, 0, self.place.core_peer)]

    def vec_chips(self):
        return [
            transfer(
                self.vec_held.at[0],
                self.vec_parts.at[1 + e],
                self.vec_sems,
                1 + e,
                self.place.at(chip),
            )
            for e, chip in enumerate(self.chip_ids())
        ]

    def vec_shards(self):
        chips = self.place.chips
        return [
            transfer(
                self.vec_held.at[1],
                self.vec_parts.at[chips + d],
                self.vec_sems,
                chips + d,
                target,
            )
            for d, target in enumerate(self.place.shard_peers)
        ]

    def greet(self):
        place = self.place
        greet(
            place.shard_peers + [place.at(c) for c in self.chip_ids()] + [place.core_peer]
        )

    def begin(self):
        for i in range(len(self.chunks)):
            start(self.cores(i))
        if self.vec_in is not None:
            start(self.vec_cores())

    def all_to_chips(self):
        for i in range(len(self.chunks)):
            self.to_chips(i)
        if self.vec_in is not None:
            self.vec_to_chips()

    def all_to_shards(self):
        for i in range(len(self.chunks)):
            self.to_shards(i)
        if self.vec_in is not None:
            self.vec_to_shards()

    def all_to_spread(self):
        for i in range(len(self.chunks)):
            self.to_spread(i)
        if self.vec_in is not None:
            self.vec_end()

    def all_to_join(self):
        for i in range(len(self.chunks)):
            self.to_join(i)

    def to_chips(self, i):
        chunk = self.chunks[i]
        own = chunk.part(self.ins[chunk.array], self.place.core)[...]
        arrive(self.cores(i))
        self.core_sum[i][...] = own + self.core_sum[i][...]
        start(self.chips(i))

    def vec_to_chips(self):
        arrive(self.vec_cores())
        self.vec_held[0] = self.vec_in[...] + self.vec_parts[0]
        start(self.vec_chips())

    def to_shards(self, i):
        chunk = self.chunks[i]
        piece = self.place.piece(chunk)
        own = self.core_sum[i][:, pl.ds(piece * chunk.run, chunk.run)]
        copies = self.chips(i)
        arrive(copies)
        total = add_up(own, [self.from_chips[i][e] for e in range(len(copies))])
        self.chip_sum[i][...] = total.astype(BF16)
        start(self.shards(i))

    def vec_to_shards(self):
        copies = self.vec_chips()
        arrive(copies)
        self.vec_held[1] = add_up(
            self.vec_held[0], [self.vec_parts[1 + e] for e in range(len(copies))]
        )
        start(self.vec_shards())

    def to_spread(self, i):
        chunk, place = self.chunks[i], self.place
        copies = self.shards(i)
        arrive(copies)
        total = add_up(
            self.chip_sum[i][place.mine], [self.from_shards[i][d] for d in range(len(copies))]
        )
        block = chunk.part(self.outs[chunk.array], place.core, place.piece(chunk), 0)
        block[...] = total.astype(BF16)
        start(self.spread(i))

    def vec_end(self):
        copies = self.vec_shards()
        arrive(copies)
        self.vec_out[...] = add_up(
            self.vec_held[1], [self.vec_parts[self.place.chips + d] for d in range(len(copies))]
        )

    def to_join(self, i):
        arrive(self.spread(i))
        start(self.join(i))

    def finish(self):
        every = range(len(self.chunks))
        for i in every:
            arrive(self.join(i))
        copies = []
        if self.vec_in is not None:
            copies = self.vec_cores() + self.vec_chips() + self.vec_shards()
        for i in every:
            copies += self.cores(i) + self.chips(i) + self.shards(i)
            copies += self.spread(i) + self.join(i)
        for copy in copies:
            copy.wait_send()


def on_device(
    reps,
    images,
    cotangent,
    ln1_gain,
    ln1_bias,
    w_qkv,
    q_bias,
    v_bias,
    w_proj,
    proj_bias,
    ln2_gain,
    ln2_bias,
    w_up,
    up_bias,
    w_down,
    down_bias,
):
    groups = lax.axis_size("grp")
    sizes = (groups, reps)
    layers, part = ln1_gain.shape
    width = part * groups
    hidden_part = up_bias.shape[1]
    plan = Plan(images.shape, hidden_part * groups)
    vectors = [ln1_gain, ln1_bias, q_bias, v_bias, proj_bias, ln2_gain, ln2_bias, down_bias]
    extra = hidden_part // part
    packed = jnp.stack(vectors, axis=1)
    packed = jnp.concatenate([packed, up_bias.reshape(layers, extra, part)], axis=1)
    packed = packed.astype(F32)
    joined = jnp.concatenate([w_qkv, w_proj], axis=2)

    def shards_of(layer):
        return [m[layer].reshape(1, -1, 8, m.shape[2]) for m in (joined, w_up, w_down)]

    def unpack(vecs):
        vectors = vecs[:, :VECTORS].transpose(1, 0, 2).reshape(VECTORS, width)
        up = vecs[:, VECTORS:].reshape(extra, width)
        rest = plan.vec_rows - VECTORS - extra
        return jnp.concatenate([vectors, up, jnp.zeros((rest, width), F32)], axis=0)

    shards0, shards1 = shards_of(0), shards_of(1)
    first_matrix, vecs0 = gather(shards0[0], packed[0][None], sizes, 0)
    first_matrix, vecs0 = first_matrix.reshape(width, -1), unpack(vecs0)
    hidden, keeps, mlp0, gathered = plan.first(
        images, first_matrix, vecs0, shards0[1:], shards1 + [packed[1][None]], sizes, 1
    )
    weights1 = [g.reshape(-1, g.shape[3]) for g in gathered[:3]]
    encoded, flowing, grads1 = plan.middle(hidden, cotangent, weights1, unpack(gathered[3]))
    blocks = [g.reshape(groups, -1, 8, g.shape[1]) for g in grads1[:3]] + [grads1[3]]
    images_grad, sums, small0, small1 = plan.last(
        flowing, images, [first_matrix] + list(mlp0), vecs0, keeps, blocks, sizes, 2
    )
    full = [x.reshape(layers, -1, x.shape[3]) for x in sums]
    small = jnp.stack([small0, small1])
    me = lax.axis_index("grp")
    vec_out = lax.dynamic_slice_in_dim(small[:, :VECTORS], me * part, part, axis=2)
    up_out = small[:, VECTORS : VECTORS + extra].reshape(layers, -1)
    up_out = lax.dynamic_slice_in_dim(up_out, me * hidden_part, hidden_part, axis=1)
    return (
        encoded,
        images_grad,
        vec_out[:, G1],
        vec_out[:, B1],
        full[0][:, :, : 3 * width],
        vec_out[:, QB],
        vec_out[:, VB],
        full[0][:, :, 3 * width :],
        vec_out[:, PB],
        vec_out[:, G2],
        vec_out[:, B2],
        full[1],
        up_out,
        full[2],
        vec_out[:, DB],
    )


def solution(mesh):
    batch = P(("rep", "grp"), None, None)
    vector = P(None, "grp")
    matrix = P(None, "grp", None)
    params = (
        vector,
        vector,
        matrix,
        vector,
        vector,
        matrix,
        vector,
        vector,
        vector,
        matrix,
        vector,
        matrix,
        vector,
    )
    specs = (batch, batch) + params
    return jax.shard_map(
        functools.partial(on_device, mesh.shape["rep"]), mesh=mesh, in_specs=specs, out_specs=specs, check_vma=False
    )
```

```python
import functools
import math

import jax
import jax.numpy as jnp
from jax import lax
from jax.experimental import pallas as pl
from jax.experimental.pallas import tpu as pltpu
from jax.sharding import PartitionSpec as P

HEAD_DIM = 64
PAIR = 2 * HEAD_DIM
EPS = 1e-06
INV_ROOT_TWO = 0.7071067811865476
INV_ROOT_TAU = 0.3989422804014327
MASKED = -1e30
F32 = jnp.float32
BF16 = jnp.bfloat16

VECTORS = 8
G1, B1, QB, VB, PB, G2, B2, DB = range(VECTORS)


def dot(left, right):
    return jnp.dot(left, right, preferred_element_type=F32)


def dot_nt(left, right):
    return lax.dot_general(
        left, right, (((1,), (1,)), ((), ())), preferred_element_type=F32
    )


def col_sum(rows):
    return jnp.sum(rows, axis=0, keepdims=True)


def norm(rows):
    mean = jnp.mean(rows, axis=-1, keepdims=True)
    centered = rows - mean
    inv = lax.rsqrt(jnp.mean(centered * centered, axis=-1, keepdims=True) + EPS)
    return centered * inv, inv


def norm_backward(grad, normed, inv, gain):
    scaled = grad * gain
    return inv * (
        scaled
        - jnp.mean(scaled, axis=-1, keepdims=True)
        - normed * jnp.mean(scaled * normed, axis=-1, keepdims=True)
    )


def attn_forward(qkv, keep, image, seq, pad):
    width = qkv.shape[1] // 3
    base = image * pad
    rows = pl.ds(base, pad)
    value_t = qkv[rows, pl.ds(2 * width, width)].T
    lane = lax.broadcasted_iota(jnp.int32, (1, PAIR), 1)
    halves = [(lane < HEAD_DIM).astype(F32).astype(BF16), (lane >= HEAD_DIM).astype(F32).astype(BF16)]
    full = seq // 8 * 8
    for pair in range(width // PAIR):
        queries = qkv[rows, pl.ds(pair * PAIR, PAIR)]
        keys = qkv[rows, pl.ds(width + pair * PAIR, PAIR)]
        for half in range(2):
            head = 2 * pair + half
            scores = dot_nt(keys * halves[half], queries)
            parts = [scores[:full]]
            if full < seq:
                tail = scores[full : full + 8]
                row = lax.broadcasted_iota(jnp.int32, tail.shape, 0)
                parts.append(jnp.where(row < seq - full, tail, MASKED))
            scores = jnp.concatenate(parts, axis=0)
            top = jnp.max(scores, axis=0, keepdims=True)
            raised = jnp.exp(scores - top)
            probs = raised * (1.0 / col_sum(raised))
            rest = pad - probs.shape[0]
            if rest:
                probs = jnp.concatenate([probs, jnp.zeros((rest, pad), F32)], axis=0)
            keep["probs"][image, head] = probs
            context = dot(value_t[head * HEAD_DIM : (head + 1) * HEAD_DIM], probs.astype(BF16))
            keep["context"][image, pl.ds(head * HEAD_DIM, HEAD_DIM), :] = context.astype(BF16)


def split_attention(packed):
    width = packed.shape[0]
    return packed.at[:, pl.ds(0, 3 * width)], packed.at[:, pl.ds(3 * width, width)]


def up_bias_of(vecs, hidden_width):
    rows = hidden_width // vecs.shape[1]
    return jnp.concatenate([vecs[VECTORS + i : VECTORS + i + 1] for i in range(rows)], axis=1)


def attention_part(hidden, packed, vecs, keep, images, seq, pad):
    w_qkv, w_proj = split_attention(packed)
    width = hidden.shape[1]
    normed, _ = norm(hidden)
    rows_in = (normed * vecs[G1 : G1 + 1] + vecs[B1 : B1 + 1]).astype(BF16)
    qkv = keep["qkv"]
    projected = dot(rows_in, w_qkv[...])
    qkv[:, :width] = (projected[:, :width] + vecs[QB : QB + 1]).astype(BF16) * jnp.asarray(
        HEAD_DIM**-0.5, BF16
    )
    qkv[:, width : 2 * width] = projected[:, width : 2 * width].astype(BF16)
    qkv[:, 2 * width :] = (projected[:, 2 * width :] + vecs[VB : VB + 1]).astype(BF16)
    for image in range(images):
        attn_forward(qkv, keep, image, seq, pad)
    context = jnp.concatenate([keep["context"][image].T for image in range(images)], axis=0)
    mixed = hidden + dot(context, w_proj[...]) + vecs[PB : PB + 1]
    keep["mixed"][...] = mixed
    return mixed


def mlp_part(mixed, w_up, w_down, vecs, keep):
    up_bias = up_bias_of(vecs, w_down.shape[0])
    normed, _ = norm(mixed)
    rows_mid = (normed * vecs[G2 : G2 + 1] + vecs[B2 : B2 + 1]).astype(BF16)
    upward = dot(rows_mid, w_up[...]) + up_bias
    cumul = 0.5 * (1.0 + lax.erf(upward * INV_ROOT_TWO))
    keep["active"][...] = (upward * cumul).astype(BF16)
    slope = cumul + upward * jnp.exp(-0.5 * upward * upward) * INV_ROOT_TAU
    keep["slope"][...] = slope.astype(keep["slope"].dtype)
    return mixed + dot(keep["active"][...], w_down[...]) + vecs[DB : DB + 1]


def attn_backward(qkv, keep, context_grad, joint, vec_grads, image, pad):
    width = qkv.shape[1] // 3
    rows = pl.ds(image * pad, pad)
    keys_t = qkv[rows, pl.ds(width, width)].T
    lane = lax.broadcasted_iota(jnp.int32, (1, PAIR), 1)
    low = lax.broadcasted_iota(jnp.int32, (pad, PAIR), 1) < HEAD_DIM
    halves = [(lane < HEAD_DIM).astype(F32).astype(BF16), (lane >= HEAD_DIM).astype(F32).astype(BF16)]
    query_parts = []
    for pair in range(width // PAIR):
        queries = qkv[rows, pl.ds(pair * PAIR, PAIR)]
        values = qkv[rows, pl.ds(2 * width + pair * PAIR, PAIR)]
        ctx = context_grad[rows, pl.ds(pair * PAIR, PAIR)]
        key_parts, value_parts = [], []
        for half in range(2):
            head = 2 * pair + half
            probs = keep["probs"][image, head]
            prob_grad = dot_nt(values * halves[half], ctx)
            value_parts.append(dot(probs.astype(BF16), ctx))
            row_dot = col_sum(probs * prob_grad)
            score_grad = (probs * (prob_grad - row_dot)).astype(BF16)
            key_parts.append(dot(score_grad, queries))
            query_parts.append(dot(keys_t[head * HEAD_DIM : (head + 1) * HEAD_DIM], score_grad))
        key_grad = jnp.where(low, key_parts[0], key_parts[1])
        value_grad = jnp.where(low, value_parts[0], value_parts[1])
        joint[rows, pl.ds(width + pair * PAIR, PAIR)] = key_grad.astype(BF16)
        joint[rows, pl.ds(2 * width + pair * PAIR, PAIR)] = value_grad.astype(BF16)
        vec_grads[VB : VB + 1, pl.ds(pair * PAIR, PAIR)] += col_sum(value_grad)
    query_grad = jnp.concatenate(query_parts, axis=0).T * HEAD_DIM**-0.5
    joint[rows, pl.ds(0, width)] = query_grad.astype(BF16)
    vec_grads[QB : QB + 1, :] += col_sum(query_grad)


def mlp_backward(out_grad, w_up, w_down, vecs, keep, acc):
    _, _, g_up, g_down, vec_grads, up_bias_grad = acc[:6]
    rounded = out_grad.astype(BF16)
    vec_grads[DB : DB + 1, :] += col_sum(out_grad)
    g_down[...] += dot(rounded.T, keep["active"][...])
    up_grad = dot_nt(rounded, w_down[...]) * keep["slope"][...].astype(F32)
    up_bias_grad[...] += col_sum(up_grad)
    up_rounded = up_grad.astype(BF16)
    normed, inv = norm(keep["mixed"][...])
    gain = vecs[G2 : G2 + 1]
    rows_mid = (normed * gain + vecs[B2 : B2 + 1]).astype(BF16)
    g_up[...] += dot(rows_mid.T, up_rounded)
    mid_grad = dot_nt(up_rounded, w_up[...])
    vec_grads[G2 : G2 + 1, :] += col_sum(mid_grad * normed)
    vec_grads[B2 : B2 + 1, :] += col_sum(mid_grad)
    return out_grad + norm_backward(mid_grad, normed, inv, gain)


def attention_backward(mixed_grad, hidden, packed, vecs, keep, acc, joint, images, pad):
    _, w_proj = split_attention(packed)
    g_qkv, g_proj, _, _, vec_grads, _, context_grad = acc
    vec_grads[PB : PB + 1, :] += col_sum(mixed_grad)
    mixed_rounded = mixed_grad.astype(BF16)
    part = g_proj[...]
    for image in range(images):
        part += dot(keep["context"][image], mixed_rounded[image * pad : (image + 1) * pad])
    g_proj[...] = part
    context_grad[...] = dot_nt(mixed_rounded, w_proj[...]).astype(BF16)
    for image in range(images):
        attn_backward(keep["qkv"], keep, context_grad, joint, vec_grads, image, pad)
    normed, _ = norm(hidden)
    rows_in = (normed * vecs[G1 : G1 + 1] + vecs[B1 : B1 + 1]).astype(BF16)
    g_qkv[...] += dot(rows_in.T, joint[...])


def input_backward(mixed_grad, hidden, packed, vecs, vec_grads, joint):
    w_qkv, _ = split_attention(packed)
    normed, inv = norm(hidden)
    in_grad = dot_nt(joint[...], w_qkv[...])
    vec_grads[G1 : G1 + 1, :] += col_sum(in_grad * normed)
    vec_grads[B1 : B1 + 1, :] += col_sum(in_grad)
    return mixed_grad + norm_backward(in_grad, normed, inv, vecs[G1 : G1 + 1])


def load_padded(ref, buf, pad):
    images, seq, width = ref.shape
    for image in range(images):
        buf[pl.ds(image * pad, seq), :] = ref[image].astype(F32)
        if pad > seq:
            buf[pl.ds(image * pad + seq, pad - seq), :] = jnp.zeros((pad - seq, width), F32)


def store_images(ref, rows, pad):
    images, seq, _ = ref.shape
    for image in range(images):
        ref[image] = rows[image * pad : image * pad + seq].astype(ref.dtype)


KEEP = ("qkv", "probs", "context", "mixed", "active", "slope")


def keep_shapes(images, pad, width, hidden_width):
    heads = width // HEAD_DIM
    return {
        "qkv": ((images * pad, 3 * width), BF16),
        "probs": ((images, heads, pad, pad), F32),
        "context": ((images, width, pad), BF16),
        "mixed": ((images * pad, width), F32),
        "active": ((images * pad, hidden_width), BF16),
        "slope": ((images * pad, hidden_width), F32),
    }


def init_grads(acc):
    @pl.when(pl.program_id(0) == 0)
    def _():
        for ref in acc[:6]:
            ref[...] = jnp.zeros_like(ref)


def flush_vectors(acc, vecs):
    vec_grads, up_bias_grad = acc[4:6]
    width = vecs.shape[1]
    extra = up_bias_grad.shape[1] // width
    vecs[:VECTORS, :] = vec_grads[...]
    for i in range(extra):
        vecs[VECTORS + i : VECTORS + i + 1, :] = up_bias_grad[:, i * width : (i + 1) * width]
    rest = vecs.shape[0] - VECTORS - extra
    if rest:
        vecs[VECTORS + extra :, :] = jnp.zeros((rest, width), F32)


def step_at(step):
    return pl.when(pl.program_id(0) == step)


def first_kernel(sizes, steps, mesh_sizes, chunks, *refs):
    group, seq, pad = sizes
    images, packed, vecs = refs[:3]
    shards0, shards1 = refs[3:5], refs[5:9]
    out = refs[9]
    keep = dict(zip(KEEP, refs[10:16]))
    mlp_out = refs[16:18]
    full1 = refs[18:22]
    buf, mixed_rows = refs[22:24]
    landed = refs[24:26]
    rest = refs[26:]
    half = len(rest) // 2
    now = Gather(chunks[0], mesh_sizes, shards0, None, landed, None, rest[:half])
    later = Gather(
        chunks[1], mesh_sizes, shards1[:3], shards1[3], full1[:3], full1[3], rest[half:]
    )
    step = pl.program_id(0)
    rows = group * pad

    @step_at(0)
    def _():
        now.greet()
        now.begin()
        later.begin()

    @step_at(2 * steps // 5)
    def _():
        now.all_to_chips()

    @pl.when(step < steps)
    def _():
        load_padded(images, buf, pad)
        mixed = attention_part(buf[...], packed, vecs, keep, group, seq, pad)
        mixed_rows[pl.ds(pl.multiple_of(step * rows, rows), rows), :] = mixed

    @step_at(steps)
    def _():
        now.all_to_cores()
        later.all_to_chips()
        now.finish()
        for matrix, source in zip(mlp_out, landed):
            flat = source[...].astype(F32).reshape(matrix.shape)
            matrix[...] = flat.astype(BF16)

    @step_at(2 * steps - 1)
    def _():
        later.all_to_cores()

    @pl.when(step >= steps)
    def _():
        at = pl.multiple_of((step - steps) * rows, rows)
        mixed = mixed_rows[pl.ds(at, rows), :]
        out[...] = mlp_part(mixed, mlp_out[0], mlp_out[1], vecs, keep)

    @step_at(2 * steps - 1)
    def _():
        later.finish()


def middle_kernel(sizes, *refs):
    group, seq, pad = sizes
    hidden, cotangent, packed, w_up, w_down, vecs, encoded, flowing = refs[:8]
    outs, vec_out = refs[8:11], refs[11]
    keep = dict(zip(KEEP, refs[12:18]))
    acc = refs[18:25]
    joint, buf = refs[25:]
    init_grads(acc)
    mixed = attention_part(hidden[...], packed, vecs, keep, group, seq, pad)
    result = mlp_part(mixed, w_up, w_down, vecs, keep)
    store_images(encoded, result, pad)
    load_padded(cotangent, buf, pad)
    mixed_grad = mlp_backward(buf[...], w_up, w_down, vecs, keep, acc)
    attention_backward(mixed_grad, hidden[...], packed, vecs, keep, acc, joint, group, pad)
    flowing[...] = input_backward(mixed_grad, hidden[...], packed, vecs, acc[4], joint)

    @step_at(pl.num_programs(0) - 1)
    def _():
        g_qkv_out, g_proj_out = split_attention(outs[0])
        g_qkv_out[...] = acc[0][...].astype(BF16)
        g_proj_out[...] = acc[1][...].astype(BF16)
        outs[1][...] = acc[2][...].astype(BF16)
        outs[2][...] = acc[3][...].astype(BF16).T
        flush_vectors(acc, vec_out)


def last_kernel(sizes, steps, mesh_sizes, chunks, counts, *refs):
    group, seq, pad = sizes
    flowing, images, packed, w_up, w_down, vecs = refs[:6]
    keep = dict(zip(KEEP, refs[6:12]))
    grads1, vec1 = refs[12:15], refs[15]
    images_grad, sums, vec_out0, vec_out1 = refs[16], refs[17:21], refs[21], refs[22]
    acc = refs[23:30]
    buf, grad_rows, joint_rows, vec0 = refs[30:34]
    grads0, shares0, shares1 = refs[34:37], refs[37:40], refs[40:43]
    scratch = refs[43:]
    ends = [sum(counts[: i + 1]) for i in range(3)]
    later = Reduce(chunks[0], mesh_sizes, grads1, vec1, shares1, vec_out1, scratch[: ends[0]])
    mlp = Reduce(
        chunks[1], mesh_sizes, grads0[1:], None, shares0[1:], None, scratch[ends[0] : ends[1]]
    )
    tail = Reduce(
        chunks[2],
        mesh_sizes,
        grads0[:1],
        vec0,
        shares0[:1],
        vec_out0,
        scratch[ends[1] :],
        vec_along=False,
    )
    step = pl.program_id(0)
    rows = group * pad
    last = 3 * steps - 1
    three = acc[0].shape[1]

    def rows_at(start):
        return pl.ds(pl.multiple_of((step - start) * rows, rows), rows)

    @step_at(0)
    def _():
        later.greet()
        later.begin()

    @step_at(1 * steps // 5)
    def _():
        later.all_to_chips()

    init_grads(acc)

    @pl.when(step < steps)
    def _():
        grad_rows[rows_at(0), :] = mlp_backward(flowing[...], w_up, w_down, vecs, keep, acc)

    @step_at(steps)
    def _():
        grads0[1][...] = acc[2][...].reshape(grads0[1].shape).astype(BF16)
        grads0[2][...] = acc[3][...].T.reshape(grads0[2].shape).astype(BF16)
        mlp.begin()

    @step_at(steps + 1 * steps // 5)
    def _():
        later.all_to_shards()
        mlp.all_to_chips()

    @step_at(steps + 3 * steps // 5)
    def _():
        later.all_to_spread()

    @step_at(2 * steps - 1)
    def _():
        later.all_to_join()

    @pl.when((step >= steps) & (step < 2 * steps))
    def _():
        load_padded(images, buf, pad)
        attention_backward(
            grad_rows[rows_at(steps), :],
            buf[...],
            packed,
            vecs,
            keep,
            acc,
            joint_rows.at[rows_at(steps), :],
            group,
            pad,
        )

    @step_at(2 * steps)
    def _():
        shape = grads0[0].shape
        grads0[0][:, :, :, :three] = acc[0][...].reshape(shape[:3] + (three,)).astype(BF16)
        grads0[0][:, :, :, three:] = (
            acc[1][...].reshape(shape[:3] + (shape[3] - three,)).astype(BF16)
        )
        tail.begin()
        mlp.all_to_shards()

    @step_at(2 * steps + 2 * steps // 5)
    def _():
        tail.all_to_chips()

    @step_at(last)
    def _():
        mlp.all_to_spread()

    @pl.when(step >= 2 * steps)
    def _():
        load_padded(images, buf, pad)
        result = input_backward(
            grad_rows[rows_at(2 * steps), :],
            buf[...],
            packed,
            vecs,
            acc[4],
            joint_rows.at[rows_at(2 * steps), :],
        )
        store_images(images_grad, result, pad)

    def store_sums(layer, shares):
        sums[0][layer] = shares[0][0, :, :, :three].astype(F32)
        sums[1][layer] = shares[0][0, :, :, three:].astype(F32)

    @step_at(last)
    def _():
        flush_vectors(acc, vec0)
        tail.vec_begin()
        tail.all_to_shards()
        tail.vec_to_chips()
        mlp.all_to_join()
        later.finish()
        store_sums(1, shares1)
        for total, share in zip(sums[2:], shares1[1:]):
            total[1] = share[0].astype(F32)
        tail.vec_to_shards()
        tail.all_to_spread()
        mlp.finish()
        for total, share in zip(sums[2:], shares0[1:]):
            total[0] = share[0].astype(F32)
        tail.all_to_join()
        tail.vec_end()
        tail.finish()
        store_sums(0, shares0)


def whole(shape):
    return pl.BlockSpec(shape, lambda i: (0,) * len(shape), pipeline_mode=pl.Buffered(1))


def rows_spec(shape, steps, start=0, again=False):
    def block(i):
        at = jnp.maximum(i - start, 0)
        return lax.rem(at, steps) if again else jnp.minimum(at, steps - 1)

    return pl.BlockSpec(
        (shape[0] // steps,) + tuple(shape[1:]), lambda i: (block(i),) + (0,) * (len(shape) - 1)
    )


class Plan:
    def __init__(self, images_shape, hidden_width):
        self.count, self.seq, self.width = images_shape
        self.hidden_width = hidden_width
        self.pad = -(-self.seq // 16) * 16
        self.group = 2 if self.count % 2 == 0 else 1
        self.steps = self.count // self.group
        self.rows = self.count * self.pad
        self.keep = keep_shapes(self.count, self.pad, self.width, hidden_width)
        self.keep_block = keep_shapes(self.group, self.pad, self.width, hidden_width)
        self.weight_shapes = [
            (self.width, 3 * self.width),
            (self.width, self.width),
            (self.width, hidden_width),
            (hidden_width, self.width),
        ]
        self.sizes = (self.group, self.seq, self.pad)
        block_rows = self.group * self.pad
        self.buffer = pltpu.VMEM((block_rows, self.width), F32)
        self.acc = [
            pltpu.VMEM(self.weight_shapes[0], F32),
            pltpu.VMEM(self.weight_shapes[1], F32),
            pltpu.VMEM(self.weight_shapes[2], F32),
            pltpu.VMEM((self.width, hidden_width), F32),
            pltpu.VMEM((8, self.width), F32),
            pltpu.VMEM((1, hidden_width), F32),
            pltpu.VMEM((block_rows, self.width), BF16),
        ]
        self.joint = pltpu.VMEM((block_rows, 3 * self.width), BF16)
        self.vec_rows = -(-(VECTORS + hidden_width // self.width) // 8) * 8
        self.packed_shapes = [
            (self.width, 4 * self.width),
            (self.width, hidden_width),
            (hidden_width, self.width),
        ]
        self.vec_shape = (self.vec_rows, self.width)
        self.grad_shapes = [jax.ShapeDtypeStruct(s, BF16) for s in self.packed_shapes] + [
            jax.ShapeDtypeStruct(self.vec_shape, F32)
        ]
        self.params = pltpu.CompilerParams(
            dimension_semantics=("arbitrary",), vmem_limit_bytes=60 * 2**20
        )

    def image_spec(self, start=0, again=False):
        return rows_spec((self.count, self.seq, self.width), self.steps, start, again)

    def state_spec(self, start=0):
        return rows_spec((self.rows, self.width), self.steps, start)

    def param_specs(self):
        return [whole(s) for s in self.packed_shapes + [self.vec_shape]]

    def keep_specs(self, starts):
        return [rows_spec(self.keep[k][0], self.steps, at) for k, at in zip(KEEP, starts)]

    def grad_specs(self):
        return [whole(s.shape) for s in self.grad_shapes]

    def cost(self, layers):
        rows, width, hidden = self.count * self.seq, self.width, self.hidden_width
        flops = 2 * rows * width * (4 * width + 2 * hidden) * layers
        return pl.CostEstimate(
            flops=int(flops), bytes_accessed=int(40 * 2**20), transcendentals=0
        )

    def comm_params(self, collective_id):
        return pltpu.CompilerParams(
            dimension_semantics=("arbitrary",),
            vmem_limit_bytes=62 * 2**20,
            collective_id=collective_id,
            has_side_effects=True,
        )

    def first(self, images, packed, vecs, shards0, shards1, mesh_sizes, collective_id):
        state = jax.ShapeDtypeStruct((self.rows, self.width), F32)
        keeps = [jax.ShapeDtypeStruct(*self.keep[k]) for k in KEEP]
        mlp = [jax.ShapeDtypeStruct(s, BF16) for s in self.packed_shapes[1:]]
        chunks = [chunks_of(shards0, mesh_sizes), chunks_of(shards1[:3], mesh_sizes)]
        n = self.steps
        out = pl.pallas_call(
            functools.partial(first_kernel, self.sizes, n, mesh_sizes, chunks),
            name="layer_first",
            out_shape=[state] + keeps + mlp + gathered_shapes(shards1, mesh_sizes[0]),
            grid=(2 * n,),
            in_specs=[self.image_spec(), whole(packed.shape), whole(self.vec_shape)]
            + [ANY_SPEC] * 6,
            out_specs=[self.state_spec(n)]
            + self.keep_specs((0, 0, 0, 0, n, n))
            + [whole(m.shape) for m in mlp]
            + [ANY_SPEC] * 4,
            scratch_shapes=[self.buffer, pltpu.VMEM((self.rows, self.width), F32)]
            + [pltpu.VMEM(s.shape, BF16) for s in gathered_shapes(shards0, mesh_sizes[0])]
            + Gather.semaphores(chunks[0], mesh_sizes)
            + Gather.semaphores(chunks[1], mesh_sizes),
            compiler_params=self.comm_params(collective_id),
            cost_estimate=self.cost(1),
        )(images, packed, vecs, *shards0, *shards1)
        return out[0], out[1:7], out[7:9], out[9:]

    def middle(self, hidden, cotangent, weights, vecs):
        state = jax.ShapeDtypeStruct((self.rows, self.width), F32)
        out = pl.pallas_call(
            functools.partial(middle_kernel, self.sizes),
            name="layer_middle",
            out_shape=[jax.ShapeDtypeStruct(cotangent.shape, BF16), state] + self.grad_shapes,
            grid=(self.steps,),
            in_specs=[self.state_spec(), self.image_spec()] + self.param_specs(),
            out_specs=[self.image_spec(), self.state_spec()] + self.grad_specs(),
            scratch_shapes=[pltpu.VMEM(*self.keep_block[k]) for k in KEEP]
            + self.acc
            + [self.joint, self.buffer],
            compiler_params=self.params,
            cost_estimate=self.cost(3),
        )(hidden, cotangent, *weights, vecs)
        return out[0], out[1], out[2:]

    def last(self, flowing, images, weights, vecs, keeps, grads, mesh_sizes, collective_id):
        groups = mesh_sizes[0]
        whole_grads = [
            jax.ShapeDtypeStruct(g.shape, BF16) for g in grads[:3]
        ]
        chunks = [
            chunks_of(whole_grads, mesh_sizes, 1, (1,)),
            chunks_of(whole_grads[1:], mesh_sizes, 1, (0,)),
            chunks_of(whole_grads[:1], mesh_sizes, 3, (0,)),
        ]
        shares = [(1,) + g.shape[1:] for g in whole_grads]
        blocks = whole_grads[0].shape[1:3]
        sums = [
            jax.ShapeDtypeStruct((2,) + shape, F32)
            for shape in (
                blocks + (3 * self.width,),
                blocks + (self.width,),
                whole_grads[1].shape[1:],
                whole_grads[2].shape[1:],
            )
        ]
        vec = jax.ShapeDtypeStruct(self.vec_shape, F32)
        scratch = [
            Reduce.scratch(chunks[0], mesh_sizes, self.vec_shape),
            Reduce.scratch(chunks[1], mesh_sizes, None),
            Reduce.scratch(chunks[2], mesh_sizes, self.vec_shape),
        ]
        n = self.steps
        outs = [jax.ShapeDtypeStruct(images.shape, BF16)] + sums + [vec, vec]
        out = pl.pallas_call(
            functools.partial(
                last_kernel, self.sizes, n, mesh_sizes, chunks, [len(x) for x in scratch]
            ),
            name="layer_last",
            out_shape=outs,
            grid=(3 * n,),
            in_specs=[self.state_spec(), self.image_spec(n, True)]
            + self.param_specs()
            + self.keep_specs((n, n, n, 0, 0, 0))
            + [whole(g.shape) for g in grads],
            out_specs=[self.image_spec(2 * n)] + [whole(o.shape) for o in outs[1:]],
            scratch_shapes=self.acc
            + [
                self.buffer,
                pltpu.VMEM((self.rows, self.width), F32),
                pltpu.VMEM((self.rows, 3 * self.width), BF16),
                pltpu.VMEM(self.vec_shape, F32),
            ]
            + [pltpu.VMEM(g.shape, BF16) for g in whole_grads]
            + [pltpu.VMEM(s, BF16) for s in shares]
            + [pltpu.VMEM(s, BF16) for s in shares]
            + sum(scratch, []),
            compiler_params=self.comm_params(collective_id),
            cost_estimate=self.cost(2),
        )(flowing, images, *weights, vecs, *keeps, *grads)
        return out[0], out[1:5], out[5], out[6]


def greet(targets):
    barrier = pltpu.get_barrier_semaphore()
    for target in targets:
        pl.semaphore_signal(
            barrier, inc=1, device_id=target, device_id_type=pl.DeviceIdType.MESH
        )
    pl.semaphore_wait(barrier, len(targets))


def transfer(src, dst, sems, at, target):
    return pltpu.make_async_remote_copy(
        src_ref=src,
        dst_ref=dst,
        send_sem=sems[0].at[at],
        recv_sem=sems[1].at[at],
        device_id=target,
        device_id_type=pl.DeviceIdType.MESH,
    )


class Chunk:
    def __init__(self, array, blocks, columns, by_columns, extent, start, chips, shards_first):
        self.shards_first = shards_first
        self.array, self.by_columns, self.start, self.extent = array, by_columns, start, extent
        self.blocks = blocks if by_columns else extent
        self.columns = extent if by_columns else columns
        self.stride = (columns if by_columns else blocks) // 2
        self.pieces = math.gcd(self.blocks, chips)
        self.run = self.blocks // self.pieces

    def part(self, ref, core, piece=None, shard=slice(None)):
        at = core * self.stride + self.start
        first, size = (0, self.blocks) if piece is None else (piece * self.run, self.run)
        if self.by_columns:
            columns = pl.ds(pl.multiple_of(at, 128), self.columns)
            return ref.at[shard, pl.ds(first, size), :, columns]
        return ref.at[shard, pl.ds(at + first, size)]


def chunks_of(arrays, mesh_sizes, want=1, shards_first=()):
    chips = mesh_sizes[1] // 2
    lists = []
    for array, (_, blocks, _, columns) in enumerate(a.shape for a in arrays):
        by_columns = columns % 256 == 0 and columns > blocks * 8
        half = columns // 2 if by_columns else blocks // 2
        unit = 128 if by_columns else 1
        parts = want if half % (want * unit) == 0 else 1
        extent = half // parts
        lists.append(
            [
                Chunk(
                    array, blocks, columns, by_columns, extent, j * extent, chips,
                    array * want + j in shards_first,
                )
                for j in range(parts)
            ]
        )
    return sum(lists, [])


class Place:
    def __init__(self, sizes):
        self.groups, self.reps = sizes
        self.rep, self.mine = lax.axis_index("rep"), lax.axis_index("grp")
        self.chip, self.core = self.rep // 2, lax.rem(self.rep, 2)
        self.chips = self.reps // 2
        self.shard_peers = [
            (self.rep, lax.rem(self.mine + d, self.groups)) for d in range(1, self.groups)
        ]
        self.core_peer = (self.chip * 2 + 1 - self.core, self.mine)

    def piece(self, chunk):
        return lax.rem(self.chip, chunk.pieces)

    def mate(self, chunk, step):
        piece = self.piece(chunk)
        return self.chip - piece + lax.rem(piece + step, chunk.pieces)

    def at(self, chip):
        return (chip * 2 + self.core, self.mine)


class Gather:
    def __init__(self, chunks, sizes, ins, vec_in, outs, vec_out, sems):
        self.chunks, self.place = chunks, Place(sizes)
        self.ins, self.outs, self.vec_in, self.vec_out = ins, outs, vec_in, vec_out
        self.own_sem, self.vec_own_sem = sems[:2]
        self.vec_sems, self.shard_sems, self.chip_sems, self.core_sems = (
            sems[2 + 2 * i : 4 + 2 * i] for i in range(4)
        )

    @staticmethod
    def semaphores(chunks, sizes):
        groups = sizes[0]
        most = max(c.pieces for c in chunks)
        count = len(chunks)
        return (
            [pltpu.SemaphoreType.DMA((count,)), pltpu.SemaphoreType.DMA]
            + dma_pair(groups - 1)
            + dma_pair(count, groups - 1)
            + dma_pair(count, max(most - 1, 1))
            + dma_pair(count)
        )

    def shards(self, i):
        chunk, place = self.chunks[i], self.place
        piece = place.piece(chunk)
        src = chunk.part(self.ins[chunk.array], place.core, piece, 0)
        dst = chunk.part(self.outs[chunk.array], place.core, piece, place.mine)
        return [
            transfer(src, dst, self.shard_sems, (i, d), t)
            for d, t in enumerate(place.shard_peers)
        ]

    def own(self, i):
        chunk, place = self.chunks[i], self.place
        piece = place.piece(chunk)
        src = chunk.part(self.ins[chunk.array], place.core, piece, 0)
        dst = chunk.part(self.outs[chunk.array], place.core, piece, place.mine)
        return pltpu.make_async_copy(src, dst, self.own_sem.at[i])

    def vectors(self):
        return [
            transfer(self.vec_in.at[0], self.vec_out.at[self.place.mine], self.vec_sems, d, t)
            for d, t in enumerate(self.place.shard_peers)
        ]

    def vector_own(self):
        return pltpu.make_async_copy(
            self.vec_in.at[0], self.vec_out.at[self.place.mine], self.vec_own_sem
        )

    def chips(self, i):
        chunk, place = self.chunks[i], self.place
        block = chunk.part(self.outs[chunk.array], place.core, place.piece(chunk))
        return [
            transfer(block, block, self.chip_sems, (i, e - 1), place.at(place.mate(chunk, e)))
            for e in range(1, chunk.pieces)
        ]

    def cores(self, i):
        chunk, place = self.chunks[i], self.place
        block = chunk.part(self.outs[chunk.array], place.core)
        return [transfer(block, block, self.core_sems, i, place.core_peer)]

    def greet(self):
        place = self.place
        most = max(self.chunks, key=lambda c: c.pieces)
        greet(
            place.shard_peers
            + [place.at(place.mate(most, e)) for e in range(1, most.pieces)]
            + [place.core_peer]
        )

    def begin(self):
        for i in range(len(self.chunks)):
            start(self.shards(i))
            self.own(i).start()
        if self.vec_in is not None:
            start(self.vectors())
            self.vector_own().start()

    def all_to_chips(self):
        for i in range(len(self.chunks)):
            self.to_chips(i)

    def all_to_cores(self):
        for i in range(len(self.chunks)):
            self.to_cores(i)

    def to_chips(self, i):
        self.own(i).wait()
        arrive(self.shards(i))
        start(self.chips(i))

    def to_cores(self, i):
        arrive(self.chips(i))
        start(self.cores(i))

    def finish(self):
        every = range(len(self.chunks))
        for i in every:
            arrive(self.cores(i))
        if self.vec_in is not None:
            arrive(self.vectors())
            self.vector_own().wait()
            for copy in self.vectors():
                copy.wait_send()
        for i in every:
            for copy in self.shards(i) + self.chips(i) + self.cores(i):
                copy.wait_send()


def start(copies):
    for copy in copies:
        copy.start()


def arrive(copies):
    for copy in copies:
        copy.wait_recv()


def gather_kernel(chunks, sizes, *refs):
    work = Gather(chunks, sizes, refs[:1], refs[1], refs[2:3], refs[3], refs[4:])
    work.greet()
    work.begin()
    work.all_to_chips()
    work.all_to_cores()
    work.finish()


def dma_pair(*shape):
    return [pltpu.SemaphoreType.DMA(shape), pltpu.SemaphoreType.DMA(shape)]


VMEM_SPEC = pl.BlockSpec(memory_space=pltpu.VMEM)
ANY_SPEC = pl.BlockSpec(memory_space=pl.ANY)


def gathered_shapes(shards, groups):
    return [jax.ShapeDtypeStruct((groups,) + s.shape[1:], s.dtype) for s in shards]


def gather(shard, vec, sizes, collective_id):
    chunks = chunks_of([shard], sizes, 2)
    return pl.pallas_call(
        functools.partial(gather_kernel, chunks, sizes),
        name="gather_params",
        out_shape=gathered_shapes([shard, vec], sizes[0]),
        in_specs=[VMEM_SPEC] * 2,
        out_specs=[VMEM_SPEC] * 2,
        scratch_shapes=Gather.semaphores(chunks, sizes),
        compiler_params=pltpu.CompilerParams(
            collective_id=collective_id, has_side_effects=True, vmem_limit_bytes=40 * 2**20
        ),
    )(shard, vec)


def add_up(first, rest):
    total = first.astype(F32)
    for term in rest:
        total = total + term.astype(F32)
    return total


class Reduce:
    def __init__(self, chunks, sizes, ins, vec_in, outs, vec_out, scratch, vec_along=True):
        self.vec_along = vec_along and vec_in is not None
        count = len(chunks)
        self.chunks, self.place = chunks, Place(sizes)
        self.ins, self.vec_in, self.outs, self.vec_out = ins, vec_in, outs, vec_out
        self.core_sum, self.from_chips, self.chip_sum, self.from_shards = (
            scratch[i * count : (i + 1) * count] for i in range(4)
        )
        sems = scratch[4 * count :]
        names = ("core_sems", "chip_sems", "shard_sems", "spread_sems", "join_sems")
        for i, name in enumerate(names):
            setattr(self, name, sems[2 * i : 2 * i + 2])
        if vec_in is not None:
            self.vec_sems = sems[10:12]
            self.vec_parts, self.vec_held = sems[12:]

    @staticmethod
    def scratch(chunks, sizes, vec_shape):
        groups, reps = sizes
        chips, count = reps // 2, len(chunks)
        most = max(c.pieces for c in chunks)
        shapes = [(groups, c.blocks, 8, c.columns) for c in chunks]
        for lead in ("chips", "sum", "shards"):
            for c in chunks:
                piece, block = (c.run, 8, c.columns), (c.blocks, 8, c.columns)
                shapes.append(
                    {
                        "chips": (chips - 1,) + (piece if c.shards_first else (groups,) + piece),
                        "sum": block if c.shards_first else (groups,) + piece,
                        "shards": (groups - 1,) + (block if c.shards_first else piece),
                    }[lead]
                )
        made = (
            [pltpu.VMEM(s, BF16) for s in shapes]
            + dma_pair(count)
            + dma_pair(count, chips - 1)
            + dma_pair(count, groups - 1)
            + dma_pair(count, max(most - 1, 1))
            + dma_pair(count)
        )
        if vec_shape is not None:
            terms = chips + groups - 1
            made += dma_pair(terms)
            made += [pltpu.VMEM((terms,) + vec_shape, F32), pltpu.VMEM((2,) + vec_shape, F32)]
        return made

    def chip_ids(self):
        place = self.place
        return [lax.rem(place.chip + e, place.chips) for e in range(1, place.chips)]

    def cores(self, i):
        chunk, place = self.chunks[i], self.place
        src = chunk.part(self.ins[chunk.array], 1 - place.core)
        return [transfer(src, self.core_sum[i], self.core_sems, i, place.core_peer)]

    def chips(self, i):
        chunk, copies = self.chunks[i], []
        for e, chip in enumerate(self.chip_ids()):
            piece = lax.rem(chip, chunk.pieces)
            run = pl.ds(piece * chunk.run, chunk.run)
            src = self.chip_sum[i].at[run] if chunk.shards_first else self.core_sum[i].at[:, run]
            dst = self.from_chips[i].at[e]
            copies.append(transfer(src, dst, self.chip_sems, (i, e), self.place.at(chip)))
        return copies

    def shards(self, i):
        place = self.place
        source = self.core_sum[i] if self.chunks[i].shards_first else self.chip_sum[i]
        return [
            transfer(
                source.at[lax.rem(place.mine + d + 1, place.groups)],
                self.from_shards[i].at[d],
                self.shard_sems,
                (i, d),
                target,
            )
            for d, target in enumerate(place.shard_peers)
        ]

    def spread(self, i):
        chunk, place = self.chunks[i], self.place
        block = chunk.part(self.outs[chunk.array], place.core, place.piece(chunk), 0)
        return [
            transfer(block, block, self.spread_sems, (i, e - 1), place.at(place.mate(chunk, e)))
            for e in range(1, chunk.pieces)
        ]

    def join(self, i):
        chunk, place = self.chunks[i], self.place
        block = chunk.part(self.outs[chunk.array], place.core, None, 0)
        return [transfer(block, block, self.join_sems, i, place.core_peer)]

    def vec_cores(self):
        return [transfer(self.vec_in, self.vec_parts.at[0], self.vec_sems, 0, self.place.core_peer)]

    def vec_chips(self):
        return [
            transfer(
                self.vec_held.at[0],
                self.vec_parts.at[1 + e],
                self.vec_sems,
                1 + e,
                self.place.at(chip),
            )
            for e, chip in enumerate(self.chip_ids())
        ]

    def vec_shards(self):
        chips = self.place.chips
        return [
            transfer(
                self.vec_held.at[1],
                self.vec_parts.at[chips + d],
                self.vec_sems,
                chips + d,
                target,
            )
            for d, target in enumerate(self.place.shard_peers)
        ]

    def greet(self):
        place = self.place
        greet(
            place.shard_peers + [place.at(c) for c in self.chip_ids()] + [place.core_peer]
        )

    def begin(self):
        for i in range(len(self.chunks)):
            start(self.cores(i))
        if self.vec_along:
            self.vec_begin()

    def vec_begin(self):
        start(self.vec_cores())

    def all_to_chips(self):
        for i in range(len(self.chunks)):
            self.to_chips(i)
        if self.vec_along:
            self.vec_to_chips()

    def all_to_shards(self):
        for i in range(len(self.chunks)):
            self.to_shards(i)
        if self.vec_along:
            self.vec_to_shards()

    def all_to_spread(self):
        for i in range(len(self.chunks)):
            self.to_spread(i)
        if self.vec_along:
            self.vec_end()

    def all_to_join(self):
        for i in range(len(self.chunks)):
            self.to_join(i)

    def to_chips(self, i):
        chunk = self.chunks[i]
        own = chunk.part(self.ins[chunk.array], self.place.core)[...]
        arrive(self.cores(i))
        self.core_sum[i][...] = own + self.core_sum[i][...]
        start(self.shards(i) if chunk.shards_first else self.chips(i))

    def vec_to_chips(self):
        arrive(self.vec_cores())
        self.vec_held[0] = self.vec_in[...] + self.vec_parts[0]
        start(self.vec_chips())

    def to_shards(self, i):
        chunk = self.chunks[i]
        piece = self.place.piece(chunk)
        if chunk.shards_first:
            own, copies, terms = self.core_sum[i][self.place.mine], self.shards(i), self.from_shards[i]
        else:
            own = self.core_sum[i][:, pl.ds(piece * chunk.run, chunk.run)]
            copies, terms = self.chips(i), self.from_chips[i]
        arrive(copies)
        total = add_up(own, [terms[e] for e in range(len(copies))])
        self.chip_sum[i][...] = total.astype(BF16)
        start(self.chips(i) if chunk.shards_first else self.shards(i))

    def vec_to_shards(self):
        copies = self.vec_chips()
        arrive(copies)
        self.vec_held[1] = add_up(
            self.vec_held[0], [self.vec_parts[1 + e] for e in range(len(copies))]
        )
        start(self.vec_shards())

    def to_spread(self, i):
        chunk, place = self.chunks[i], self.place
        if chunk.shards_first:
            own = self.chip_sum[i][pl.ds(place.piece(chunk) * chunk.run, chunk.run)]
            copies, terms = self.chips(i), self.from_chips[i]
        else:
            own, copies, terms = self.chip_sum[i][place.mine], self.shards(i), self.from_shards[i]
        arrive(copies)
        total = add_up(own, [terms[d] for d in range(len(copies))])
        block = chunk.part(self.outs[chunk.array], place.core, place.piece(chunk), 0)
        block[...] = total.astype(BF16)
        start(self.spread(i))

    def vec_end(self):
        copies = self.vec_shards()
        arrive(copies)
        self.vec_out[...] = add_up(
            self.vec_held[1], [self.vec_parts[self.place.chips + d] for d in range(len(copies))]
        )

    def to_join(self, i):
        arrive(self.spread(i))
        start(self.join(i))

    def finish(self):
        every = range(len(self.chunks))
        for i in every:
            arrive(self.join(i))
        copies = []
        if self.vec_in is not None:
            copies = self.vec_cores() + self.vec_chips() + self.vec_shards()
        for i in every:
            copies += self.cores(i) + self.chips(i) + self.shards(i)
            copies += self.spread(i) + self.join(i)
        for copy in copies:
            copy.wait_send()


def on_device(
    reps,
    images,
    cotangent,
    ln1_gain,
    ln1_bias,
    w_qkv,
    q_bias,
    v_bias,
    w_proj,
    proj_bias,
    ln2_gain,
    ln2_bias,
    w_up,
    up_bias,
    w_down,
    down_bias,
):
    groups = lax.axis_size("grp")
    sizes = (groups, reps)
    layers, part = ln1_gain.shape
    width = part * groups
    hidden_part = up_bias.shape[1]
    plan = Plan(images.shape, hidden_part * groups)
    vectors = [ln1_gain, ln1_bias, q_bias, v_bias, proj_bias, ln2_gain, ln2_bias, down_bias]
    extra = hidden_part // part
    packed = jnp.stack(vectors, axis=1)
    packed = jnp.concatenate([packed, up_bias.reshape(layers, extra, part)], axis=1)
    packed = packed.astype(F32)
    joined = jnp.concatenate([w_qkv, w_proj], axis=2)

    def shards_of(layer):
        return [m[layer].reshape(1, -1, 8, m.shape[2]) for m in (joined, w_up, w_down)]

    def unpack(vecs):
        vectors = vecs[:, :VECTORS].transpose(1, 0, 2).reshape(VECTORS, width)
        up = vecs[:, VECTORS:].reshape(extra, width)
        rest = plan.vec_rows - VECTORS - extra
        return jnp.concatenate([vectors, up, jnp.zeros((rest, width), F32)], axis=0)

    shards0, shards1 = shards_of(0), shards_of(1)
    first_matrix, vecs0 = gather(shards0[0], packed[0][None], sizes, 0)
    first_matrix, vecs0 = first_matrix.reshape(width, -1), unpack(vecs0)
    hidden, keeps, mlp0, gathered = plan.first(
        images, first_matrix, vecs0, shards0[1:], shards1 + [packed[1][None]], sizes, 1
    )
    weights1 = [g.reshape(-1, g.shape[3]) for g in gathered[:3]]
    encoded, flowing, grads1 = plan.middle(hidden, cotangent, weights1, unpack(gathered[3]))
    blocks = [g.reshape(groups, -1, 8, g.shape[1]) for g in grads1[:3]] + [grads1[3]]
    images_grad, sums, small0, small1 = plan.last(
        flowing, images, [first_matrix] + list(mlp0), vecs0, keeps, blocks, sizes, 2
    )
    full = [x.reshape(layers, -1, x.shape[3]) for x in sums]
    small = jnp.stack([small0, small1])
    me = lax.axis_index("grp")
    vec_out = lax.dynamic_slice_in_dim(small[:, :VECTORS], me * part, part, axis=2)
    up_out = small[:, VECTORS : VECTORS + extra].reshape(layers, -1)
    up_out = lax.dynamic_slice_in_dim(up_out, me * hidden_part, hidden_part, axis=1)
    return (
        encoded,
        images_grad,
        vec_out[:, G1],
        vec_out[:, B1],
        full[0],
        vec_out[:, QB],
        vec_out[:, VB],
        full[1],
        vec_out[:, PB],
        vec_out[:, G2],
        vec_out[:, B2],
        full[2],
        up_out,
        full[3],
        vec_out[:, DB],
    )


def solution(mesh):
    batch = P(("rep", "grp"), None, None)
    vector = P(None, "grp")
    matrix = P(None, "grp", None)
    params = (
        vector,
        vector,
        matrix,
        vector,
        vector,
        matrix,
        vector,
        vector,
        vector,
        matrix,
        vector,
        matrix,
        vector,
    )
    specs = (batch, batch) + params
    return jax.shard_map(
        functools.partial(on_device, mesh.shape["rep"]), mesh=mesh, in_specs=specs, out_specs=specs, check_vma=False
    )
```

```python
import functools
import math

import jax
import jax.numpy as jnp
from jax import lax
from jax.experimental import pallas as pl
from jax.experimental.pallas import tpu as pltpu
from jax.sharding import PartitionSpec as P

HEAD_DIM = 64
PAIR = 2 * HEAD_DIM
EPS = 1e-06
INV_ROOT_TWO = 0.7071067811865476
INV_ROOT_TAU = 0.3989422804014327
MASKED = -1e30
F32 = jnp.float32
BF16 = jnp.bfloat16

VECTORS = 8
G1, B1, QB, VB, PB, G2, B2, DB = range(VECTORS)


def dot(left, right):
    return jnp.dot(left, right, preferred_element_type=F32)


def dot_nt(left, right):
    return lax.dot_general(
        left, right, (((1,), (1,)), ((), ())), preferred_element_type=F32
    )


def col_sum(rows):
    return jnp.sum(rows, axis=0, keepdims=True)


def norm(rows):
    mean = jnp.mean(rows, axis=-1, keepdims=True)
    centered = rows - mean
    inv = lax.rsqrt(jnp.mean(centered * centered, axis=-1, keepdims=True) + EPS)
    return centered * inv, inv


def norm_backward(grad, normed, inv, gain):
    scaled = grad * gain
    return inv * (
        scaled
        - jnp.mean(scaled, axis=-1, keepdims=True)
        - normed * jnp.mean(scaled * normed, axis=-1, keepdims=True)
    )


def attn_forward(qkv, keep, image, seq, pad):
    width = qkv.shape[1] // 3
    base = image * pad
    rows = pl.ds(base, pad)
    value_t = qkv[rows, pl.ds(2 * width, width)].T
    lane = lax.broadcasted_iota(jnp.int32, (1, PAIR), 1)
    halves = [(lane < HEAD_DIM).astype(F32).astype(BF16), (lane >= HEAD_DIM).astype(F32).astype(BF16)]
    full = seq // 8 * 8
    for pair in range(width // PAIR):
        queries = qkv[rows, pl.ds(pair * PAIR, PAIR)]
        keys = qkv[rows, pl.ds(width + pair * PAIR, PAIR)]
        for half in range(2):
            head = 2 * pair + half
            scores = dot_nt(keys * halves[half], queries)
            parts = [scores[:full]]
            if full < seq:
                tail = scores[full : full + 8]
                row = lax.broadcasted_iota(jnp.int32, tail.shape, 0)
                parts.append(jnp.where(row < seq - full, tail, MASKED))
            scores = jnp.concatenate(parts, axis=0)
            top = jnp.max(scores, axis=0, keepdims=True)
            raised = jnp.exp(scores - top)
            probs = raised * (1.0 / col_sum(raised))
            rest = pad - probs.shape[0]
            if rest:
                probs = jnp.concatenate([probs, jnp.zeros((rest, pad), F32)], axis=0)
            keep["probs"][image, head] = probs
            context = dot(value_t[head * HEAD_DIM : (head + 1) * HEAD_DIM], probs.astype(BF16))
            keep["context"][image, pl.ds(head * HEAD_DIM, HEAD_DIM), :] = context.astype(BF16)


def split_attention(packed):
    width = packed.shape[0]
    return packed.at[:, pl.ds(0, 3 * width)], packed.at[:, pl.ds(3 * width, width)]


def up_bias_of(vecs, hidden_width):
    rows = hidden_width // vecs.shape[1]
    return jnp.concatenate([vecs[VECTORS + i : VECTORS + i + 1] for i in range(rows)], axis=1)


def attention_part(hidden, packed, vecs, keep, images, seq, pad):
    w_qkv, w_proj = split_attention(packed)
    width = hidden.shape[1]
    normed, _ = norm(hidden)
    rows_in = (normed * vecs[G1 : G1 + 1] + vecs[B1 : B1 + 1]).astype(BF16)
    qkv = keep["qkv"]
    projected = dot(rows_in, w_qkv[...])
    qkv[:, :width] = (projected[:, :width] + vecs[QB : QB + 1]).astype(BF16) * jnp.asarray(
        HEAD_DIM**-0.5, BF16
    )
    qkv[:, width : 2 * width] = projected[:, width : 2 * width].astype(BF16)
    qkv[:, 2 * width :] = (projected[:, 2 * width :] + vecs[VB : VB + 1]).astype(BF16)
    for image in range(images):
        attn_forward(qkv, keep, image, seq, pad)
    context = jnp.concatenate([keep["context"][image].T for image in range(images)], axis=0)
    mixed = hidden + dot(context, w_proj[...]) + vecs[PB : PB + 1]
    keep["mixed"][...] = mixed
    return mixed


def mlp_part(mixed, w_up, w_down, vecs, keep):
    up_bias = up_bias_of(vecs, w_down.shape[0])
    normed, _ = norm(mixed)
    rows_mid = (normed * vecs[G2 : G2 + 1] + vecs[B2 : B2 + 1]).astype(BF16)
    upward = dot(rows_mid, w_up[...]) + up_bias
    cumul = 0.5 * (1.0 + lax.erf(upward * INV_ROOT_TWO))
    keep["active"][...] = (upward * cumul).astype(BF16)
    slope = cumul + upward * jnp.exp(-0.5 * upward * upward) * INV_ROOT_TAU
    keep["slope"][...] = slope.astype(keep["slope"].dtype)
    return mixed + dot(keep["active"][...], w_down[...]) + vecs[DB : DB + 1]


def attn_backward(qkv, keep, context_grad, joint, vec_grads, image, pad):
    width = qkv.shape[1] // 3
    rows = pl.ds(image * pad, pad)
    keys_t = qkv[rows, pl.ds(width, width)].T
    lane = lax.broadcasted_iota(jnp.int32, (1, PAIR), 1)
    low = lax.broadcasted_iota(jnp.int32, (pad, PAIR), 1) < HEAD_DIM
    halves = [(lane < HEAD_DIM).astype(F32).astype(BF16), (lane >= HEAD_DIM).astype(F32).astype(BF16)]
    query_parts = []
    for pair in range(width // PAIR):
        queries = qkv[rows, pl.ds(pair * PAIR, PAIR)]
        values = qkv[rows, pl.ds(2 * width + pair * PAIR, PAIR)]
        ctx = context_grad[rows, pl.ds(pair * PAIR, PAIR)]
        key_parts, value_parts = [], []
        for half in range(2):
            head = 2 * pair + half
            probs = keep["probs"][image, head]
            prob_grad = dot_nt(values * halves[half], ctx)
            value_parts.append(dot(probs.astype(BF16), ctx))
            row_dot = col_sum(probs * prob_grad)
            score_grad = (probs * (prob_grad - row_dot)).astype(BF16)
            key_parts.append(dot(score_grad, queries))
            query_parts.append(dot(keys_t[head * HEAD_DIM : (head + 1) * HEAD_DIM], score_grad))
        key_grad = jnp.where(low, key_parts[0], key_parts[1])
        value_grad = jnp.where(low, value_parts[0], value_parts[1])
        joint[rows, pl.ds(width + pair * PAIR, PAIR)] = key_grad.astype(BF16)
        joint[rows, pl.ds(2 * width + pair * PAIR, PAIR)] = value_grad.astype(BF16)
        vec_grads[VB : VB + 1, pl.ds(pair * PAIR, PAIR)] += col_sum(value_grad)
    query_grad = jnp.concatenate(query_parts, axis=0).T * HEAD_DIM**-0.5
    joint[rows, pl.ds(0, width)] = query_grad.astype(BF16)
    vec_grads[QB : QB + 1, :] += col_sum(query_grad)


def mlp_backward(out_grad, w_up, w_down, vecs, keep, acc):
    _, _, g_up, g_down, vec_grads, up_bias_grad = acc[:6]
    rounded = out_grad.astype(BF16)
    vec_grads[DB : DB + 1, :] += col_sum(out_grad)
    g_down[...] += dot(rounded.T, keep["active"][...])
    up_grad = dot_nt(rounded, w_down[...]) * keep["slope"][...].astype(F32)
    up_bias_grad[...] += col_sum(up_grad)
    up_rounded = up_grad.astype(BF16)
    normed, inv = norm(keep["mixed"][...])
    gain = vecs[G2 : G2 + 1]
    rows_mid = (normed * gain + vecs[B2 : B2 + 1]).astype(BF16)
    g_up[...] += dot(rows_mid.T, up_rounded)
    mid_grad = dot_nt(up_rounded, w_up[...])
    vec_grads[G2 : G2 + 1, :] += col_sum(mid_grad * normed)
    vec_grads[B2 : B2 + 1, :] += col_sum(mid_grad)
    return out_grad + norm_backward(mid_grad, normed, inv, gain)


def attention_backward(mixed_grad, hidden, packed, vecs, keep, acc, joint, images, pad):
    _, w_proj = split_attention(packed)
    g_qkv, g_proj, _, _, vec_grads, _, context_grad = acc
    vec_grads[PB : PB + 1, :] += col_sum(mixed_grad)
    mixed_rounded = mixed_grad.astype(BF16)
    part = g_proj[...]
    for image in range(images):
        part += dot(keep["context"][image], mixed_rounded[image * pad : (image + 1) * pad])
    g_proj[...] = part
    context_grad[...] = dot_nt(mixed_rounded, w_proj[...]).astype(BF16)
    for image in range(images):
        attn_backward(keep["qkv"], keep, context_grad, joint, vec_grads, image, pad)
    normed, _ = norm(hidden)
    rows_in = (normed * vecs[G1 : G1 + 1] + vecs[B1 : B1 + 1]).astype(BF16)
    g_qkv[...] += dot(rows_in.T, joint[...])


def input_backward(mixed_grad, hidden, packed, vecs, vec_grads, joint):
    w_qkv, _ = split_attention(packed)
    normed, inv = norm(hidden)
    in_grad = dot_nt(joint[...], w_qkv[...])
    vec_grads[G1 : G1 + 1, :] += col_sum(in_grad * normed)
    vec_grads[B1 : B1 + 1, :] += col_sum(in_grad)
    return mixed_grad + norm_backward(in_grad, normed, inv, vecs[G1 : G1 + 1])


def load_padded(ref, buf, pad):
    images, seq, width = ref.shape
    for image in range(images):
        buf[pl.ds(image * pad, seq), :] = ref[image].astype(F32)
        if pad > seq:
            buf[pl.ds(image * pad + seq, pad - seq), :] = jnp.zeros((pad - seq, width), F32)


def store_images(ref, rows, pad):
    images, seq, _ = ref.shape
    for image in range(images):
        ref[image] = rows[image * pad : image * pad + seq].astype(ref.dtype)


KEEP = ("qkv", "probs", "context", "mixed", "active", "slope")


def keep_shapes(images, pad, width, hidden_width):
    heads = width // HEAD_DIM
    return {
        "qkv": ((images * pad, 3 * width), BF16),
        "probs": ((images, heads, pad, pad), F32),
        "context": ((images, width, pad), BF16),
        "mixed": ((images * pad, width), F32),
        "active": ((images * pad, hidden_width), BF16),
        "slope": ((images * pad, hidden_width), F32),
    }


def init_grads(acc):
    @pl.when(pl.program_id(0) == 0)
    def _():
        for ref in acc[:6]:
            ref[...] = jnp.zeros_like(ref)


def flush_vectors(acc, vecs):
    vec_grads, up_bias_grad = acc[4:6]
    width = vecs.shape[1]
    extra = up_bias_grad.shape[1] // width
    vecs[:VECTORS, :] = vec_grads[...]
    for i in range(extra):
        vecs[VECTORS + i : VECTORS + i + 1, :] = up_bias_grad[:, i * width : (i + 1) * width]
    rest = vecs.shape[0] - VECTORS - extra
    if rest:
        vecs[VECTORS + extra :, :] = jnp.zeros((rest, width), F32)


def step_at(step):
    return pl.when(pl.program_id(0) == step)


def first_kernel(sizes, steps, mesh_sizes, chunks, *refs):
    group, seq, pad = sizes
    images, packed, vecs = refs[:3]
    shards0, shards1 = refs[3:5], refs[5:9]
    out = refs[9]
    keep = dict(zip(KEEP, refs[10:16]))
    mlp_out = refs[16:18]
    full1 = refs[18:22]
    buf, mixed_rows = refs[22:24]
    landed = refs[24:26]
    rest = refs[26:]
    half = len(rest) // 2
    now = Gather(chunks[0], mesh_sizes, shards0, None, landed, None, rest[:half])
    later = Gather(
        chunks[1], mesh_sizes, shards1[:3], shards1[3], full1[:3], full1[3], rest[half:]
    )
    step = pl.program_id(0)
    rows = group * pad

    @step_at(0)
    def _():
        now.greet()
        now.begin()
        later.begin()

    @step_at(2 * steps // 5)
    def _():
        now.all_to_chips()

    @pl.when(step < steps)
    def _():
        load_padded(images, buf, pad)
        mixed = attention_part(buf[...], packed, vecs, keep, group, seq, pad)
        mixed_rows[pl.ds(pl.multiple_of(step * rows, rows), rows), :] = mixed

    @step_at(4 * steps // 5)
    def _():
        now.to_cores(0)
        later.to_chips(0)
        later.to_chips(1)

    @step_at(steps)
    def _():
        now.to_cores(1)
        now.finish()
        for matrix, source in zip(mlp_out, landed):
            flat = source[...].astype(F32).reshape(matrix.shape)
            matrix[...] = flat.astype(BF16)

    @step_at(steps + 3 * steps // 5)
    def _():
        later.to_chips(2)
        later.to_cores(2)

    @step_at(2 * steps - 1)
    def _():
        later.to_cores(0)
        later.to_cores(1)

    @pl.when(step >= steps)
    def _():
        at = pl.multiple_of((step - steps) * rows, rows)
        mixed = mixed_rows[pl.ds(at, rows), :]
        out[...] = mlp_part(mixed, mlp_out[0], mlp_out[1], vecs, keep)

    @step_at(2 * steps - 1)
    def _():
        later.finish()


def middle_kernel(sizes, *refs):
    group, seq, pad = sizes
    hidden, cotangent, packed, w_up, w_down, vecs, encoded, flowing = refs[:8]
    outs, vec_out = refs[8:11], refs[11]
    keep = dict(zip(KEEP, refs[12:18]))
    acc = refs[18:25]
    joint, buf = refs[25:]
    init_grads(acc)
    mixed = attention_part(hidden[...], packed, vecs, keep, group, seq, pad)
    result = mlp_part(mixed, w_up, w_down, vecs, keep)
    store_images(encoded, result, pad)
    load_padded(cotangent, buf, pad)
    mixed_grad = mlp_backward(buf[...], w_up, w_down, vecs, keep, acc)
    attention_backward(mixed_grad, hidden[...], packed, vecs, keep, acc, joint, group, pad)
    flowing[...] = input_backward(mixed_grad, hidden[...], packed, vecs, acc[4], joint)

    @step_at(pl.num_programs(0) - 1)
    def _():
        g_qkv_out, g_proj_out = split_attention(outs[0])
        g_qkv_out[...] = acc[0][...].astype(BF16)
        g_proj_out[...] = acc[1][...].astype(BF16)
        outs[1][...] = acc[2][...].astype(BF16)
        outs[2][...] = acc[3][...].astype(BF16).T
        flush_vectors(acc, vec_out)


def last_kernel(sizes, steps, mesh_sizes, chunks, counts, *refs):
    group, seq, pad = sizes
    flowing, images, packed, w_up, w_down, vecs = refs[:6]
    keep = dict(zip(KEEP, refs[6:12]))
    grads1, vec1 = refs[12:15], refs[15]
    images_grad, sums, vec_out0, vec_out1 = refs[16], refs[17:21], refs[21], refs[22]
    acc = refs[23:30]
    buf, grad_rows, joint_rows, vec0 = refs[30:34]
    grads0, shares0, shares1 = refs[34:37], refs[37:40], refs[40:43]
    scratch = refs[43:]
    ends = [sum(counts[: i + 1]) for i in range(3)]
    later = Reduce(chunks[0], mesh_sizes, grads1, vec1, shares1, vec_out1, scratch[: ends[0]])
    mlp = Reduce(
        chunks[1], mesh_sizes, grads0[1:], None, shares0[1:], None, scratch[ends[0] : ends[1]]
    )
    tail = Reduce(
        chunks[2],
        mesh_sizes,
        grads0[:1],
        vec0,
        shares0[:1],
        vec_out0,
        scratch[ends[1] :],
        vec_along=False,
    )
    step = pl.program_id(0)
    rows = group * pad
    last = 3 * steps - 1
    three = acc[0].shape[1]

    def rows_at(start):
        return pl.ds(pl.multiple_of((step - start) * rows, rows), rows)

    @step_at(0)
    def _():
        later.greet()
        later.begin()

    @step_at(1 * steps // 5)
    def _():
        later.all_to_chips()

    init_grads(acc)

    @pl.when(step < steps)
    def _():
        grad_rows[rows_at(0), :] = mlp_backward(flowing[...], w_up, w_down, vecs, keep, acc)

    @step_at(steps)
    def _():
        grads0[1][...] = acc[2][...].reshape(grads0[1].shape).astype(BF16)
        grads0[2][...] = acc[3][...].T.reshape(grads0[2].shape).astype(BF16)
        mlp.begin()

    @step_at(steps + 1 * steps // 5)
    def _():
        later.all_to_shards()
        mlp.all_to_chips()

    @step_at(steps + 3 * steps // 5)
    def _():
        later.all_to_spread()

    @step_at(2 * steps - 1)
    def _():
        mlp.all_to_shards()
        later.all_to_join()

    @pl.when((step >= steps) & (step < 2 * steps))
    def _():
        load_padded(images, buf, pad)
        attention_backward(
            grad_rows[rows_at(steps), :],
            buf[...],
            packed,
            vecs,
            keep,
            acc,
            joint_rows.at[rows_at(steps), :],
            group,
            pad,
        )

    @step_at(2 * steps)
    def _():
        shape = grads0[0].shape
        grads0[0][:, :, :, :three] = acc[0][...].reshape(shape[:3] + (three,)).astype(BF16)
        grads0[0][:, :, :, three:] = (
            acc[1][...].reshape(shape[:3] + (shape[3] - three,)).astype(BF16)
        )
        tail.begin()

    @step_at(2 * steps + steps // 5)
    def _():
        tail.all_to_chips()

    @step_at(2 * steps + 2 * steps // 5)
    def _():
        mlp.all_to_spread()

    @step_at(last)
    def _():
        tail.all_to_shards()

    @pl.when(step >= 2 * steps)
    def _():
        load_padded(images, buf, pad)
        result = input_backward(
            grad_rows[rows_at(2 * steps), :],
            buf[...],
            packed,
            vecs,
            acc[4],
            joint_rows.at[rows_at(2 * steps), :],
        )
        store_images(images_grad, result, pad)

    def store_sums(layer, shares):
        sums[0][layer] = shares[0][0, :, :, :three]
        sums[1][layer] = shares[0][0, :, :, three:]

    @step_at(last)
    def _():
        flush_vectors(acc, vec0)
        tail.vec_begin()
        tail.vec_to_chips()
        mlp.all_to_join()
        later.finish()
        store_sums(1, shares1)
        for total, share in zip(sums[2:], shares1[1:]):
            total[1] = share[0]
        tail.vec_to_shards()
        tail.all_to_spread()
        mlp.finish()
        for total, share in zip(sums[2:], shares0[1:]):
            total[0] = share[0]
        tail.all_to_join()
        tail.vec_end()
        tail.finish()
        store_sums(0, shares0)


def whole(shape):
    return pl.BlockSpec(shape, lambda i: (0,) * len(shape), pipeline_mode=pl.Buffered(1))


def rows_spec(shape, steps, start=0, again=False):
    def block(i):
        at = jnp.maximum(i - start, 0)
        return lax.rem(at, steps) if again else jnp.minimum(at, steps - 1)

    return pl.BlockSpec(
        (shape[0] // steps,) + tuple(shape[1:]), lambda i: (block(i),) + (0,) * (len(shape) - 1)
    )


class Plan:
    def __init__(self, images_shape, hidden_width):
        self.count, self.seq, self.width = images_shape
        self.hidden_width = hidden_width
        self.pad = -(-self.seq // 16) * 16
        self.group = 2 if self.count % 2 == 0 else 1
        self.steps = self.count // self.group
        self.rows = self.count * self.pad
        self.keep = keep_shapes(self.count, self.pad, self.width, hidden_width)
        self.keep_block = keep_shapes(self.group, self.pad, self.width, hidden_width)
        self.weight_shapes = [
            (self.width, 3 * self.width),
            (self.width, self.width),
            (self.width, hidden_width),
            (hidden_width, self.width),
        ]
        self.sizes = (self.group, self.seq, self.pad)
        block_rows = self.group * self.pad
        self.buffer = pltpu.VMEM((block_rows, self.width), F32)
        self.acc = [
            pltpu.VMEM(self.weight_shapes[0], F32),
            pltpu.VMEM(self.weight_shapes[1], F32),
            pltpu.VMEM(self.weight_shapes[2], F32),
            pltpu.VMEM((self.width, hidden_width), F32),
            pltpu.VMEM((8, self.width), F32),
            pltpu.VMEM((1, hidden_width), F32),
            pltpu.VMEM((block_rows, self.width), BF16),
        ]
        self.joint = pltpu.VMEM((block_rows, 3 * self.width), BF16)
        self.vec_rows = -(-(VECTORS + hidden_width // self.width) // 8) * 8
        self.packed_shapes = [
            (self.width, 4 * self.width),
            (self.width, hidden_width),
            (hidden_width, self.width),
        ]
        self.vec_shape = (self.vec_rows, self.width)
        self.grad_shapes = [jax.ShapeDtypeStruct(s, BF16) for s in self.packed_shapes] + [
            jax.ShapeDtypeStruct(self.vec_shape, F32)
        ]
        self.params = pltpu.CompilerParams(
            dimension_semantics=("arbitrary",), vmem_limit_bytes=60 * 2**20
        )

    def image_spec(self, start=0, again=False):
        return rows_spec((self.count, self.seq, self.width), self.steps, start, again)

    def state_spec(self, start=0):
        return rows_spec((self.rows, self.width), self.steps, start)

    def param_specs(self):
        return [whole(s) for s in self.packed_shapes + [self.vec_shape]]

    def keep_specs(self, starts):
        return [rows_spec(self.keep[k][0], self.steps, at) for k, at in zip(KEEP, starts)]

    def grad_specs(self):
        return [whole(s.shape) for s in self.grad_shapes]

    def cost(self, layers):
        rows, width, hidden = self.count * self.seq, self.width, self.hidden_width
        flops = 2 * rows * width * (4 * width + 2 * hidden) * layers
        return pl.CostEstimate(
            flops=int(flops), bytes_accessed=int(40 * 2**20), transcendentals=0
        )

    def comm_params(self, collective_id):
        return pltpu.CompilerParams(
            dimension_semantics=("arbitrary",),
            vmem_limit_bytes=67_043_328,
            collective_id=collective_id,
            has_side_effects=True,
        )

    def first(self, images, packed, vecs, shards0, shards1, mesh_sizes, collective_id):
        state = jax.ShapeDtypeStruct((self.rows, self.width), F32)
        keeps = [jax.ShapeDtypeStruct(*self.keep[k]) for k in KEEP]
        mlp = [jax.ShapeDtypeStruct(s, BF16) for s in self.packed_shapes[1:]]
        chunks = [
            chunks_of(shards0, mesh_sizes),
            chunks_of(shards1[:3], mesh_sizes, undivided=(2,)),
        ]
        n = self.steps
        out = pl.pallas_call(
            functools.partial(first_kernel, self.sizes, n, mesh_sizes, chunks),
            name="layer_first",
            out_shape=[state] + keeps + mlp + gathered_shapes(shards1, mesh_sizes[0]),
            grid=(2 * n,),
            in_specs=[self.image_spec(), whole(packed.shape), whole(self.vec_shape)]
            + [ANY_SPEC] * 6,
            out_specs=[self.state_spec(n)]
            + self.keep_specs((0, 0, 0, 0, n, n))
            + [whole(m.shape) for m in mlp]
            + [ANY_SPEC] * 4,
            scratch_shapes=[self.buffer, pltpu.VMEM((self.rows, self.width), F32)]
            + [pltpu.VMEM(s.shape, BF16) for s in gathered_shapes(shards0, mesh_sizes[0])]
            + Gather.semaphores(chunks[0], mesh_sizes)
            + Gather.semaphores(chunks[1], mesh_sizes),
            compiler_params=self.comm_params(collective_id),
            cost_estimate=self.cost(1),
        )(images, packed, vecs, *shards0, *shards1)
        return out[0], out[1:7], out[7:9], out[9:]

    def middle(self, hidden, cotangent, weights, vecs):
        state = jax.ShapeDtypeStruct((self.rows, self.width), F32)
        out = pl.pallas_call(
            functools.partial(middle_kernel, self.sizes),
            name="layer_middle",
            out_shape=[jax.ShapeDtypeStruct(cotangent.shape, BF16), state] + self.grad_shapes,
            grid=(self.steps,),
            in_specs=[self.state_spec(), self.image_spec()] + self.param_specs(),
            out_specs=[self.image_spec(), self.state_spec()] + self.grad_specs(),
            scratch_shapes=[pltpu.VMEM(*self.keep_block[k]) for k in KEEP]
            + self.acc
            + [self.joint, self.buffer],
            compiler_params=self.params,
            cost_estimate=self.cost(3),
        )(hidden, cotangent, *weights, vecs)
        return out[0], out[1], out[2:]

    def last(self, flowing, images, weights, vecs, keeps, grads, mesh_sizes, collective_id):
        groups = mesh_sizes[0]
        whole_grads = [
            jax.ShapeDtypeStruct(g.shape, BF16) for g in grads[:3]
        ]
        chunks = [
            chunks_of(whole_grads, mesh_sizes, 1, (1,)),
            chunks_of(whole_grads[1:], mesh_sizes, 1, ()),
            chunks_of(whole_grads[:1], mesh_sizes, 3, (0,)),
        ]
        shares = [(1,) + g.shape[1:] for g in whole_grads]
        blocks = whole_grads[0].shape[1:3]
        sums = [
            jax.ShapeDtypeStruct((2,) + shape, BF16)
            for shape in (
                blocks + (3 * self.width,),
                blocks + (self.width,),
                whole_grads[1].shape[1:],
                whole_grads[2].shape[1:],
            )
        ]
        vec = jax.ShapeDtypeStruct(self.vec_shape, F32)
        scratch = [
            Reduce.scratch(chunks[0], mesh_sizes, self.vec_shape),
            Reduce.scratch(chunks[1], mesh_sizes, None),
            Reduce.scratch(chunks[2], mesh_sizes, self.vec_shape),
        ]
        n = self.steps
        outs = [jax.ShapeDtypeStruct(images.shape, BF16)] + sums + [vec, vec]
        out = pl.pallas_call(
            functools.partial(
                last_kernel, self.sizes, n, mesh_sizes, chunks, [len(x) for x in scratch]
            ),
            name="layer_last",
            out_shape=outs,
            grid=(3 * n,),
            in_specs=[self.state_spec(), self.image_spec(n, True)]
            + self.param_specs()
            + self.keep_specs((n, n, n, 0, 0, 0))
            + [whole(g.shape) for g in grads],
            out_specs=[self.image_spec(2 * n)] + [whole(o.shape) for o in outs[1:]],
            scratch_shapes=self.acc
            + [
                self.buffer,
                pltpu.VMEM((self.rows, self.width), F32),
                pltpu.VMEM((self.rows, 3 * self.width), BF16),
                pltpu.VMEM(self.vec_shape, F32),
            ]
            + [pltpu.VMEM(g.shape, BF16) for g in whole_grads]
            + [pltpu.VMEM(s, BF16) for s in shares]
            + [pltpu.VMEM(s, BF16) for s in shares]
            + sum(scratch, []),
            compiler_params=self.comm_params(collective_id),
            cost_estimate=self.cost(2),
        )(flowing, images, *weights, vecs, *keeps, *grads)
        return out[0], out[1:5], out[5], out[6]


def greet(targets):
    barrier = pltpu.get_barrier_semaphore()
    for target in targets:
        pl.semaphore_signal(
            barrier, inc=1, device_id=target, device_id_type=pl.DeviceIdType.MESH
        )
    pl.semaphore_wait(barrier, len(targets))


def transfer(src, dst, sems, at, target):
    return pltpu.make_async_remote_copy(
        src_ref=src,
        dst_ref=dst,
        send_sem=sems[0].at[at],
        recv_sem=sems[1].at[at],
        device_id=target,
        device_id_type=pl.DeviceIdType.MESH,
    )


class Chunk:
    def __init__(self, array, blocks, columns, by_columns, extent, start, chips, shards_first):
        self.shards_first = shards_first
        self.array, self.by_columns, self.start, self.extent = array, by_columns, start, extent
        self.blocks = blocks if by_columns else extent
        self.columns = extent if by_columns else columns
        self.stride = (columns if by_columns else blocks) // 2
        self.pieces = math.gcd(self.blocks, chips)
        self.run = self.blocks // self.pieces

    def part(self, ref, core, piece=None, shard=slice(None)):
        at = core * self.stride + self.start
        first, size = (0, self.blocks) if piece is None else (piece * self.run, self.run)
        if self.by_columns:
            columns = pl.ds(pl.multiple_of(at, 128), self.columns)
            return ref.at[shard, pl.ds(first, size), :, columns]
        return ref.at[shard, pl.ds(at + first, size)]


def chunks_of(arrays, mesh_sizes, want=1, shards_first=(), undivided=()):
    chips = mesh_sizes[1] // 2
    lists = []
    for array, (_, blocks, _, columns) in enumerate(a.shape for a in arrays):
        by_columns = columns % 256 == 0 and columns > blocks * 8
        half = columns // 2 if by_columns else blocks // 2
        unit = 128 if by_columns else 1
        parts = want if half % (want * unit) == 0 else 1
        extent = half // parts
        lists.append(
            [
                Chunk(
                    array, blocks, columns, by_columns, extent, j * extent,
                    1 if array in undivided else chips,
                    array * want + j in shards_first,
                )
                for j in range(parts)
            ]
        )
    return sum(lists, [])


class Place:
    def __init__(self, sizes):
        self.groups, self.reps = sizes
        self.rep, self.mine = lax.axis_index("rep"), lax.axis_index("grp")
        self.chip, self.core = self.rep // 2, lax.rem(self.rep, 2)
        self.chips = self.reps // 2
        self.shard_peers = [
            (self.rep, lax.rem(self.mine + d, self.groups)) for d in range(1, self.groups)
        ]
        self.core_peer = (self.chip * 2 + 1 - self.core, self.mine)

    def piece(self, chunk):
        return lax.rem(self.chip, chunk.pieces)

    def mate(self, chunk, step):
        piece = self.piece(chunk)
        return self.chip - piece + lax.rem(piece + step, chunk.pieces)

    def at(self, chip):
        return (chip * 2 + self.core, self.mine)


class Gather:
    def __init__(self, chunks, sizes, ins, vec_in, outs, vec_out, sems):
        self.chunks, self.place = chunks, Place(sizes)
        self.ins, self.outs, self.vec_in, self.vec_out = ins, outs, vec_in, vec_out
        self.own_sem, self.vec_own_sem = sems[:2]
        self.vec_sems, self.shard_sems, self.chip_sems, self.core_sems = (
            sems[2 + 2 * i : 4 + 2 * i] for i in range(4)
        )

    @staticmethod
    def semaphores(chunks, sizes):
        groups = sizes[0]
        most = max(c.pieces for c in chunks)
        count = len(chunks)
        return (
            [pltpu.SemaphoreType.DMA((count,)), pltpu.SemaphoreType.DMA]
            + dma_pair(groups - 1)
            + dma_pair(count, groups - 1)
            + dma_pair(count, max(most - 1, 1))
            + dma_pair(count)
        )

    def shards(self, i):
        chunk, place = self.chunks[i], self.place
        piece = place.piece(chunk)
        src = chunk.part(self.ins[chunk.array], place.core, piece, 0)
        dst = chunk.part(self.outs[chunk.array], place.core, piece, place.mine)
        return [
            transfer(src, dst, self.shard_sems, (i, d), t)
            for d, t in enumerate(place.shard_peers)
        ]

    def own(self, i):
        chunk, place = self.chunks[i], self.place
        piece = place.piece(chunk)
        src = chunk.part(self.ins[chunk.array], place.core, piece, 0)
        dst = chunk.part(self.outs[chunk.array], place.core, piece, place.mine)
        return pltpu.make_async_copy(src, dst, self.own_sem.at[i])

    def vectors(self):
        return [
            transfer(self.vec_in.at[0], self.vec_out.at[self.place.mine], self.vec_sems, d, t)
            for d, t in enumerate(self.place.shard_peers)
        ]

    def vector_own(self):
        return pltpu.make_async_copy(
            self.vec_in.at[0], self.vec_out.at[self.place.mine], self.vec_own_sem
        )

    def chips(self, i):
        chunk, place = self.chunks[i], self.place
        block = chunk.part(self.outs[chunk.array], place.core, place.piece(chunk))
        return [
            transfer(block, block, self.chip_sems, (i, e - 1), place.at(place.mate(chunk, e)))
            for e in range(1, chunk.pieces)
        ]

    def cores(self, i):
        chunk, place = self.chunks[i], self.place
        block = chunk.part(self.outs[chunk.array], place.core)
        return [transfer(block, block, self.core_sems, i, place.core_peer)]

    def greet(self):
        place = self.place
        most = max(self.chunks, key=lambda c: c.pieces)
        greet(
            place.shard_peers
            + [place.at(place.mate(most, e)) for e in range(1, most.pieces)]
            + [place.core_peer]
        )

    def begin(self):
        for i in range(len(self.chunks)):
            start(self.shards(i))
            self.own(i).start()
        if self.vec_in is not None:
            start(self.vectors())
            self.vector_own().start()

    def all_to_chips(self):
        for i in range(len(self.chunks)):
            self.to_chips(i)

    def all_to_cores(self):
        for i in range(len(self.chunks)):
            self.to_cores(i)

    def to_chips(self, i):
        self.own(i).wait()
        arrive(self.shards(i))
        start(self.chips(i))

    def to_cores(self, i):
        arrive(self.chips(i))
        start(self.cores(i))

    def finish(self):
        every = range(len(self.chunks))
        for i in every:
            arrive(self.cores(i))
        if self.vec_in is not None:
            arrive(self.vectors())
            self.vector_own().wait()
            for copy in self.vectors():
                copy.wait_send()
        for i in every:
            for copy in self.shards(i) + self.chips(i) + self.cores(i):
                copy.wait_send()


def start(copies):
    for copy in copies:
        copy.start()


def arrive(copies):
    for copy in copies:
        copy.wait_recv()


def gather_kernel(chunks, sizes, *refs):
    work = Gather(chunks, sizes, refs[:1], refs[1], refs[2:3], refs[3], refs[4:])
    work.greet()
    work.begin()
    work.all_to_chips()
    work.all_to_cores()
    work.finish()


def dma_pair(*shape):
    return [pltpu.SemaphoreType.DMA(shape), pltpu.SemaphoreType.DMA(shape)]


VMEM_SPEC = pl.BlockSpec(memory_space=pltpu.VMEM)
ANY_SPEC = pl.BlockSpec(memory_space=pl.ANY)


def gathered_shapes(shards, groups):
    return [jax.ShapeDtypeStruct((groups,) + s.shape[1:], s.dtype) for s in shards]


def gather(shard, vec, sizes, collective_id):
    chunks = chunks_of([shard], sizes, 2)
    return pl.pallas_call(
        functools.partial(gather_kernel, chunks, sizes),
        name="gather_params",
        out_shape=gathered_shapes([shard, vec], sizes[0]),
        in_specs=[VMEM_SPEC] * 2,
        out_specs=[VMEM_SPEC] * 2,
        scratch_shapes=Gather.semaphores(chunks, sizes),
        compiler_params=pltpu.CompilerParams(
            collective_id=collective_id, has_side_effects=True, vmem_limit_bytes=40 * 2**20
        ),
    )(shard, vec)


def add_up(first, rest):
    total = first.astype(F32)
    for term in rest:
        total = total + term.astype(F32)
    return total


class Reduce:
    def __init__(self, chunks, sizes, ins, vec_in, outs, vec_out, scratch, vec_along=True):
        self.vec_along = vec_along and vec_in is not None
        count = len(chunks)
        self.chunks, self.place = chunks, Place(sizes)
        self.ins, self.vec_in, self.outs, self.vec_out = ins, vec_in, outs, vec_out
        self.core_sum, self.from_chips, self.chip_sum, self.from_shards = (
            scratch[i * count : (i + 1) * count] for i in range(4)
        )
        sems = scratch[4 * count :]
        names = ("core_sems", "chip_sems", "shard_sems", "spread_sems", "join_sems")
        for i, name in enumerate(names):
            setattr(self, name, sems[2 * i : 2 * i + 2])
        if vec_in is not None:
            self.vec_sems = sems[10:12]
            self.vec_parts, self.vec_held = sems[12:]

    @staticmethod
    def scratch(chunks, sizes, vec_shape):
        groups, reps = sizes
        chips, count = reps // 2, len(chunks)
        most = max(c.pieces for c in chunks)
        shapes = [(groups, c.blocks, 8, c.columns) for c in chunks]
        for lead in ("chips", "sum", "shards"):
            for c in chunks:
                piece, block = (c.run, 8, c.columns), (c.blocks, 8, c.columns)
                shapes.append(
                    {
                        "chips": (chips - 1,) + (piece if c.shards_first else (groups,) + piece),
                        "sum": block if c.shards_first else (groups,) + piece,
                        "shards": (groups - 1,) + (block if c.shards_first else piece),
                    }[lead]
                )
        made = (
            [pltpu.VMEM(s, BF16) for s in shapes]
            + dma_pair(count)
            + dma_pair(count, chips - 1)
            + dma_pair(count, groups - 1)
            + dma_pair(count, max(most - 1, 1))
            + dma_pair(count)
        )
        if vec_shape is not None:
            terms = chips + groups - 1
            made += dma_pair(terms)
            made += [pltpu.VMEM((terms,) + vec_shape, F32), pltpu.VMEM((2,) + vec_shape, F32)]
        return made

    def chip_ids(self):
        place = self.place
        return [lax.rem(place.chip + e, place.chips) for e in range(1, place.chips)]

    def cores(self, i):
        chunk, place = self.chunks[i], self.place
        src = chunk.part(self.ins[chunk.array], 1 - place.core)
        return [transfer(src, self.core_sum[i], self.core_sems, i, place.core_peer)]

    def chips(self, i):
        chunk, copies = self.chunks[i], []
        for e, chip in enumerate(self.chip_ids()):
            piece = lax.rem(chip, chunk.pieces)
            run = pl.ds(piece * chunk.run, chunk.run)
            src = self.chip_sum[i].at[run] if chunk.shards_first else self.core_sum[i].at[:, run]
            dst = self.from_chips[i].at[e]
            copies.append(transfer(src, dst, self.chip_sems, (i, e), self.place.at(chip)))
        return copies

    def shards(self, i):
        place = self.place
        source = self.core_sum[i] if self.chunks[i].shards_first else self.chip_sum[i]
        return [
            transfer(
                source.at[lax.rem(place.mine + d + 1, place.groups)],
                self.from_shards[i].at[d],
                self.shard_sems,
                (i, d),
                target,
            )
            for d, target in enumerate(place.shard_peers)
        ]

    def spread(self, i):
        chunk, place = self.chunks[i], self.place
        block = chunk.part(self.outs[chunk.array], place.core, place.piece(chunk), 0)
        return [
            transfer(block, block, self.spread_sems, (i, e - 1), place.at(place.mate(chunk, e)))
            for e in range(1, chunk.pieces)
        ]

    def join(self, i):
        chunk, place = self.chunks[i], self.place
        block = chunk.part(self.outs[chunk.array], place.core, None, 0)
        return [transfer(block, block, self.join_sems, i, place.core_peer)]

    def vec_cores(self):
        return [transfer(self.vec_in, self.vec_parts.at[0], self.vec_sems, 0, self.place.core_peer)]

    def vec_chips(self):
        return [
            transfer(
                self.vec_held.at[0],
                self.vec_parts.at[1 + e],
                self.vec_sems,
                1 + e,
                self.place.at(chip),
            )
            for e, chip in enumerate(self.chip_ids())
        ]

    def vec_shards(self):
        chips = self.place.chips
        return [
            transfer(
                self.vec_held.at[1],
                self.vec_parts.at[chips + d],
                self.vec_sems,
                chips + d,
                target,
            )
            for d, target in enumerate(self.place.shard_peers)
        ]

    def greet(self):
        place = self.place
        greet(
            place.shard_peers + [place.at(c) for c in self.chip_ids()] + [place.core_peer]
        )

    def begin(self):
        for i in range(len(self.chunks)):
            start(self.cores(i))
        if self.vec_along:
            self.vec_begin()

    def vec_begin(self):
        start(self.vec_cores())

    def all_to_chips(self):
        for i in range(len(self.chunks)):
            self.to_chips(i)
        if self.vec_along:
            self.vec_to_chips()

    def all_to_shards(self):
        for i in range(len(self.chunks)):
            self.to_shards(i)
        if self.vec_along:
            self.vec_to_shards()

    def all_to_spread(self):
        for i in range(len(self.chunks)):
            self.to_spread(i)
        if self.vec_along:
            self.vec_end()

    def all_to_join(self):
        for i in range(len(self.chunks)):
            self.to_join(i)

    def to_chips(self, i):
        chunk = self.chunks[i]
        own = chunk.part(self.ins[chunk.array], self.place.core)[...]
        arrive(self.cores(i))
        self.core_sum[i][...] = own + self.core_sum[i][...]
        start(self.shards(i) if chunk.shards_first else self.chips(i))

    def vec_to_chips(self):
        arrive(self.vec_cores())
        self.vec_held[0] = self.vec_in[...] + self.vec_parts[0]
        start(self.vec_chips())

    def to_shards(self, i):
        chunk = self.chunks[i]
        piece = self.place.piece(chunk)
        if chunk.shards_first:
            own, copies, terms = self.core_sum[i][self.place.mine], self.shards(i), self.from_shards[i]
        else:
            own = self.core_sum[i][:, pl.ds(piece * chunk.run, chunk.run)]
            copies, terms = self.chips(i), self.from_chips[i]
        arrive(copies)
        total = add_up(own, [terms[e] for e in range(len(copies))])
        self.chip_sum[i][...] = total.astype(BF16)
        start(self.chips(i) if chunk.shards_first else self.shards(i))

    def vec_to_shards(self):
        copies = self.vec_chips()
        arrive(copies)
        self.vec_held[1] = add_up(
            self.vec_held[0], [self.vec_parts[1 + e] for e in range(len(copies))]
        )
        start(self.vec_shards())

    def to_spread(self, i):
        chunk, place = self.chunks[i], self.place
        if chunk.shards_first:
            own = self.chip_sum[i][pl.ds(place.piece(chunk) * chunk.run, chunk.run)]
            copies, terms = self.chips(i), self.from_chips[i]
        else:
            own, copies, terms = self.chip_sum[i][place.mine], self.shards(i), self.from_shards[i]
        arrive(copies)
        total = add_up(own, [terms[d] for d in range(len(copies))])
        block = chunk.part(self.outs[chunk.array], place.core, place.piece(chunk), 0)
        block[...] = total.astype(BF16)
        start(self.spread(i))

    def vec_end(self):
        copies = self.vec_shards()
        arrive(copies)
        self.vec_out[...] = add_up(
            self.vec_held[1], [self.vec_parts[self.place.chips + d] for d in range(len(copies))]
        )

    def to_join(self, i):
        arrive(self.spread(i))
        start(self.join(i))

    def finish(self):
        every = range(len(self.chunks))
        for i in every:
            arrive(self.join(i))
        copies = []
        if self.vec_in is not None:
            copies = self.vec_cores() + self.vec_chips() + self.vec_shards()
        for i in every:
            copies += self.cores(i) + self.chips(i) + self.shards(i)
            copies += self.spread(i) + self.join(i)
        for copy in copies:
            copy.wait_send()


def on_device(
    reps,
    images,
    cotangent,
    ln1_gain,
    ln1_bias,
    w_qkv,
    q_bias,
    v_bias,
    w_proj,
    proj_bias,
    ln2_gain,
    ln2_bias,
    w_up,
    up_bias,
    w_down,
    down_bias,
):
    groups = lax.axis_size("grp")
    sizes = (groups, reps)
    layers, part = ln1_gain.shape
    width = part * groups
    hidden_part = up_bias.shape[1]
    plan = Plan(images.shape, hidden_part * groups)
    vectors = [ln1_gain, ln1_bias, q_bias, v_bias, proj_bias, ln2_gain, ln2_bias, down_bias]
    extra = hidden_part // part
    packed = jnp.stack(vectors, axis=1)
    packed = jnp.concatenate([packed, up_bias.reshape(layers, extra, part)], axis=1)
    packed = packed.astype(F32)
    joined = jnp.concatenate([w_qkv, w_proj], axis=2)

    def shards_of(layer):
        return [m[layer].reshape(1, -1, 8, m.shape[2]) for m in (joined, w_up, w_down)]

    def unpack(vecs):
        vectors = vecs[:, :VECTORS].transpose(1, 0, 2).reshape(VECTORS, width)
        up = vecs[:, VECTORS:].reshape(extra, width)
        rest = plan.vec_rows - VECTORS - extra
        return jnp.concatenate([vectors, up, jnp.zeros((rest, width), F32)], axis=0)

    shards0, shards1 = shards_of(0), shards_of(1)
    first_matrix, vecs0 = gather(shards0[0], packed[0][None], sizes, 0)
    first_matrix, vecs0 = first_matrix.reshape(width, -1), unpack(vecs0)
    hidden, keeps, mlp0, gathered = plan.first(
        images, first_matrix, vecs0, shards0[1:], shards1 + [packed[1][None]], sizes, 1
    )
    weights1 = [g.reshape(-1, g.shape[3]) for g in gathered[:3]]
    encoded, flowing, grads1 = plan.middle(hidden, cotangent, weights1, unpack(gathered[3]))
    blocks = [g.reshape(groups, -1, 8, g.shape[1]) for g in grads1[:3]] + [grads1[3]]
    images_grad, sums, small0, small1 = plan.last(
        flowing, images, [first_matrix] + list(mlp0), vecs0, keeps, blocks, sizes, 2
    )
    full = [x.reshape(layers, -1, x.shape[3]).astype(F32) for x in sums]
    small = jnp.stack([small0, small1])
    me = lax.axis_index("grp")
    vec_out = lax.dynamic_slice_in_dim(small[:, :VECTORS], me * part, part, axis=2)
    up_out = small[:, VECTORS : VECTORS + extra].reshape(layers, -1)
    up_out = lax.dynamic_slice_in_dim(up_out, me * hidden_part, hidden_part, axis=1)
    return (
        encoded,
        images_grad,
        vec_out[:, G1],
        vec_out[:, B1],
        full[0],
        vec_out[:, QB],
        vec_out[:, VB],
        full[1],
        vec_out[:, PB],
        vec_out[:, G2],
        vec_out[:, B2],
        full[2],
        up_out,
        full[3],
        vec_out[:, DB],
    )


def solution(mesh):
    batch = P(("rep", "grp"), None, None)
    vector = P(None, "grp")
    matrix = P(None, "grp", None)
    params = (
        vector,
        vector,
        matrix,
        vector,
        vector,
        matrix,
        vector,
        vector,
        vector,
        matrix,
        vector,
        matrix,
        vector,
    )
    specs = (batch, batch) + params
    return jax.shard_map(
        functools.partial(on_device, mesh.shape["rep"]), mesh=mesh, in_specs=specs, out_specs=specs, check_vma=False
    )
```

```python
import functools
import math

import jax
import jax.numpy as jnp
from jax import lax
from jax.experimental import pallas as pl
from jax.experimental.pallas import tpu as pltpu
from jax.sharding import PartitionSpec as P

HEAD_DIM = 64
PAIR = 2 * HEAD_DIM
EPS = 1e-06
INV_ROOT_TWO = 0.7071067811865476
INV_ROOT_TAU = 0.3989422804014327
MASKED = -1e30
F32 = jnp.float32
BF16 = jnp.bfloat16

VECTORS = 8
G1, B1, QB, VB, PB, G2, B2, DB = range(VECTORS)


def dot(left, right):
    return jnp.dot(left, right, preferred_element_type=F32)


def dot_nt(left, right):
    return lax.dot_general(
        left, right, (((1,), (1,)), ((), ())), preferred_element_type=F32
    )


def col_sum(rows):
    return jnp.sum(rows, axis=0, keepdims=True)


def norm(rows):
    mean = jnp.mean(rows, axis=-1, keepdims=True)
    centered = rows - mean
    inv = lax.rsqrt(jnp.mean(centered * centered, axis=-1, keepdims=True) + EPS)
    return centered * inv, inv


def norm_backward(grad, normed, inv, gain):
    scaled = grad * gain
    return inv * (
        scaled
        - jnp.mean(scaled, axis=-1, keepdims=True)
        - normed * jnp.mean(scaled * normed, axis=-1, keepdims=True)
    )


def attn_forward(qkv, keep, image, seq, pad):
    width = qkv.shape[1] // 3
    base = image * pad
    rows = pl.ds(base, pad)
    value_t = qkv[rows, pl.ds(2 * width, width)].T
    lane = lax.broadcasted_iota(jnp.int32, (1, PAIR), 1)
    halves = [(lane < HEAD_DIM).astype(F32).astype(BF16), (lane >= HEAD_DIM).astype(F32).astype(BF16)]
    full = seq // 8 * 8
    for pair in range(width // PAIR):
        queries = qkv[rows, pl.ds(pair * PAIR, PAIR)]
        keys = qkv[rows, pl.ds(width + pair * PAIR, PAIR)]
        for half in range(2):
            head = 2 * pair + half
            scores = dot_nt(keys * halves[half], queries)
            parts = [scores[:full]]
            if full < seq:
                tail = scores[full : full + 8]
                row = lax.broadcasted_iota(jnp.int32, tail.shape, 0)
                parts.append(jnp.where(row < seq - full, tail, MASKED))
            scores = jnp.concatenate(parts, axis=0)
            top = jnp.max(scores, axis=0, keepdims=True)
            raised = jnp.exp(scores - top)
            probs = raised * (1.0 / col_sum(raised))
            rest = pad - probs.shape[0]
            if rest:
                probs = jnp.concatenate([probs, jnp.zeros((rest, pad), F32)], axis=0)
            keep["probs"][image, head] = probs
            context = dot(value_t[head * HEAD_DIM : (head + 1) * HEAD_DIM], probs.astype(BF16))
            keep["context"][image, pl.ds(head * HEAD_DIM, HEAD_DIM), :] = context.astype(BF16)


def split_attention(packed):
    width = packed.shape[0]
    return packed.at[:, pl.ds(0, 3 * width)], packed.at[:, pl.ds(3 * width, width)]


def up_bias_of(vecs, hidden_width):
    rows = hidden_width // vecs.shape[1]
    return jnp.concatenate([vecs[VECTORS + i : VECTORS + i + 1] for i in range(rows)], axis=1)


def attention_part(hidden, packed, vecs, keep, images, seq, pad):
    w_qkv, w_proj = split_attention(packed)
    width = hidden.shape[1]
    normed, _ = norm(hidden)
    rows_in = (normed * vecs[G1 : G1 + 1] + vecs[B1 : B1 + 1]).astype(BF16)
    qkv = keep["qkv"]
    projected = dot(rows_in, w_qkv[...])
    qkv[:, :width] = (projected[:, :width] + vecs[QB : QB + 1]).astype(BF16) * jnp.asarray(
        HEAD_DIM**-0.5, BF16
    )
    qkv[:, width : 2 * width] = projected[:, width : 2 * width].astype(BF16)
    qkv[:, 2 * width :] = (projected[:, 2 * width :] + vecs[VB : VB + 1]).astype(BF16)
    for image in range(images):
        attn_forward(qkv, keep, image, seq, pad)
    context = jnp.concatenate([keep["context"][image].T for image in range(images)], axis=0)
    mixed = hidden + dot(context, w_proj[...]) + vecs[PB : PB + 1]
    keep["mixed"][...] = mixed
    return mixed


def mlp_part(mixed, w_up, w_down, vecs, keep):
    up_bias = up_bias_of(vecs, w_down.shape[0])
    normed, _ = norm(mixed)
    rows_mid = (normed * vecs[G2 : G2 + 1] + vecs[B2 : B2 + 1]).astype(BF16)
    upward = dot(rows_mid, w_up[...]) + up_bias
    cumul = 0.5 * (1.0 + lax.erf(upward * INV_ROOT_TWO))
    keep["active"][...] = (upward * cumul).astype(BF16)
    slope = cumul + upward * jnp.exp(-0.5 * upward * upward) * INV_ROOT_TAU
    keep["slope"][...] = slope.astype(keep["slope"].dtype)
    return mixed + dot(keep["active"][...], w_down[...]) + vecs[DB : DB + 1]


def attn_backward(qkv, keep, context_grad, joint, vec_grads, image, pad):
    width = qkv.shape[1] // 3
    rows = pl.ds(image * pad, pad)
    keys_t = qkv[rows, pl.ds(width, width)].T
    lane = lax.broadcasted_iota(jnp.int32, (1, PAIR), 1)
    low = lax.broadcasted_iota(jnp.int32, (pad, PAIR), 1) < HEAD_DIM
    halves = [(lane < HEAD_DIM).astype(F32).astype(BF16), (lane >= HEAD_DIM).astype(F32).astype(BF16)]
    query_parts = []
    for pair in range(width // PAIR):
        queries = qkv[rows, pl.ds(pair * PAIR, PAIR)]
        values = qkv[rows, pl.ds(2 * width + pair * PAIR, PAIR)]
        ctx = context_grad[rows, pl.ds(pair * PAIR, PAIR)]
        key_parts, value_parts = [], []
        for half in range(2):
            head = 2 * pair + half
            probs = keep["probs"][image, head]
            prob_grad = dot_nt(values * halves[half], ctx)
            value_parts.append(dot(probs.astype(BF16), ctx))
            row_dot = col_sum(probs * prob_grad)
            score_grad = (probs * (prob_grad - row_dot)).astype(BF16)
            key_parts.append(dot(score_grad, queries))
            query_parts.append(dot(keys_t[head * HEAD_DIM : (head + 1) * HEAD_DIM], score_grad))
        key_grad = jnp.where(low, key_parts[0], key_parts[1])
        value_grad = jnp.where(low, value_parts[0], value_parts[1])
        joint[rows, pl.ds(width + pair * PAIR, PAIR)] = key_grad.astype(BF16)
        joint[rows, pl.ds(2 * width + pair * PAIR, PAIR)] = value_grad.astype(BF16)
        vec_grads[VB : VB + 1, pl.ds(pair * PAIR, PAIR)] += col_sum(value_grad)
    query_grad = jnp.concatenate(query_parts, axis=0).T * HEAD_DIM**-0.5
    joint[rows, pl.ds(0, width)] = query_grad.astype(BF16)
    vec_grads[QB : QB + 1, :] += col_sum(query_grad)


def mlp_backward(out_grad, w_up, w_down, vecs, keep, acc):
    _, _, g_up, g_down, vec_grads, up_bias_grad = acc[:6]
    rounded = out_grad.astype(BF16)
    vec_grads[DB : DB + 1, :] += col_sum(out_grad)
    g_down[...] += dot(rounded.T, keep["active"][...])
    up_grad = dot_nt(rounded, w_down[...]) * keep["slope"][...].astype(F32)
    up_bias_grad[...] += col_sum(up_grad)
    up_rounded = up_grad.astype(BF16)
    normed, inv = norm(keep["mixed"][...])
    gain = vecs[G2 : G2 + 1]
    rows_mid = (normed * gain + vecs[B2 : B2 + 1]).astype(BF16)
    g_up[...] += dot(rows_mid.T, up_rounded)
    mid_grad = dot_nt(up_rounded, w_up[...])
    vec_grads[G2 : G2 + 1, :] += col_sum(mid_grad * normed)
    vec_grads[B2 : B2 + 1, :] += col_sum(mid_grad)
    return out_grad + norm_backward(mid_grad, normed, inv, gain)


def attention_backward(mixed_grad, hidden, packed, vecs, keep, acc, joint, images, pad):
    _, w_proj = split_attention(packed)
    g_qkv, g_proj, _, _, vec_grads, _, context_grad = acc
    vec_grads[PB : PB + 1, :] += col_sum(mixed_grad)
    mixed_rounded = mixed_grad.astype(BF16)
    part = g_proj[...]
    for image in range(images):
        part += dot(keep["context"][image], mixed_rounded[image * pad : (image + 1) * pad])
    g_proj[...] = part
    context_grad[...] = dot_nt(mixed_rounded, w_proj[...]).astype(BF16)
    for image in range(images):
        attn_backward(keep["qkv"], keep, context_grad, joint, vec_grads, image, pad)
    normed, _ = norm(hidden)
    rows_in = (normed * vecs[G1 : G1 + 1] + vecs[B1 : B1 + 1]).astype(BF16)
    g_qkv[...] += dot(rows_in.T, joint[...])


def input_backward(mixed_grad, hidden, packed, vecs, vec_grads, joint):
    w_qkv, _ = split_attention(packed)
    normed, inv = norm(hidden)
    in_grad = dot_nt(joint[...], w_qkv[...])
    vec_grads[G1 : G1 + 1, :] += col_sum(in_grad * normed)
    vec_grads[B1 : B1 + 1, :] += col_sum(in_grad)
    return mixed_grad + norm_backward(in_grad, normed, inv, vecs[G1 : G1 + 1])


def load_padded(ref, buf, pad):
    images, seq, width = ref.shape
    for image in range(images):
        buf[pl.ds(image * pad, seq), :] = ref[image].astype(F32)
        if pad > seq:
            buf[pl.ds(image * pad + seq, pad - seq), :] = jnp.zeros((pad - seq, width), F32)


def store_images(ref, rows, pad):
    images, seq, _ = ref.shape
    for image in range(images):
        ref[image] = rows[image * pad : image * pad + seq].astype(ref.dtype)


KEEP = ("qkv", "probs", "context", "mixed", "active", "slope")


def keep_shapes(images, pad, width, hidden_width):
    heads = width // HEAD_DIM
    return {
        "qkv": ((images * pad, 3 * width), BF16),
        "probs": ((images, heads, pad, pad), F32),
        "context": ((images, width, pad), BF16),
        "mixed": ((images * pad, width), F32),
        "active": ((images * pad, hidden_width), BF16),
        "slope": ((images * pad, hidden_width), F32),
    }


def init_grads(acc):
    @pl.when(pl.program_id(0) == 0)
    def _():
        for ref in acc[:6]:
            ref[...] = jnp.zeros_like(ref)


def flush_vectors(acc, vecs):
    vec_grads, up_bias_grad = acc[4:6]
    width = vecs.shape[1]
    extra = up_bias_grad.shape[1] // width
    vecs[:VECTORS, :] = vec_grads[...]
    for i in range(extra):
        vecs[VECTORS + i : VECTORS + i + 1, :] = up_bias_grad[:, i * width : (i + 1) * width]
    rest = vecs.shape[0] - VECTORS - extra
    if rest:
        vecs[VECTORS + extra :, :] = jnp.zeros((rest, width), F32)


def step_at(step):
    return pl.when(pl.program_id(0) == step)


def first_kernel(sizes, steps, mesh_sizes, chunks, *refs):
    group, seq, pad = sizes
    images, packed, vecs = refs[:3]
    shards0, shards1 = refs[3:5], refs[5:9]
    out = refs[9]
    keep = dict(zip(KEEP, refs[10:16]))
    mlp_out = refs[16:18]
    full1 = refs[18:22]
    buf, mixed_rows = refs[22:24]
    landed = refs[24:26]
    rest = refs[26:]
    half = len(rest) // 2
    now = Gather(chunks[0], mesh_sizes, shards0, None, landed, None, rest[:half])
    later = Gather(
        chunks[1], mesh_sizes, shards1[:3], shards1[3], full1[:3], full1[3], rest[half:]
    )
    step = pl.program_id(0)
    rows = group * pad

    @step_at(0)
    def _():
        now.greet()
        now.begin()
        later.begin()

    @step_at(2 * steps // 5)
    def _():
        now.all_to_chips()

    @pl.when(step < steps)
    def _():
        load_padded(images, buf, pad)
        mixed = attention_part(buf[...], packed, vecs, keep, group, seq, pad)
        mixed_rows[pl.ds(pl.multiple_of(step * rows, rows), rows), :] = mixed

    @step_at(4 * steps // 5)
    def _():
        now.to_cores(0)
        later.to_chips(0)
        later.to_chips(1)

    @step_at(steps)
    def _():
        now.to_cores(1)
        now.finish()
        for matrix, source in zip(mlp_out, landed):
            flat = source[...].astype(F32).reshape(matrix.shape)
            matrix[...] = flat.astype(BF16)

    @step_at(steps + 3 * steps // 5)
    def _():
        later.to_chips(2)
        later.to_cores(2)

    @step_at(2 * steps - 1)
    def _():
        later.to_cores(0)
        later.to_cores(1)

    @pl.when(step >= steps)
    def _():
        at = pl.multiple_of((step - steps) * rows, rows)
        mixed = mixed_rows[pl.ds(at, rows), :]
        out[...] = mlp_part(mixed, mlp_out[0], mlp_out[1], vecs, keep)

    @step_at(2 * steps - 1)
    def _():
        later.finish()


def middle_kernel(sizes, *refs):
    group, seq, pad = sizes
    hidden, cotangent, packed, w_up, w_down, vecs, encoded, flowing = refs[:8]
    outs, vec_out = refs[8:11], refs[11]
    keep = dict(zip(KEEP, refs[12:18]))
    acc = refs[18:25]
    joint, buf = refs[25:]
    init_grads(acc)
    mixed = attention_part(hidden[...], packed, vecs, keep, group, seq, pad)
    result = mlp_part(mixed, w_up, w_down, vecs, keep)
    store_images(encoded, result, pad)
    load_padded(cotangent, buf, pad)
    mixed_grad = mlp_backward(buf[...], w_up, w_down, vecs, keep, acc)
    attention_backward(mixed_grad, hidden[...], packed, vecs, keep, acc, joint, group, pad)
    flowing[...] = input_backward(mixed_grad, hidden[...], packed, vecs, acc[4], joint)

    @step_at(pl.num_programs(0) - 1)
    def _():
        g_qkv_out, g_proj_out = split_attention(outs[0])
        g_qkv_out[...] = acc[0][...].astype(BF16)
        g_proj_out[...] = acc[1][...].astype(BF16)
        outs[1][...] = acc[2][...].astype(BF16)
        outs[2][...] = acc[3][...].astype(BF16).T
        flush_vectors(acc, vec_out)


def last_kernel(sizes, steps, mesh_sizes, chunks, counts, *refs):
    group, seq, pad = sizes
    flowing, images, packed, w_up, w_down, vecs = refs[:6]
    keep = dict(zip(KEEP, refs[6:12]))
    grads1, vec1 = refs[12:15], refs[15]
    images_grad, sums, vec_out0, vec_out1 = refs[16], refs[17:21], refs[21], refs[22]
    acc = refs[23:30]
    buf, grad_rows, joint_rows, vec0 = refs[30:34]
    grads0, shares0, shares1 = refs[34:37], refs[37:40], refs[40:43]
    scratch = refs[43:]
    ends = [sum(counts[: i + 1]) for i in range(3)]
    later = Reduce(chunks[0], mesh_sizes, grads1, vec1, shares1, vec_out1, scratch[: ends[0]])
    mlp = Reduce(
        chunks[1], mesh_sizes, grads0[1:], None, shares0[1:], None, scratch[ends[0] : ends[1]]
    )
    tail = Reduce(
        chunks[2],
        mesh_sizes,
        grads0[:1],
        vec0,
        shares0[:1],
        vec_out0,
        scratch[ends[1] :],
        vec_along=False,
    )
    step = pl.program_id(0)
    rows = group * pad
    last = 3 * steps - 1
    three = acc[0].shape[1]

    def rows_at(start):
        return pl.ds(pl.multiple_of((step - start) * rows, rows), rows)

    @step_at(0)
    def _():
        later.greet()
        later.begin()

    @step_at(1 * steps // 5)
    def _():
        later.all_to_chips()

    init_grads(acc)

    @pl.when(step < steps)
    def _():
        grad_rows[rows_at(0), :] = mlp_backward(flowing[...], w_up, w_down, vecs, keep, acc)

    @step_at(steps)
    def _():
        grads0[1][...] = acc[2][...].reshape(grads0[1].shape).astype(BF16)
        grads0[2][...] = acc[3][...].T.reshape(grads0[2].shape).astype(BF16)
        mlp.begin()

    @step_at(steps + 1 * steps // 5)
    def _():
        later.all_to_shards()
        mlp.all_to_chips()

    @step_at(steps + 3 * steps // 5)
    def _():
        later.all_to_spread()

    @step_at(2 * steps - 1)
    def _():
        mlp.all_to_shards()
        later.all_to_join()

    @pl.when((step >= steps) & (step < 2 * steps))
    def _():
        load_padded(images, buf, pad)
        attention_backward(
            grad_rows[rows_at(steps), :],
            buf[...],
            packed,
            vecs,
            keep,
            acc,
            joint_rows.at[rows_at(steps), :],
            group,
            pad,
        )

    @step_at(2 * steps)
    def _():
        shape = grads0[0].shape
        grads0[0][:, :, :, :three] = acc[0][...].reshape(shape[:3] + (three,)).astype(BF16)
        grads0[0][:, :, :, three:] = (
            acc[1][...].reshape(shape[:3] + (shape[3] - three,)).astype(BF16)
        )
        tail.begin()

    @step_at(2 * steps + steps // 5)
    def _():
        tail.all_to_chips()

    @step_at(2 * steps + 2 * steps // 5)
    def _():
        mlp.all_to_spread()

    @step_at(last)
    def _():
        tail.all_to_shards()

    @pl.when(step >= 2 * steps)
    def _():
        load_padded(images, buf, pad)
        result = input_backward(
            grad_rows[rows_at(2 * steps), :],
            buf[...],
            packed,
            vecs,
            acc[4],
            joint_rows.at[rows_at(2 * steps), :],
        )
        store_images(images_grad, result, pad)

    def store_sums(layer, shares):
        sums[0][layer] = shares[0][0, :, :, :three]
        sums[1][layer] = shares[0][0, :, :, three:]

    @step_at(last)
    def _():
        flush_vectors(acc, vec0)
        tail.vec_begin()
        tail.vec_to_chips()
        mlp.all_to_join()
        later.finish()
        store_sums(1, shares1)
        for total, share in zip(sums[2:], shares1[1:]):
            total[1] = share[0]
        tail.vec_to_shards()
        tail.all_to_spread()
        mlp.finish()
        for total, share in zip(sums[2:], shares0[1:]):
            total[0] = share[0]
        tail.all_to_join()
        tail.vec_end()
        tail.finish()
        store_sums(0, shares0)


def whole(shape):
    return pl.BlockSpec(shape, lambda i: (0,) * len(shape), pipeline_mode=pl.Buffered(1))


def rows_spec(shape, steps, start=0, again=False):
    def block(i):
        at = jnp.maximum(i - start, 0)
        return lax.rem(at, steps) if again else jnp.minimum(at, steps - 1)

    return pl.BlockSpec(
        (shape[0] // steps,) + tuple(shape[1:]), lambda i: (block(i),) + (0,) * (len(shape) - 1)
    )


class Plan:
    def __init__(self, images_shape, hidden_width):
        self.count, self.seq, self.width = images_shape
        self.hidden_width = hidden_width
        self.pad = -(-self.seq // 16) * 16
        self.group = 2 if self.count % 2 == 0 else 1
        self.steps = self.count // self.group
        self.rows = self.count * self.pad
        self.keep = keep_shapes(self.count, self.pad, self.width, hidden_width)
        self.keep_block = keep_shapes(self.group, self.pad, self.width, hidden_width)
        self.weight_shapes = [
            (self.width, 3 * self.width),
            (self.width, self.width),
            (self.width, hidden_width),
            (hidden_width, self.width),
        ]
        self.sizes = (self.group, self.seq, self.pad)
        block_rows = self.group * self.pad
        self.buffer = pltpu.VMEM((block_rows, self.width), F32)
        self.acc = [
            pltpu.VMEM(self.weight_shapes[0], F32),
            pltpu.VMEM(self.weight_shapes[1], F32),
            pltpu.VMEM(self.weight_shapes[2], F32),
            pltpu.VMEM((self.width, hidden_width), F32),
            pltpu.VMEM((8, self.width), F32),
            pltpu.VMEM((1, hidden_width), F32),
            pltpu.VMEM((block_rows, self.width), BF16),
        ]
        self.joint = pltpu.VMEM((block_rows, 3 * self.width), BF16)
        self.vec_rows = -(-(VECTORS + hidden_width // self.width) // 8) * 8
        self.packed_shapes = [
            (self.width, 4 * self.width),
            (self.width, hidden_width),
            (hidden_width, self.width),
        ]
        self.vec_shape = (self.vec_rows, self.width)
        self.grad_shapes = [jax.ShapeDtypeStruct(s, BF16) for s in self.packed_shapes] + [
            jax.ShapeDtypeStruct(self.vec_shape, F32)
        ]
        self.params = pltpu.CompilerParams(
            dimension_semantics=("arbitrary",), vmem_limit_bytes=60 * 2**20
        )

    def image_spec(self, start=0, again=False):
        return rows_spec((self.count, self.seq, self.width), self.steps, start, again)

    def state_spec(self, start=0):
        return rows_spec((self.rows, self.width), self.steps, start)

    def param_specs(self):
        return [whole(s) for s in self.packed_shapes + [self.vec_shape]]

    def keep_specs(self, starts):
        return [rows_spec(self.keep[k][0], self.steps, at) for k, at in zip(KEEP, starts)]

    def grad_specs(self):
        return [whole(s.shape) for s in self.grad_shapes]

    def cost(self, layers):
        rows, width, hidden = self.count * self.seq, self.width, self.hidden_width
        flops = 2 * rows * width * (4 * width + 2 * hidden) * layers
        return pl.CostEstimate(
            flops=int(flops), bytes_accessed=int(40 * 2**20), transcendentals=0
        )

    def comm_params(self, collective_id):
        return pltpu.CompilerParams(
            dimension_semantics=("arbitrary",),
            vmem_limit_bytes=67_043_328,
            collective_id=collective_id,
            has_side_effects=True,
        )

    def first(self, images, packed, vecs, shards0, shards1, mesh_sizes, collective_id):
        state = jax.ShapeDtypeStruct((self.rows, self.width), F32)
        keeps = [jax.ShapeDtypeStruct(*self.keep[k]) for k in KEEP]
        mlp = [jax.ShapeDtypeStruct(s, BF16) for s in self.packed_shapes[1:]]
        chunks = [
            chunks_of(shards0, mesh_sizes),
            chunks_of(shards1[:3], mesh_sizes, undivided=(2,)),
        ]
        n = self.steps
        out = pl.pallas_call(
            functools.partial(first_kernel, self.sizes, n, mesh_sizes, chunks),
            name="layer_first",
            out_shape=[state] + keeps + mlp + gathered_shapes(shards1, mesh_sizes[0]),
            grid=(2 * n,),
            in_specs=[self.image_spec(), whole(packed.shape), whole(self.vec_shape)]
            + [ANY_SPEC] * 6,
            out_specs=[self.state_spec(n)]
            + self.keep_specs((0, 0, 0, 0, n, n))
            + [whole(m.shape) for m in mlp]
            + [ANY_SPEC] * 4,
            scratch_shapes=[self.buffer, pltpu.VMEM((self.rows, self.width), F32)]
            + [pltpu.VMEM(s.shape, BF16) for s in gathered_shapes(shards0, mesh_sizes[0])]
            + Gather.semaphores(chunks[0], mesh_sizes)
            + Gather.semaphores(chunks[1], mesh_sizes),
            compiler_params=self.comm_params(collective_id),
            cost_estimate=self.cost(1),
        )(images, packed, vecs, *shards0, *shards1)
        return out[0], out[1:7], out[7:9], out[9:]

    def middle(self, hidden, cotangent, weights, vecs):
        state = jax.ShapeDtypeStruct((self.rows, self.width), F32)
        out = pl.pallas_call(
            functools.partial(middle_kernel, self.sizes),
            name="layer_middle",
            out_shape=[jax.ShapeDtypeStruct(cotangent.shape, BF16), state] + self.grad_shapes,
            grid=(self.steps,),
            in_specs=[self.state_spec(), self.image_spec()] + self.param_specs(),
            out_specs=[self.image_spec(), self.state_spec()] + self.grad_specs(),
            scratch_shapes=[pltpu.VMEM(*self.keep_block[k]) for k in KEEP]
            + self.acc
            + [self.joint, self.buffer],
            compiler_params=self.params,
            cost_estimate=self.cost(3),
        )(hidden, cotangent, *weights, vecs)
        return out[0], out[1], out[2:]

    def last(self, flowing, images, weights, vecs, keeps, grads, mesh_sizes, collective_id):
        groups = mesh_sizes[0]
        whole_grads = [
            jax.ShapeDtypeStruct(g.shape, BF16) for g in grads[:3]
        ]
        chunks = [
            chunks_of(whole_grads, mesh_sizes, 1, (1,)),
            chunks_of(whole_grads[1:], mesh_sizes, 1, ()),
            chunks_of(whole_grads[:1], mesh_sizes, 3, (0,)),
        ]
        shares = [(1,) + g.shape[1:] for g in whole_grads]
        blocks = whole_grads[0].shape[1:3]
        sums = [
            jax.ShapeDtypeStruct((2,) + shape, BF16)
            for shape in (
                blocks + (3 * self.width,),
                blocks + (self.width,),
                whole_grads[1].shape[1:],
                whole_grads[2].shape[1:],
            )
        ]
        vec = jax.ShapeDtypeStruct(self.vec_shape, F32)
        scratch = [
            Reduce.scratch(chunks[0], mesh_sizes, self.vec_shape),
            Reduce.scratch(chunks[1], mesh_sizes, None),
            Reduce.scratch(chunks[2], mesh_sizes, self.vec_shape),
        ]
        n = self.steps
        outs = [jax.ShapeDtypeStruct(images.shape, BF16)] + sums + [vec, vec]
        out = pl.pallas_call(
            functools.partial(
                last_kernel, self.sizes, n, mesh_sizes, chunks, [len(x) for x in scratch]
            ),
            name="layer_last",
            out_shape=outs,
            grid=(3 * n,),
            in_specs=[self.state_spec(), self.image_spec(n, True)]
            + self.param_specs()
            + self.keep_specs((n, n, n, 0, 0, 0))
            + [whole(g.shape) for g in grads],
            out_specs=[self.image_spec(2 * n)] + [whole(o.shape) for o in outs[1:]],
            scratch_shapes=self.acc
            + [
                self.buffer,
                pltpu.VMEM((self.rows, self.width), F32),
                pltpu.VMEM((self.rows, 3 * self.width), BF16),
                pltpu.VMEM(self.vec_shape, F32),
            ]
            + [pltpu.VMEM(g.shape, BF16) for g in whole_grads]
            + [pltpu.VMEM(s, BF16) for s in shares]
            + [pltpu.VMEM(s, BF16) for s in shares]
            + sum(scratch, []),
            compiler_params=self.comm_params(collective_id),
            cost_estimate=self.cost(2),
        )(flowing, images, *weights, vecs, *keeps, *grads)
        return out[0], out[1:5], out[5], out[6]


def greet(targets):
    barrier = pltpu.get_barrier_semaphore()
    for target in targets:
        pl.semaphore_signal(
            barrier, inc=1, device_id=target, device_id_type=pl.DeviceIdType.MESH
        )
    pl.semaphore_wait(barrier, len(targets))


def transfer(src, dst, sems, at, target):
    return pltpu.make_async_remote_copy(
        src_ref=src,
        dst_ref=dst,
        send_sem=sems[0].at[at],
        recv_sem=sems[1].at[at],
        device_id=target,
        device_id_type=pl.DeviceIdType.MESH,
    )


class Chunk:
    def __init__(self, array, blocks, columns, by_columns, extent, start, chips, shards_first):
        self.shards_first = shards_first
        self.array, self.by_columns, self.start, self.extent = array, by_columns, start, extent
        self.blocks = blocks if by_columns else extent
        self.columns = extent if by_columns else columns
        self.stride = (columns if by_columns else blocks) // 2
        self.pieces = math.gcd(self.blocks, chips)
        self.run = self.blocks // self.pieces

    def part(self, ref, core, piece=None, shard=slice(None)):
        at = core * self.stride + self.start
        first, size = (0, self.blocks) if piece is None else (piece * self.run, self.run)
        if self.by_columns:
            columns = pl.ds(pl.multiple_of(at, 128), self.columns)
            return ref.at[shard, pl.ds(first, size), :, columns]
        return ref.at[shard, pl.ds(at + first, size)]


def chunks_of(arrays, mesh_sizes, want=1, shards_first=(), undivided=()):
    chips = mesh_sizes[1] // 2
    lists = []
    for array, (_, blocks, _, columns) in enumerate(a.shape for a in arrays):
        by_columns = columns % 256 == 0 and columns > blocks * 8
        half = columns // 2 if by_columns else blocks // 2
        unit = 128 if by_columns else 1
        parts = want if half % (want * unit) == 0 else 1
        extent = half // parts
        lists.append(
            [
                Chunk(
                    array, blocks, columns, by_columns, extent, j * extent,
                    1 if array * want + j in undivided else chips,
                    array * want + j in shards_first,
                )
                for j in range(parts)
            ]
        )
    return sum(lists, [])


class Place:
    def __init__(self, sizes):
        self.groups, self.reps = sizes
        self.rep, self.mine = lax.axis_index("rep"), lax.axis_index("grp")
        self.chip, self.core = self.rep // 2, lax.rem(self.rep, 2)
        self.chips = self.reps // 2
        self.shard_peers = [
            (self.rep, lax.rem(self.mine + d, self.groups)) for d in range(1, self.groups)
        ]
        self.core_peer = (self.chip * 2 + 1 - self.core, self.mine)

    def piece(self, chunk):
        return lax.rem(self.chip, chunk.pieces)

    def mate(self, chunk, step):
        piece = self.piece(chunk)
        return self.chip - piece + lax.rem(piece + step, chunk.pieces)

    def at(self, chip):
        return (chip * 2 + self.core, self.mine)


class Gather:
    def __init__(self, chunks, sizes, ins, vec_in, outs, vec_out, sems):
        self.chunks, self.place = chunks, Place(sizes)
        self.ins, self.outs, self.vec_in, self.vec_out = ins, outs, vec_in, vec_out
        self.own_sem, self.vec_own_sem = sems[:2]
        self.vec_sems, self.shard_sems, self.chip_sems, self.core_sems = (
            sems[2 + 2 * i : 4 + 2 * i] for i in range(4)
        )

    @staticmethod
    def semaphores(chunks, sizes):
        groups = sizes[0]
        most = max(c.pieces for c in chunks)
        count = len(chunks)
        return (
            [pltpu.SemaphoreType.DMA((count,)), pltpu.SemaphoreType.DMA]
            + dma_pair(groups - 1)
            + dma_pair(count, groups - 1)
            + dma_pair(count, max(most - 1, 1))
            + dma_pair(count)
        )

    def shards(self, i):
        chunk, place = self.chunks[i], self.place
        piece = place.piece(chunk)
        src = chunk.part(self.ins[chunk.array], place.core, piece, 0)
        dst = chunk.part(self.outs[chunk.array], place.core, piece, place.mine)
        return [
            transfer(src, dst, self.shard_sems, (i, d), t)
            for d, t in enumerate(place.shard_peers)
        ]

    def own(self, i):
        chunk, place = self.chunks[i], self.place
        piece = place.piece(chunk)
        src = chunk.part(self.ins[chunk.array], place.core, piece, 0)
        dst = chunk.part(self.outs[chunk.array], place.core, piece, place.mine)
        return pltpu.make_async_copy(src, dst, self.own_sem.at[i])

    def vectors(self):
        return [
            transfer(self.vec_in.at[0], self.vec_out.at[self.place.mine], self.vec_sems, d, t)
            for d, t in enumerate(self.place.shard_peers)
        ]

    def vector_own(self):
        return pltpu.make_async_copy(
            self.vec_in.at[0], self.vec_out.at[self.place.mine], self.vec_own_sem
        )

    def chips(self, i):
        chunk, place = self.chunks[i], self.place
        block = chunk.part(self.outs[chunk.array], place.core, place.piece(chunk))
        return [
            transfer(block, block, self.chip_sems, (i, e - 1), place.at(place.mate(chunk, e)))
            for e in range(1, chunk.pieces)
        ]

    def cores(self, i):
        chunk, place = self.chunks[i], self.place
        block = chunk.part(self.outs[chunk.array], place.core)
        return [transfer(block, block, self.core_sems, i, place.core_peer)]

    def greet(self):
        place = self.place
        most = max(self.chunks, key=lambda c: c.pieces)
        greet(
            place.shard_peers
            + [place.at(place.mate(most, e)) for e in range(1, most.pieces)]
            + [place.core_peer]
        )

    def begin(self):
        for i in range(len(self.chunks)):
            start(self.shards(i))
            self.own(i).start()
        if self.vec_in is not None:
            start(self.vectors())
            self.vector_own().start()

    def all_to_chips(self):
        for i in range(len(self.chunks)):
            self.to_chips(i)

    def all_to_cores(self):
        for i in range(len(self.chunks)):
            self.to_cores(i)

    def to_chips(self, i):
        self.own(i).wait()
        arrive(self.shards(i))
        start(self.chips(i))

    def to_cores(self, i):
        arrive(self.chips(i))
        start(self.cores(i))

    def finish(self):
        every = range(len(self.chunks))
        for i in every:
            arrive(self.cores(i))
        if self.vec_in is not None:
            arrive(self.vectors())
            self.vector_own().wait()
            for copy in self.vectors():
                copy.wait_send()
        for i in every:
            for copy in self.shards(i) + self.chips(i) + self.cores(i):
                copy.wait_send()


def start(copies):
    for copy in copies:
        copy.start()


def arrive(copies):
    for copy in copies:
        copy.wait_recv()


def gather_kernel(chunks, sizes, *refs):
    work = Gather(chunks, sizes, refs[:1], refs[1], refs[2:3], refs[3], refs[4:])
    work.greet()
    work.begin()
    work.all_to_chips()
    work.all_to_cores()
    work.finish()


def dma_pair(*shape):
    return [pltpu.SemaphoreType.DMA(shape), pltpu.SemaphoreType.DMA(shape)]


VMEM_SPEC = pl.BlockSpec(memory_space=pltpu.VMEM)
ANY_SPEC = pl.BlockSpec(memory_space=pl.ANY)


def gathered_shapes(shards, groups):
    return [jax.ShapeDtypeStruct((groups,) + s.shape[1:], s.dtype) for s in shards]


def gather(shard, vec, sizes, collective_id):
    chunks = chunks_of([shard], sizes, 3, undivided=(2,))
    return pl.pallas_call(
        functools.partial(gather_kernel, chunks, sizes),
        name="gather_params",
        out_shape=gathered_shapes([shard, vec], sizes[0]),
        in_specs=[VMEM_SPEC] * 2,
        out_specs=[VMEM_SPEC] * 2,
        scratch_shapes=Gather.semaphores(chunks, sizes),
        compiler_params=pltpu.CompilerParams(
            collective_id=collective_id, has_side_effects=True, vmem_limit_bytes=40 * 2**20
        ),
    )(shard, vec)


def add_up(first, rest):
    total = first.astype(F32)
    for term in rest:
        total = total + term.astype(F32)
    return total


class Reduce:
    def __init__(self, chunks, sizes, ins, vec_in, outs, vec_out, scratch, vec_along=True):
        self.vec_along = vec_along and vec_in is not None
        count = len(chunks)
        self.chunks, self.place = chunks, Place(sizes)
        self.ins, self.vec_in, self.outs, self.vec_out = ins, vec_in, outs, vec_out
        self.core_sum, self.from_chips, self.chip_sum, self.from_shards = (
            scratch[i * count : (i + 1) * count] for i in range(4)
        )
        sems = scratch[4 * count :]
        names = ("core_sems", "chip_sems", "shard_sems", "spread_sems", "join_sems")
        for i, name in enumerate(names):
            setattr(self, name, sems[2 * i : 2 * i + 2])
        if vec_in is not None:
            self.vec_sems = sems[10:12]
            self.vec_parts, self.vec_held = sems[12:]

    @staticmethod
    def scratch(chunks, sizes, vec_shape):
        groups, reps = sizes
        chips, count = reps // 2, len(chunks)
        most = max(c.pieces for c in chunks)
        shapes = [(groups, c.blocks, 8, c.columns) for c in chunks]
        for lead in ("chips", "sum", "shards"):
            for c in chunks:
                piece, block = (c.run, 8, c.columns), (c.blocks, 8, c.columns)
                shapes.append(
                    {
                        "chips": (chips - 1,) + (piece if c.shards_first else (groups,) + piece),
                        "sum": block if c.shards_first else (groups,) + piece,
                        "shards": (groups - 1,) + (block if c.shards_first else piece),
                    }[lead]
                )
        made = (
            [pltpu.VMEM(s, BF16) for s in shapes]
            + dma_pair(count)
            + dma_pair(count, chips - 1)
            + dma_pair(count, groups - 1)
            + dma_pair(count, max(most - 1, 1))
            + dma_pair(count)
        )
        if vec_shape is not None:
            terms = chips + groups - 1
            made += dma_pair(terms)
            made += [pltpu.VMEM((terms,) + vec_shape, F32), pltpu.VMEM((2,) + vec_shape, F32)]
        return made

    def chip_ids(self):
        place = self.place
        return [lax.rem(place.chip + e, place.chips) for e in range(1, place.chips)]

    def cores(self, i):
        chunk, place = self.chunks[i], self.place
        src = chunk.part(self.ins[chunk.array], 1 - place.core)
        return [transfer(src, self.core_sum[i], self.core_sems, i, place.core_peer)]

    def chips(self, i):
        chunk, copies = self.chunks[i], []
        for e, chip in enumerate(self.chip_ids()):
            piece = lax.rem(chip, chunk.pieces)
            run = pl.ds(piece * chunk.run, chunk.run)
            src = self.chip_sum[i].at[run] if chunk.shards_first else self.core_sum[i].at[:, run]
            dst = self.from_chips[i].at[e]
            copies.append(transfer(src, dst, self.chip_sems, (i, e), self.place.at(chip)))
        return copies

    def shards(self, i):
        place = self.place
        source = self.core_sum[i] if self.chunks[i].shards_first else self.chip_sum[i]
        return [
            transfer(
                source.at[lax.rem(place.mine + d + 1, place.groups)],
                self.from_shards[i].at[d],
                self.shard_sems,
                (i, d),
                target,
            )
            for d, target in enumerate(place.shard_peers)
        ]

    def spread(self, i):
        chunk, place = self.chunks[i], self.place
        block = chunk.part(self.outs[chunk.array], place.core, place.piece(chunk), 0)
        return [
            transfer(block, block, self.spread_sems, (i, e - 1), place.at(place.mate(chunk, e)))
            for e in range(1, chunk.pieces)
        ]

    def join(self, i):
        chunk, place = self.chunks[i], self.place
        block = chunk.part(self.outs[chunk.array], place.core, None, 0)
        return [transfer(block, block, self.join_sems, i, place.core_peer)]

    def vec_cores(self):
        return [transfer(self.vec_in, self.vec_parts.at[0], self.vec_sems, 0, self.place.core_peer)]

    def vec_chips(self):
        return [
            transfer(
                self.vec_held.at[0],
                self.vec_parts.at[1 + e],
                self.vec_sems,
                1 + e,
                self.place.at(chip),
            )
            for e, chip in enumerate(self.chip_ids())
        ]

    def vec_shards(self):
        chips = self.place.chips
        return [
            transfer(
                self.vec_held.at[1],
                self.vec_parts.at[chips + d],
                self.vec_sems,
                chips + d,
                target,
            )
            for d, target in enumerate(self.place.shard_peers)
        ]

    def greet(self):
        place = self.place
        greet(
            place.shard_peers + [place.at(c) for c in self.chip_ids()] + [place.core_peer]
        )

    def begin(self):
        for i in range(len(self.chunks)):
            start(self.cores(i))
        if self.vec_along:
            self.vec_begin()

    def vec_begin(self):
        start(self.vec_cores())

    def all_to_chips(self):
        for i in range(len(self.chunks)):
            self.to_chips(i)
        if self.vec_along:
            self.vec_to_chips()

    def all_to_shards(self):
        for i in range(len(self.chunks)):
            self.to_shards(i)
        if self.vec_along:
            self.vec_to_shards()

    def all_to_spread(self):
        for i in range(len(self.chunks)):
            self.to_spread(i)
        if self.vec_along:
            self.vec_end()

    def all_to_join(self):
        for i in range(len(self.chunks)):
            self.to_join(i)

    def to_chips(self, i):
        chunk = self.chunks[i]
        own = chunk.part(self.ins[chunk.array], self.place.core)[...]
        arrive(self.cores(i))
        self.core_sum[i][...] = own + self.core_sum[i][...]
        start(self.shards(i) if chunk.shards_first else self.chips(i))

    def vec_to_chips(self):
        arrive(self.vec_cores())
        self.vec_held[0] = self.vec_in[...] + self.vec_parts[0]
        start(self.vec_chips())

    def to_shards(self, i):
        chunk = self.chunks[i]
        piece = self.place.piece(chunk)
        if chunk.shards_first:
            own, copies, terms = self.core_sum[i][self.place.mine], self.shards(i), self.from_shards[i]
        else:
            own = self.core_sum[i][:, pl.ds(piece * chunk.run, chunk.run)]
            copies, terms = self.chips(i), self.from_chips[i]
        arrive(copies)
        total = add_up(own, [terms[e] for e in range(len(copies))])
        self.chip_sum[i][...] = total.astype(BF16)
        start(self.chips(i) if chunk.shards_first else self.shards(i))

    def vec_to_shards(self):
        copies = self.vec_chips()
        arrive(copies)
        self.vec_held[1] = add_up(
            self.vec_held[0], [self.vec_parts[1 + e] for e in range(len(copies))]
        )
        start(self.vec_shards())

    def to_spread(self, i):
        chunk, place = self.chunks[i], self.place
        if chunk.shards_first:
            own = self.chip_sum[i][pl.ds(place.piece(chunk) * chunk.run, chunk.run)]
            copies, terms = self.chips(i), self.from_chips[i]
        else:
            own, copies, terms = self.chip_sum[i][place.mine], self.shards(i), self.from_shards[i]
        arrive(copies)
        total = add_up(own, [terms[d] for d in range(len(copies))])
        block = chunk.part(self.outs[chunk.array], place.core, place.piece(chunk), 0)
        block[...] = total.astype(BF16)
        start(self.spread(i))

    def vec_end(self):
        copies = self.vec_shards()
        arrive(copies)
        self.vec_out[...] = add_up(
            self.vec_held[1], [self.vec_parts[self.place.chips + d] for d in range(len(copies))]
        )

    def to_join(self, i):
        arrive(self.spread(i))
        start(self.join(i))

    def finish(self):
        every = range(len(self.chunks))
        for i in every:
            arrive(self.join(i))
        copies = []
        if self.vec_in is not None:
            copies = self.vec_cores() + self.vec_chips() + self.vec_shards()
        for i in every:
            copies += self.cores(i) + self.chips(i) + self.shards(i)
            copies += self.spread(i) + self.join(i)
        for copy in copies:
            copy.wait_send()


def on_device(
    reps,
    images,
    cotangent,
    ln1_gain,
    ln1_bias,
    w_qkv,
    q_bias,
    v_bias,
    w_proj,
    proj_bias,
    ln2_gain,
    ln2_bias,
    w_up,
    up_bias,
    w_down,
    down_bias,
):
    groups = lax.axis_size("grp")
    sizes = (groups, reps)
    layers, part = ln1_gain.shape
    width = part * groups
    hidden_part = up_bias.shape[1]
    plan = Plan(images.shape, hidden_part * groups)
    vectors = [ln1_gain, ln1_bias, q_bias, v_bias, proj_bias, ln2_gain, ln2_bias, down_bias]
    extra = hidden_part // part
    packed = jnp.stack(vectors, axis=1)
    packed = jnp.concatenate([packed, up_bias.reshape(layers, extra, part)], axis=1)
    packed = packed.astype(F32)
    joined = jnp.concatenate([w_qkv, w_proj], axis=2)

    def shards_of(layer):
        return [m[layer].reshape(1, -1, 8, m.shape[2]) for m in (joined, w_up, w_down)]

    def unpack(vecs):
        vectors = vecs[:, :VECTORS].transpose(1, 0, 2).reshape(VECTORS, width)
        up = vecs[:, VECTORS:].reshape(extra, width)
        rest = plan.vec_rows - VECTORS - extra
        return jnp.concatenate([vectors, up, jnp.zeros((rest, width), F32)], axis=0)

    shards0, shards1 = shards_of(0), shards_of(1)
    first_matrix, vecs0 = gather(shards0[0], packed[0][None], sizes, 0)
    first_matrix, vecs0 = first_matrix.reshape(width, -1), unpack(vecs0)
    hidden, keeps, mlp0, gathered = plan.first(
        images, first_matrix, vecs0, shards0[1:], shards1 + [packed[1][None]], sizes, 1
    )
    weights1 = [g.reshape(-1, g.shape[3]) for g in gathered[:3]]
    encoded, flowing, grads1 = plan.middle(hidden, cotangent, weights1, unpack(gathered[3]))
    blocks = [g.reshape(groups, -1, 8, g.shape[1]) for g in grads1[:3]] + [grads1[3]]
    images_grad, sums, small0, small1 = plan.last(
        flowing, images, [first_matrix] + list(mlp0), vecs0, keeps, blocks, sizes, 2
    )
    full = [x.reshape(layers, -1, x.shape[3]).astype(F32) for x in sums]
    small = jnp.stack([small0, small1])
    me = lax.axis_index("grp")
    vec_out = lax.dynamic_slice_in_dim(small[:, :VECTORS], me * part, part, axis=2)
    up_out = small[:, VECTORS : VECTORS + extra].reshape(layers, -1)
    up_out = lax.dynamic_slice_in_dim(up_out, me * hidden_part, hidden_part, axis=1)
    return (
        encoded,
        images_grad,
        vec_out[:, G1],
        vec_out[:, B1],
        full[0],
        vec_out[:, QB],
        vec_out[:, VB],
        full[1],
        vec_out[:, PB],
        vec_out[:, G2],
        vec_out[:, B2],
        full[2],
        up_out,
        full[3],
        vec_out[:, DB],
    )


def solution(mesh):
    batch = P(("rep", "grp"), None, None)
    vector = P(None, "grp")
    matrix = P(None, "grp", None)
    params = (
        vector,
        vector,
        matrix,
        vector,
        vector,
        matrix,
        vector,
        vector,
        vector,
        matrix,
        vector,
        matrix,
        vector,
    )
    specs = (batch, batch) + params
    return jax.shard_map(
        functools.partial(on_device, mesh.shape["rep"]), mesh=mesh, in_specs=specs, out_specs=specs, check_vma=False
    )
```
